64 devices in a mesh: dp: 4 (over x, y), sp: 16 (over z, core).
Axes of the slice: x: 2, y: 2, z: 8, core: 2. Of those that a mesh axis runs over, the one named last changes fastest.
The devices are a block of a 4x4x8 slice.
Arguments:
- latent: bfloat16 [64, 32, 32, 1280], P('dp', 'sp'), parts along dimension 0
- time_emb: bfloat16 [64, 1280], P('dp'), parts along dimension 0
- context: bfloat16 [64, 77, 2048], P('dp'), parts along dimension 0
- res_conv: bfloat16 [2, 2, 3, 3, 1280, 1280], replicated
- res_time: bfloat16 [2, 1280, 1280], replicated
- res_norm: bfloat16 [2, 2, 2, 32, 40], replicated
- attn_norm: bfloat16 [2, 32, 40], replicated
- proj_inout: bfloat16 [2, 1280, 1280], replicated
- self_qkv: bfloat16 [3, 1280, 20, 64], replicated
- self_out: bfloat16 [20, 64, 1280], replicated
- cross_q: bfloat16 [1280, 20, 64], replicated
- cross_kv: bfloat16 [2, 2048, 20, 64], replicated
- cross_out: bfloat16 [20, 64, 1280], replicated
- ff_in: bfloat16 [1280, 10240], replicated
- ff_out: bfloat16 [5120, 1280], replicated
Outputs:
- output: bfloat16 [64, 32, 32, 1280], P('dp', 'sp'), parts along dimension 0
There are 4 independent parts. The reference program is written for one: setup_inputs(seed, part) draws one part's arguments, and reference() takes and returns one part's arrays. A program takes and returns all parts, laid end to end along the dimension named above; an argument that names none is the same for every part.
All inputs are finite; a program needn't handle non-finite values.
Results may differ from the reference program's by a relative error of at most 0.0133442.
Values are sent between devices in bfloat16 or wider.
A program may use at most 768 MiB of HBM per device.

```python
import math
import jax
import jax.numpy as jnp
from jax import lax

BATCH = 16
BANDS = 16
BAND_ROWS = 2
WIDTH = 32
CHANNELS = 1280
GROUPS = 32
HEADS = 20
TEXT = 77
TEXT_DIM = 2048
TIME_DIM = 1280

HEIGHT = BANDS * BAND_ROWS
TOKENS = HEIGHT * WIDTH
BAND_TOKENS = BAND_ROWS * WIDTH
HEAD_DIM = CHANNELS // HEADS
GROUP_WIDTH = CHANNELS // GROUPS
GN_EPS = 1e-6
LN_EPS = 1e-5


def normal_weight(rng_key, out_shape, std_scale):
    return (jax.random.normal(rng_key, out_shape, jnp.float32) * std_scale).astype(jnp.bfloat16)


def norm_params(rng_key, lead_shape):
    spread = 0.4 * jax.random.normal(rng_key, lead_shape + (2, GROUPS, GROUP_WIDTH), jnp.float32)
    offset = jnp.array([1.0, 0.0], jnp.float32)[:, None, None]
    return (spread + offset).astype(jnp.bfloat16)


def setup_inputs(seed: int = 0, part: int = 0) -> dict:
    part_keys = jax.random.split(jax.random.fold_in(jax.random.key(seed), part), 5)
    weight_keys = jax.random.split(jax.random.key(seed + 1), 12)
    rows_pos = (jnp.arange(HEIGHT, dtype=jnp.float32) + 0.5) / HEIGHT
    wave_phase = jax.random.uniform(part_keys[0], (BATCH, 1, 1, 1), jnp.float32, 0.0, 2.0 * math.pi)
    loading = 1.0 + 0.5 * jax.random.normal(part_keys[1], (BATCH, 1, 1, CHANNELS), jnp.float32)
    row_wave = jnp.cos(math.pi * rows_pos[None, :, None, None] + wave_phase)
    white_noise = jax.random.normal(part_keys[2], (BATCH, HEIGHT, WIDTH, CHANNELS), jnp.float32)
    self_sharp = math.sqrt(math.log(TOKENS))
    cross_sharp = math.sqrt(math.log(TEXT))
    chan_scale = CHANNELS ** -0.5
    qkv_scale = chan_scale * jnp.array([self_sharp, 1.0, 1.0], jnp.float32)[:, None, None, None]
    return {
        'latent': (white_noise + 1.5 * row_wave * loading).astype(jnp.bfloat16),
        'time_emb': jax.random.normal(part_keys[3], (BATCH, TIME_DIM), jnp.float32).astype(jnp.bfloat16),
        'context': jax.random.normal(part_keys[4], (BATCH, TEXT, TEXT_DIM), jnp.float32).astype(jnp.bfloat16),
        'res_conv': normal_weight(weight_keys[0], (2, 2, 3, 3, CHANNELS, CHANNELS), (9 * CHANNELS) ** -0.5),
        'res_time': normal_weight(weight_keys[1], (2, TIME_DIM, CHANNELS), TIME_DIM ** -0.5),
        'res_norm': norm_params(weight_keys[2], (2, 2)),
        'attn_norm': norm_params(weight_keys[3], ()),
        'proj_inout': normal_weight(weight_keys[4], (2, CHANNELS, CHANNELS), chan_scale),
        'self_qkv': normal_weight(weight_keys[5], (3, CHANNELS, HEADS, HEAD_DIM), qkv_scale),
        'self_out': normal_weight(weight_keys[6], (HEADS, HEAD_DIM, CHANNELS), chan_scale),
        'cross_q': normal_weight(weight_keys[7], (CHANNELS, HEADS, HEAD_DIM), chan_scale * cross_sharp),
        'cross_kv': normal_weight(weight_keys[8], (2, TEXT_DIM, HEADS, HEAD_DIM), TEXT_DIM ** -0.5),
        'cross_out': normal_weight(weight_keys[9], (HEADS, HEAD_DIM, CHANNELS), chan_scale),
        'ff_in': normal_weight(weight_keys[10], (CHANNELS, 8 * CHANNELS), chan_scale),
        'ff_out': normal_weight(weight_keys[11], (4 * CHANNELS, CHANNELS), (4 * CHANNELS) ** -0.5),
    }


def group_norm(hidden, scale_shift):
    feat_f32 = hidden.astype(jnp.float32).reshape(BATCH, TOKENS, GROUPS, GROUP_WIDTH)
    grp_mean = jnp.mean(feat_f32, axis=(1, 3), keepdims=True)
    grp_msq = jnp.mean(feat_f32 * feat_f32, axis=(1, 3), keepdims=True)
    normed = (feat_f32 - grp_mean) * lax.rsqrt(grp_msq - grp_mean * grp_mean + GN_EPS)
    normed = normed * scale_shift[0].astype(jnp.float32) + scale_shift[1].astype(jnp.float32)
    return normed.reshape(BATCH, HEIGHT, WIDTH, CHANNELS)


def conv_same(act_in, kernel):
    return lax.conv_general_dilated(act_in.astype(jnp.float32), kernel.astype(jnp.float32), (1, 1), 'SAME', dimension_numbers=('NHWC', 'HWIO', 'NHWC'))


def res_block(hidden, time_emb, kernels, time_weight, norm_pair):
    act_one = jax.nn.silu(group_norm(hidden, norm_pair[0])).astype(jnp.bfloat16)
    time_act = jax.nn.silu(time_emb.astype(jnp.float32)).astype(jnp.bfloat16)
    time_proj = jnp.dot(time_act, time_weight, preferred_element_type=jnp.float32)
    mid_act = (conv_same(act_one, kernels[0]) + time_proj[:, None, None, :]).astype(jnp.bfloat16)
    act_two = jax.nn.silu(group_norm(mid_act, norm_pair[1])).astype(jnp.bfloat16)
    return (hidden.astype(jnp.float32) + conv_same(act_two, kernels[1])).astype(jnp.bfloat16)


def layer_norm(tokens):
    feat_f32 = tokens.astype(jnp.float32)
    centred = feat_f32 - jnp.mean(feat_f32, axis=-1, keepdims=True)
    return (centred * lax.rsqrt(jnp.mean(centred * centred, axis=-1, keepdims=True) + LN_EPS)).astype(jnp.bfloat16)


def project(rows_flat, weight):
    return jnp.dot(rows_flat, weight.reshape(weight.shape[0], -1), preferred_element_type=jnp.float32).astype(jnp.bfloat16)


def attend(queries, key_all, val_all):
    logits = jnp.einsum('bqhd,bkhd->bhqk', queries.astype(jnp.float32), key_all.astype(jnp.float32)) * (HEAD_DIM ** -0.5)
    row_max = jnp.max(logits, axis=-1, keepdims=True)
    weights = jnp.exp(logits - row_max)
    row_sum = jnp.sum(weights, axis=-1)
    weighted = jnp.einsum('bhqk,bkhd->bhqd', weights.astype(jnp.bfloat16).astype(jnp.float32), val_all.astype(jnp.float32))
    return (weighted / row_sum[..., None]).astype(jnp.bfloat16)


def out_project(attended, weight):
    return jnp.einsum('bhqd,hdc->bqc', attended.astype(jnp.float32), weight.astype(jnp.float32))


def transformer_block(hidden, context, attn_norm, proj_inout, self_qkv, self_out, cross_q, cross_kv, cross_out, ff_in, ff_out):
    normed = group_norm(hidden, attn_norm).astype(jnp.bfloat16).reshape(BATCH * TOKENS, CHANNELS)
    tokens = jnp.dot(normed, proj_inout[0], preferred_element_type=jnp.float32).astype(jnp.bfloat16)
    ln_tokens = layer_norm(tokens)
    key_all = project(ln_tokens, self_qkv[1]).reshape(BATCH, TOKENS, HEADS, HEAD_DIM)
    val_all = project(ln_tokens, self_qkv[2]).reshape(BATCH, TOKENS, HEADS, HEAD_DIM)
    ctx_flat = context.reshape(BATCH * TEXT, TEXT_DIM)
    ctx_key = project(ctx_flat, cross_kv[0]).reshape(BATCH, TEXT, HEADS, HEAD_DIM)
    ctx_val = project(ctx_flat, cross_kv[1]).reshape(BATCH, TEXT, HEADS, HEAD_DIM)
    flat_count = BATCH * BAND_TOKENS

    def band_step(operands):
        resid_band, tok_band, ln_band = operands
        self_query = project(ln_band.reshape(flat_count, CHANNELS), self_qkv[0]).reshape(BATCH, BAND_TOKENS, HEADS, HEAD_DIM)
        self_att = out_project(attend(self_query, key_all, val_all), self_out)
        tok_one = (tok_band.astype(jnp.float32) + self_att).astype(jnp.bfloat16)
        cross_query = project(layer_norm(tok_one).reshape(flat_count, CHANNELS), cross_q).reshape(BATCH, BAND_TOKENS, HEADS, HEAD_DIM)
        cross_att = out_project(attend(cross_query, ctx_key, ctx_val), cross_out)
        tok_two = (tok_one.astype(jnp.float32) + cross_att).astype(jnp.bfloat16).reshape(flat_count, CHANNELS)
        hidden_ff = jnp.dot(layer_norm(tok_two), ff_in, preferred_element_type=jnp.float32)
        gated_ff = (hidden_ff[:, :4 * CHANNELS] * jax.nn.gelu(hidden_ff[:, 4 * CHANNELS:], approximate=False)).astype(jnp.bfloat16)
        tok_three = (tok_two.astype(jnp.float32) + jnp.dot(gated_ff, ff_out, preferred_element_type=jnp.float32)).astype(jnp.bfloat16)
        block_out = resid_band.reshape(flat_count, CHANNELS).astype(jnp.float32) + jnp.dot(tok_three, proj_inout[1], preferred_element_type=jnp.float32)
        return block_out.astype(jnp.bfloat16).reshape(BATCH, BAND_TOKENS, CHANNELS)

    def to_bands(array_in):
        return jnp.swapaxes(array_in.reshape(BATCH, BANDS, BAND_TOKENS, CHANNELS), 0, 1)

    band_out = lax.map(band_step, (to_bands(hidden), to_bands(tokens), to_bands(ln_tokens)))
    return jnp.swapaxes(band_out, 0, 1).reshape(BATCH, HEIGHT, WIDTH, CHANNELS)


def reference(latent, time_emb, context, res_conv, res_time, res_norm, attn_norm, proj_inout, self_qkv, self_out, cross_q, cross_kv, cross_out, ff_in, ff_out):
    after_first = res_block(latent, time_emb, res_conv[0], res_time[0], res_norm[0])
    middle = transformer_block(after_first, context, attn_norm, proj_inout, self_qkv, self_out, cross_q, cross_kv, cross_out, ff_in, ff_out)
    return res_block(middle, time_emb, res_conv[1], res_time[1], res_norm[1])
```

```python
import functools

import jax
import jax.numpy as jnp
from jax import lax
from jax.experimental import pallas as pl
from jax.experimental.pallas import tpu as pltpu
from jax.sharding import PartitionSpec as P

BF16 = jnp.bfloat16
F32 = jnp.float32
MESH = pl.DeviceIdType.MESH
GN_EPS = 1e-6
LN_EPS = 1e-5
TM = 256
CK = 256
VMEM_LIMIT = 67_000_000


def nn(lhs, rhs):
    return lax.dot_general(lhs, rhs, (((1,), (0,)), ((), ())), preferred_element_type=F32)


def nt(lhs, rhs):
    return lax.dot_general(lhs, rhs, (((1,), (1,)), ((), ())), preferred_element_type=F32)


def split3(vals):
    high = vals.astype(BF16).astype(F32)
    rest = vals - high
    mid = rest.astype(BF16).astype(F32)
    return [high, mid, rest - mid]


def channel_sums(src, rows, chans):
    def step(idx, carry):
        tot, sqr = carry
        vals = src[pl.ds(pl.multiple_of(idx * 64, 64), 64), :].astype(F32).reshape(8, 8, chans)
        return tot + jnp.sum(vals, axis=0), sqr + jnp.sum(vals * vals, axis=0)

    zero = jnp.zeros((8, chans), F32)
    return lax.fori_loop(0, rows // 64, step, (zero, zero))


def group_affine(tot, sqr, gain, shift, groups, count, coef):
    chans = tot.shape[1]
    width = chans // groups
    terms = split3(jnp.sum(tot, axis=0, keepdims=True)) + split3(jnp.sum(sqr, axis=0, keepdims=True))
    rows = jnp.concatenate(terms + [jnp.zeros((2, chans), F32)], axis=0).astype(BF16)
    chan = lax.broadcasted_iota(jnp.int32, (chans, 128), 0)
    low = lax.broadcasted_iota(jnp.int32, (chans, 128), 1) * width
    member = jnp.where((chan >= low) & (chan < low + width), 1.0, 0.0).astype(BF16)
    sums = nn(rows, member)
    mean = (sums[0:1] + sums[1:2] + sums[2:3]) / count
    msq = (sums[3:4] + sums[4:5] + sums[5:6]) / count
    rstd = lax.rsqrt(msq - mean * mean + GN_EPS)
    back = jnp.concatenate(split3(mean) + split3(rstd) + [jnp.zeros((2, 128), F32)], axis=0).astype(BF16)
    wide = nt(back, member)
    coef[0:1, :] = wide[0:1] + wide[1:2] + wide[2:3]
    coef[1:2, :] = (wide[3:4] + wide[4:5] + wide[5:6]) * gain
    coef[2:3, :] = shift


def layer_norm(tokens):
    centred = tokens - jnp.mean(tokens, axis=-1, keepdims=True)
    return (centred * lax.rsqrt(jnp.mean(centred * centred, axis=-1, keepdims=True) + LN_EPS)).astype(BF16)


def exchange(blocks, collective):
    num = blocks.shape[0]

    def kernel(src, dst, stage, send_sem, recv_sem, own_sem):
        me = lax.axis_index('sp')
        barrier = pltpu.get_barrier_semaphore()
        for step in range(1, num):
            pl.semaphore_signal(barrier, inc=1, device_id={'sp': lax.rem(me + step, num)}, device_id_type=MESH)
        pl.semaphore_wait(barrier, num - 1)
        copies = []
        order = sorted(range(1, num), key=lambda step: -min(step, num - step))
        for step in order:
            peer = lax.rem(me + step, num)
            copy = pltpu.make_async_remote_copy(src.at[peer], dst.at[me], send_sem.at[step], recv_sem.at[step], device_id={'sp': peer}, device_id_type=MESH)
            copy.start()
            copies.append(copy)
        own_in = pltpu.make_async_copy(src.at[me], stage, own_sem)
        own_in.start()
        own_in.wait()
        own_out = pltpu.make_async_copy(stage, dst.at[me], own_sem)
        own_out.start()
        own_out.wait()
        for copy in copies:
            copy.wait()

    return pl.pallas_call(
        kernel,
        out_shape=jax.ShapeDtypeStruct(blocks.shape, blocks.dtype),
        in_specs=[pl.BlockSpec(memory_space=pl.ANY)],
        out_specs=pl.BlockSpec(memory_space=pl.ANY),
        scratch_shapes=[pltpu.VMEM(blocks.shape[1:], blocks.dtype), pltpu.SemaphoreType.DMA((num,)), pltpu.SemaphoreType.DMA((num,)), pltpu.SemaphoreType.DMA],
        compiler_params=pltpu.CompilerParams(collective_id=collective, has_side_effects=True),
        name='exchange',
    )(blocks)


def res_block(hidden, res_conv, norms, time_proj, which, width, groups):
    tokens, chans = hidden.shape
    chunks = chans // CK
    tiles = tokens // TM
    count = float(tokens * (chans // groups))

    def kernel(x_ref, kern, norm_ref, time_ref, out_ref, acc, mid, act, wbuf, coef, wsem):
        def fetch(step, slot):
            conv, chunk = step // chunks, lax.rem(step, chunks)
            rows = pl.ds(pl.multiple_of(chunk * CK, CK), CK)
            return [pltpu.make_async_copy(kern.at[which, conv, dy, dx, rows, :], wbuf.at[slot, dy, pl.ds(dx * CK, CK), :], wsem.at[slot])
                    for dy in range(3) for dx in range(3)]

        for copy in fetch(0, 0):
            copy.start()
        edge = jnp.zeros((width, 3 * CK), BF16)
        for slot in range(2):
            act[slot, 0:width, :] = edge
            act[slot, width + tokens:2 * width + tokens, :] = edge
        column = lax.rem(lax.broadcasted_iota(jnp.int32, (TM, CK), 0), width)

        def build(src, chunk, tile, slot):
            cols = pl.ds(pl.multiple_of(chunk * CK, CK), CK)
            rows = pl.multiple_of(tile * TM, TM)
            vals = src[pl.ds(rows, TM), cols].astype(F32)
            vals = (vals - coef[0:1, cols]) * coef[1:2, cols] + coef[2:3, cols]
            vals = vals * (1.0 / (1.0 + jnp.exp(-vals)))
            put = pl.ds(rows + width, TM)
            act[slot, put, 0:CK] = jnp.where(column == 0, 0.0, pltpu.roll(vals, 1, 0)).astype(BF16)
            act[slot, put, CK:2 * CK] = vals.astype(BF16)
            act[slot, put, 2 * CK:3 * CK] = jnp.where(column == width - 1, 0.0, pltpu.roll(vals, TM - 1, 0)).astype(BF16)

        def conv(src, index):
            @pl.loop(0, tiles)
            def _(tile):
                build(src, 0, tile, 0)

            acc[...] = jnp.zeros_like(acc)

            @pl.loop(0, chunks)
            def _(chunk):
                step = index * chunks + chunk
                wslot = lax.rem(step, 2)
                slot = lax.rem(chunk, 2)

                @pl.when(step + 1 < 2 * chunks)
                def _():
                    for copy in fetch(step + 1, 1 - wslot):
                        copy.start()

                for copy in fetch(step, wslot):
                    copy.wait()

                @pl.loop(0, tiles)
                def _(tile):
                    rows = pl.multiple_of(tile * TM, TM)
                    part = nn(act[slot, pl.ds(rows, TM), :], wbuf[wslot, 0])
                    part += nn(act[slot, pl.ds(rows + width, TM), :], wbuf[wslot, 1])
                    part += nn(act[slot, pl.ds(rows + 2 * width, TM), :], wbuf[wslot, 2])
                    acc[pl.ds(rows, TM), :] += part
                    build(src, lax.rem(chunk + 1, chunks), tile, 1 - slot)

        tot, sqr = channel_sums(x_ref, tokens, chans)
        group_affine(tot, sqr, norm_ref[0:1], norm_ref[1:2], groups, count, coef)
        conv(x_ref, 0)

        @pl.loop(0, tokens // 64)
        def _(idx):
            rows = pl.ds(pl.multiple_of(idx * 64, 64), 64)
            mid[rows, :] = (acc[rows, :] + time_ref[0:1]).astype(BF16)

        tot, sqr = channel_sums(mid, tokens, chans)
        group_affine(tot, sqr, norm_ref[2:3], norm_ref[3:4], groups, count, coef)
        conv(mid, 1)

        @pl.loop(0, tokens // 64)
        def _(idx):
            rows = pl.ds(pl.multiple_of(idx * 64, 64), 64)
            out_ref[rows, :] = (x_ref[rows, :].astype(F32) + acc[rows, :]).astype(BF16)

    flops = 2 * 2 * 9 * tokens * chans * chans
    vmem = pl.BlockSpec(memory_space=pltpu.VMEM)
    return pl.pallas_call(
        kernel,
        out_shape=jax.ShapeDtypeStruct(hidden.shape, BF16),
        in_specs=[vmem, pl.BlockSpec(memory_space=pl.ANY), vmem, vmem],
        out_specs=vmem,
        scratch_shapes=[
            pltpu.VMEM((tokens, chans), F32),
            pltpu.VMEM((tokens, chans), BF16),
            pltpu.VMEM((2, tokens + 2 * width, 3 * CK), BF16),
            pltpu.VMEM((2, 3, 3 * CK, chans), BF16),
            pltpu.VMEM((8, chans), F32),
            pltpu.SemaphoreType.DMA((2,)),
        ],
        compiler_params=pltpu.CompilerParams(vmem_limit_bytes=VMEM_LIMIT),
        cost_estimate=pl.CostEstimate(flops=flops, bytes_accessed=2 * 9 * chans * chans * 2, transcendentals=0),
        name='res_block',
    )(hidden, res_conv, norms, time_proj)


def transformer(hidden, context, norms, proj_inout, qkv_t, self_out, cross_q_t, cross_kv_t, cross_out, ff_in, ff_out, groups, heads, text):
    tokens, chans = hidden.shape
    text_rows, text_dim = context.shape
    head_dim = chans // heads
    pairs = heads // 2
    pair = 2 * head_dim
    count = float(tokens * (chans // groups))
    tiles = tokens // TM
    ff_steps = ff_out.shape[0] // chans
    slots = 4
    qb = 256
    scale = head_dim ** -0.5
    half = chans // 2

    def kernel(h_ref, ctx_ref, norm_ref, pio, wqkv, wo, cq, ckv, co, f1, f2, out_ref,
               ring, ckvbuf, tok, aux, q_t, keys, v_t, logit, acc, ctx_k, ctx_v, coef, rsem, csem):
        units = [pio.at[0], wqkv.at[0], wqkv.at[1], wqkv.at[2], wo, cq, co]
        for f in range(ff_steps):
            units += [f1.at[:, pl.ds(f * chans, chans)], f1.at[:, pl.ds((ff_steps + f) * chans, chans)], f2.at[pl.ds(f * chans, chans), :]]
        units.append(pio.at[1])

        def copy_of(unit):
            return pltpu.make_async_copy(units[unit], ring.at[unit % slots], rsem.at[unit % slots])

        def take(unit):
            copy_of(unit).wait()
            return ring.at[unit % slots]

        def done(unit):
            if unit + slots < len(units):
                copy_of(unit + slots).start()

        for unit in range(slots):
            copy_of(unit).start()
        ctx_copy = pltpu.make_async_copy(ckv, ckvbuf, csem)
        ctx_copy.start()

        def tile_rows(tile):
            return pl.ds(pl.multiple_of(tile * TM, TM), TM)

        tot, sqr = channel_sums(h_ref, tokens, chans)
        group_affine(tot, sqr, norm_ref[0:1], norm_ref[1:2], groups, count, coef)

        w_in = take(0)

        @pl.loop(0, tiles)
        def _(tile):
            rows = tile_rows(tile)
            normed = ((h_ref[rows, :].astype(F32) - coef[0:1]) * coef[1:2] + coef[2:3]).astype(BF16)
            t = nn(normed, w_in[...]).astype(BF16)
            tok[rows, :] = t
            aux[rows, :] = layer_norm(t.astype(F32))
        done(0)

        def transposed(weight, src, dst, factor):
            @pl.loop(0, 2)
            def _(part):
                rows = pl.ds(pl.multiple_of(part * half, half), half)
                dst[rows, :] = (nt(weight[rows, :], src[...]).astype(BF16) * factor).astype(BF16) if factor != 1.0 else nt(weight[rows, :], src[...]).astype(BF16)

        transposed(take(1), aux, q_t, scale)
        done(1)
        w_key = take(2)

        @pl.loop(0, tokens // 512)
        def _(part):
            rows = pl.ds(pl.multiple_of(part * 512, 512), 512)
            keys[rows, :] = nt(aux[rows, :], w_key[...]).astype(BF16)
        done(2)
        transposed(take(3), aux, v_t, 1.0)
        done(3)

        lane_head = lax.broadcasted_iota(jnp.int32, (pair, qb), 0)

        def softmax_block(scores, valid):
            if valid is not None:
                scores = jnp.where(valid, scores, -jnp.inf)
            top = jnp.max(scores, axis=0, keepdims=True)
            weights = jnp.exp(scores - top)
            return weights.astype(BF16), jnp.sum(weights, axis=0, keepdims=True)

        def attend(key_ref, val_ref, key_rows, valid, dst):
            @pl.loop(0, pairs)
            def _(hp):
                cols = pl.ds(pl.multiple_of(hp * pair, pair), pair)
                for j in range(tokens // qb):
                    both = q_t[cols, j * qb:(j + 1) * qb]
                    outs = []
                    for h in range(2):
                        mine = (lane_head < head_dim) if h == 0 else (lane_head >= head_dim)
                        query = jnp.where(mine, both, jnp.zeros_like(both))
                        scores = nn(key_ref[:, cols], query)
                        weights, denom = softmax_block(scores, valid)
                        vals = val_ref[pl.ds(pl.multiple_of(hp * pair + h * head_dim, head_dim), head_dim), :]
                        outs.append(nn(vals, weights) / denom)
                    out = jnp.concatenate(outs, axis=0)
                    dst[j * qb:(j + 1) * qb, cols] = out.T.astype(BF16)

        attend(keys, v_t, tokens, None, aux)

        w_out = take(4)

        @pl.loop(0, tiles)
        def _(tile):
            rows = tile_rows(tile)
            t = (tok[rows, :].astype(F32) + nn(aux[rows, :], w_out[...])).astype(BF16)
            tok[rows, :] = t
            keys[rows, :] = layer_norm(t.astype(F32))
        done(4)

        transposed(take(5), keys, q_t, scale)
        done(5)
        ctx_copy.wait()
        ctx_k[...] = nt(ctx_ref[...], ckvbuf[0]).astype(BF16)

        @pl.loop(0, chans // 256)
        def _(part):
            rows = pl.ds(pl.multiple_of(part * 256, 256), 256)
            ctx_v[rows, :] = nt(ckvbuf[1, rows, :], ctx_ref[...]).astype(BF16)

        text_valid = lax.broadcasted_iota(jnp.int32, (text_rows, qb), 0) < text
        attend(ctx_k, ctx_v, text_rows, text_valid, aux)

        w_cross = take(6)

        @pl.loop(0, tiles)
        def _(tile):
            rows = tile_rows(tile)
            t = (tok[rows, :].astype(F32) + nn(aux[rows, :], w_cross[...])).astype(BF16)
            tok[rows, :] = t
            keys[rows, :] = layer_norm(t.astype(F32))
        done(6)

        acc[...] = jnp.zeros_like(acc)
        for f in range(ff_steps):
            base = 7 + 3 * f
            w_val, w_gate, w_down = take(base), take(base + 1), take(base + 2)

            @pl.loop(0, tiles)
            def _(tile):
                rows = tile_rows(tile)
                src = keys[rows, :]
                value = nn(src, w_val[...])
                gate = nn(src, w_gate[...])
                gated = (value * (0.5 * gate * (1.0 + lax.erf(gate * (0.5 ** 0.5))))).astype(BF16)
                acc[rows, :] += nn(gated, w_down[...])
            done(base)
            done(base + 1)
            done(base + 2)

        last = len(units) - 1
        w_fin = take(last)

        @pl.loop(0, tiles)
        def _(tile):
            rows = tile_rows(tile)
            t = (tok[rows, :].astype(F32) + acc[rows, :]).astype(BF16)
            out_ref[rows, :] = (h_ref[rows, :].astype(F32) + nn(t, w_fin[...])).astype(BF16)

    vmem = pl.BlockSpec(memory_space=pltpu.VMEM)
    hbm = pl.BlockSpec(memory_space=pl.ANY)
    flops = 2 * tokens * chans * chans * (8 + 3 * ff_steps) + 4 * tokens * tokens * chans
    return pl.pallas_call(
        kernel,
        out_shape=jax.ShapeDtypeStruct(hidden.shape, BF16),
        in_specs=[vmem, vmem, vmem] + [hbm] * 8,
        out_specs=vmem,
        scratch_shapes=[
            pltpu.VMEM((slots, chans, chans), BF16),
            pltpu.VMEM((2, chans, text_dim), BF16),
            pltpu.VMEM((tokens, chans), BF16),
            pltpu.VMEM((tokens, chans), BF16),
            pltpu.VMEM((chans, tokens), BF16),
            pltpu.VMEM((tokens, chans), BF16),
            pltpu.VMEM((chans, tokens), BF16),
            pltpu.VMEM((8, 128), F32),
            pltpu.VMEM((tokens, chans), F32),
            pltpu.VMEM((text_rows, chans), BF16),
            pltpu.VMEM((chans, text_rows), BF16),
            pltpu.VMEM((8, chans), F32),
            pltpu.SemaphoreType.DMA((slots,)),
            pltpu.SemaphoreType.DMA,
        ],
        compiler_params=pltpu.CompilerParams(vmem_limit_bytes=VMEM_LIMIT),
        cost_estimate=pl.CostEstimate(flops=flops, bytes_accessed=80_000_000, transcendentals=tokens * tokens * heads),
        name='transformer',
    )(hidden, context, norms, proj_inout, qkv_t, self_out, cross_q_t, cross_kv_t, cross_out, ff_in, ff_out)


def solution(mesh):
    num_bands = mesh.shape['sp']

    def local_stage(latent, time_emb, context, res_conv, res_time, res_norm, attn_norm, proj_inout, self_qkv, self_out, cross_q, cross_kv, cross_out, ff_in, ff_out):
        images, band_rows, width, chans = latent.shape
        assert images == num_bands
        band = band_rows * width
        heads, head_dim = self_out.shape[:2]
        groups = res_norm.shape[3]
        text, text_dim = context.shape[1:]
        me = lax.axis_index('sp')

        image = exchange(latent.reshape(images, band, chans), 0).reshape(images * band, chans)
        time_row = lax.dynamic_slice_in_dim(time_emb, me, 1, 0)
        time_act = jax.nn.silu(time_row.astype(F32)).astype(BF16)
        time_proj = jnp.einsum('tc,bcd->btd', time_act, res_time, preferred_element_type=F32)
        norms = res_norm.astype(F32).reshape(2, 4, chans)
        ctx_rows = -(-text // 16) * 16
        ctx = lax.dynamic_index_in_dim(context, me, 0, keepdims=False)
        ctx = jnp.pad(ctx, ((0, ctx_rows - text), (0, 0)))

        first = res_block(image, res_conv, norms[0], time_proj[0], 0, width, groups)
        middle = transformer(
            first, ctx, attn_norm.astype(F32).reshape(2, chans), proj_inout,
            jnp.transpose(self_qkv, (0, 2, 3, 1)).reshape(3, chans, chans),
            self_out.reshape(chans, chans),
            jnp.transpose(cross_q, (1, 2, 0)).reshape(chans, chans),
            jnp.transpose(cross_kv, (0, 2, 3, 1)).reshape(2, chans, text_dim),
            cross_out.reshape(chans, chans), ff_in, ff_out, groups, heads, text)
        last = res_block(middle, res_conv, norms[1], time_proj[1], 1, width, groups)
        out = exchange(last.reshape(num_bands, band, chans), 1)
        return out.reshape(latent.shape)

    band_spec = P('dp', 'sp', None, None)
    shared = P()
    in_specs = (band_spec, P('dp', None), P('dp', None, None)) + (shared,) * 12
    return jax.shard_map(local_stage, mesh=mesh, in_specs=in_specs, out_specs=band_spec, check_vma=False)
```

```python
import functools

import jax
import jax.numpy as jnp
from jax import lax
from jax.experimental import pallas as pl
from jax.experimental.pallas import tpu as pltpu
from jax.sharding import PartitionSpec as P

BF16 = jnp.bfloat16
F32 = jnp.float32
MESH = pl.DeviceIdType.MESH
GN_EPS = 1e-6
LN_EPS = 1e-5
TM = 256
CK = 256
VMEM_LIMIT = 67_000_000


def nn(lhs, rhs):
    return lax.dot_general(lhs, rhs, (((1,), (0,)), ((), ())), preferred_element_type=F32)


def nt(lhs, rhs):
    return lax.dot_general(lhs, rhs, (((1,), (1,)), ((), ())), preferred_element_type=F32)


def split3(vals):
    high = vals.astype(BF16).astype(F32)
    rest = vals - high
    mid = rest.astype(BF16).astype(F32)
    return [high, mid, rest - mid]


def channel_sums(src, rows, chans):
    def step(idx, carry):
        tot, sqr = carry
        vals = src[pl.ds(pl.multiple_of(idx * 64, 64), 64), :].astype(F32).reshape(8, 8, chans)
        return tot + jnp.sum(vals, axis=0), sqr + jnp.sum(vals * vals, axis=0)

    zero = jnp.zeros((8, chans), F32)
    return lax.fori_loop(0, rows // 64, step, (zero, zero))


def group_affine(tot, sqr, gain, shift, groups, count, coef, factor):
    chans = tot.shape[1]
    width = chans // groups
    terms = split3(jnp.sum(tot, axis=0, keepdims=True)) + split3(jnp.sum(sqr, axis=0, keepdims=True))
    rows = jnp.concatenate(terms + [jnp.zeros((2, chans), F32)], axis=0).astype(BF16)
    chan = lax.broadcasted_iota(jnp.int32, (chans, 128), 0)
    low = lax.broadcasted_iota(jnp.int32, (chans, 128), 1) * width
    member = jnp.where((chan >= low) & (chan < low + width), 1.0, 0.0).astype(BF16)
    sums = nn(rows, member)
    mean = (sums[0:1] + sums[1:2] + sums[2:3]) / count
    msq = (sums[3:4] + sums[4:5] + sums[5:6]) / count
    rstd = lax.rsqrt(msq - mean * mean + GN_EPS)
    back = jnp.concatenate(split3(mean) + split3(rstd) + [jnp.zeros((2, 128), F32)], axis=0).astype(BF16)
    wide = nt(back, member)
    scale = (wide[3:4] + wide[4:5] + wide[5:6]) * gain
    coef[0:1, :] = factor * scale
    coef[1:2, :] = factor * (shift - (wide[0:1] + wide[1:2] + wide[2:3]) * scale)


def layer_norm(tokens):
    centred = tokens - jnp.mean(tokens, axis=-1, keepdims=True)
    return (centred * lax.rsqrt(jnp.mean(centred * centred, axis=-1, keepdims=True) + LN_EPS)).astype(BF16)


def exchange(blocks, collective):
    num = blocks.shape[0]

    def kernel(src, dst, stage, send_sem, recv_sem, own_sem):
        me = lax.axis_index('sp')
        barrier = pltpu.get_barrier_semaphore()
        for step in range(1, num):
            pl.semaphore_signal(barrier, inc=1, device_id={'sp': lax.rem(me + step, num)}, device_id_type=MESH)
        pl.semaphore_wait(barrier, num - 1)
        copies = []
        order = sorted(range(1, num), key=lambda step: -min(step, num - step))
        for step in order:
            peer = lax.rem(me + step, num)
            copy = pltpu.make_async_remote_copy(src.at[peer], dst.at[me], send_sem.at[step], recv_sem.at[step], device_id={'sp': peer}, device_id_type=MESH)
            copy.start()
            copies.append(copy)
        own_in = pltpu.make_async_copy(src.at[me], stage, own_sem)
        own_in.start()
        own_in.wait()
        own_out = pltpu.make_async_copy(stage, dst.at[me], own_sem)
        own_out.start()
        own_out.wait()
        for copy in copies:
            copy.wait()

    return pl.pallas_call(
        kernel,
        out_shape=jax.ShapeDtypeStruct(blocks.shape, blocks.dtype),
        in_specs=[pl.BlockSpec(memory_space=pl.ANY)],
        out_specs=pl.BlockSpec(memory_space=pl.ANY),
        scratch_shapes=[pltpu.VMEM(blocks.shape[1:], blocks.dtype), pltpu.SemaphoreType.DMA((num,)), pltpu.SemaphoreType.DMA((num,)), pltpu.SemaphoreType.DMA],
        compiler_params=pltpu.CompilerParams(collective_id=collective, has_side_effects=True),
        name='exchange',
    )(blocks)


def res_block(hidden, res_conv, norms, time_proj, which, width, groups):
    tokens, chans = hidden.shape
    chunks = chans // CK
    tiles = tokens // TM
    count = float(tokens * (chans // groups))

    def kernel(x_ref, kern, norm_ref, time_ref, out_ref, acc, mid, act, wbuf, coef, wsem):
        def fetch(step, slot):
            conv, chunk = step // chunks, lax.rem(step, chunks)
            rows = pl.ds(pl.multiple_of(chunk * CK, CK), CK)
            return [pltpu.make_async_copy(kern.at[which, conv, dy, dx, rows, :], wbuf.at[slot, dy, pl.ds(dx * CK, CK), :], wsem.at[slot])
                    for dy in range(3) for dx in range(3)]

        for copy in fetch(0, 0):
            copy.start()
        edge = jnp.zeros((width, 3 * CK), BF16)
        for slot in range(2):
            act[slot, 0:width, :] = edge
            act[slot, width + tokens:2 * width + tokens, :] = edge
        column = lax.rem(lax.broadcasted_iota(jnp.int32, (TM, CK), 0), width)

        def build(src, chunk, tile, slot):
            cols = pl.ds(pl.multiple_of(chunk * CK, CK), CK)
            rows = pl.multiple_of(tile * TM, TM)
            vals = src[pl.ds(rows, TM), cols].astype(F32)
            half = vals * coef[0:1, cols] + coef[1:2, cols]
            vals = half + half * jnp.tanh(half)
            put = pl.ds(rows + width, TM)
            act[slot, put, 0:CK] = jnp.where(column == 0, 0.0, pltpu.roll(vals, 1, 0)).astype(BF16)
            act[slot, put, CK:2 * CK] = vals.astype(BF16)
            act[slot, put, 2 * CK:3 * CK] = jnp.where(column == width - 1, 0.0, pltpu.roll(vals, TM - 1, 0)).astype(BF16)

        def conv(src, index):
            @pl.loop(0, tiles)
            def _(tile):
                build(src, 0, tile, 0)

            acc[...] = jnp.zeros_like(acc)

            @pl.loop(0, chunks)
            def _(chunk):
                step = index * chunks + chunk
                wslot = lax.rem(step, 2)
                slot = lax.rem(chunk, 2)

                @pl.when(step + 1 < 2 * chunks)
                def _():
                    for copy in fetch(step + 1, 1 - wslot):
                        copy.start()

                for copy in fetch(step, wslot):
                    copy.wait()

                @pl.loop(0, tiles)
                def _(tile):
                    rows = pl.multiple_of(tile * TM, TM)
                    part = nn(act[slot, pl.ds(rows, TM), :], wbuf[wslot, 0])
                    part += nn(act[slot, pl.ds(rows + width, TM), :], wbuf[wslot, 1])
                    part += nn(act[slot, pl.ds(rows + 2 * width, TM), :], wbuf[wslot, 2])
                    acc[pl.ds(rows, TM), :] += part
                    build(src, lax.rem(chunk + 1, chunks), tile, 1 - slot)

        tot, sqr = channel_sums(x_ref, tokens, chans)
        group_affine(tot, sqr, norm_ref[0:1], norm_ref[1:2], groups, count, coef, 0.5)
        conv(x_ref, 0)

        @pl.loop(0, tokens // 64)
        def _(idx):
            rows = pl.ds(pl.multiple_of(idx * 64, 64), 64)
            mid[rows, :] = (acc[rows, :] + time_ref[0:1]).astype(BF16)

        tot, sqr = channel_sums(mid, tokens, chans)
        group_affine(tot, sqr, norm_ref[2:3], norm_ref[3:4], groups, count, coef, 0.5)
        conv(mid, 1)

        @pl.loop(0, tokens // 64)
        def _(idx):
            rows = pl.ds(pl.multiple_of(idx * 64, 64), 64)
            out_ref[rows, :] = (x_ref[rows, :].astype(F32) + acc[rows, :]).astype(BF16)

    flops = 2 * 2 * 9 * tokens * chans * chans
    vmem = pl.BlockSpec(memory_space=pltpu.VMEM)
    return pl.pallas_call(
        kernel,
        out_shape=jax.ShapeDtypeStruct(hidden.shape, BF16),
        in_specs=[vmem, pl.BlockSpec(memory_space=pl.ANY), vmem, vmem],
        out_specs=vmem,
        scratch_shapes=[
            pltpu.VMEM((tokens, chans), F32),
            pltpu.VMEM((tokens, chans), BF16),
            pltpu.VMEM((2, tokens + 2 * width, 3 * CK), BF16),
            pltpu.VMEM((2, 3, 3 * CK, chans), BF16),
            pltpu.VMEM((8, chans), F32),
            pltpu.SemaphoreType.DMA((2,)),
        ],
        compiler_params=pltpu.CompilerParams(vmem_limit_bytes=VMEM_LIMIT),
        cost_estimate=pl.CostEstimate(flops=flops, bytes_accessed=2 * 9 * chans * chans * 2, transcendentals=0),
        name='res_block',
    )(hidden, res_conv, norms, time_proj)


def transformer(hidden, context, norms, proj_inout, qkv_t, self_out, cross_q_t, cross_kv_t, cross_out, ff_in, ff_out, groups, heads, text):
    tokens, chans = hidden.shape
    text_rows, text_dim = context.shape
    head_dim = chans // heads
    pairs = heads // 2
    pair = 2 * head_dim
    count = float(tokens * (chans // groups))
    tiles = tokens // TM
    ff_steps = ff_out.shape[0] // chans
    ctx_half = text_dim // 2
    qw = 512 if chans >= 1024 else 256
    kb = 256
    scale = head_dim ** -0.5
    half = chans // 2

    def kernel(h_ref, ctx_ref, norm_ref, pio, wqkv, wo, cq, ckv, co, f1, f2, out_ref,
               ring, tok, aux, q_t, keys, v_t, acc, ctx_k, ctx_v, coef, rsem):
        units = {
            'in': (pio.at[0], 0, 0), 'q': (wqkv.at[0], 0, 1), 'k': (wqkv.at[1], 1, 0), 'v': (wqkv.at[2], 1, 1),
            'ck0': (ckv.at[0, :, 0:ctx_half], 1, 2), 'ck1': (ckv.at[0, :, ctx_half:text_dim], 0, 2),
            'cv0': (ckv.at[1, :, 0:ctx_half], 0, 0), 'cv1': (ckv.at[1, :, ctx_half:text_dim], 0, 1),
            'o': (wo, 1, 0), 'cq': (cq, 1, 1), 'co': (co, 1, 2), 'out': (pio.at[1], 0, 0),
        }

        def spot(group, place, wide):
            return ring.at[group, place] if wide == chans else ring.at[group, place, :, 0:wide]

        def copy_of(name):
            src, group, place = units[name]
            return pltpu.make_async_copy(src, spot(group, place, src.shape[1]), rsem.at[group, place])

        def start(*names):
            for name in names:
                copy_of(name).start()

        def take(name):
            copy_of(name).wait()
            src, group, place = units[name]
            return spot(group, place, src.shape[1])

        def ff_copies(step, group):
            cols = pl.multiple_of(step * chans, chans)
            return [
                pltpu.make_async_copy(f1.at[:, pl.ds(cols, chans)], ring.at[group, 0], rsem.at[group, 0]),
                pltpu.make_async_copy(f1.at[:, pl.ds(cols + ff_steps * chans, chans)], ring.at[group, 1], rsem.at[group, 1]),
                pltpu.make_async_copy(f2.at[pl.ds(cols, chans), :], ring.at[group, 2], rsem.at[group, 2]),
            ]

        start('in', 'q', 'k', 'v', 'ck0', 'ck1')

        def tile_rows(tile):
            return pl.ds(pl.multiple_of(tile * TM, TM), TM)

        tot, sqr = channel_sums(h_ref, tokens, chans)
        group_affine(tot, sqr, norm_ref[0:1], norm_ref[1:2], groups, count, coef, 1.0)

        def project_rows(weight, src, base, normed_to):
            def norm_tile(tile):
                rows = tile_rows(tile)
                normed_to[rows, :] = layer_norm(tok[rows, :].astype(F32))

            @pl.loop(0, tiles)
            def _(tile):
                norm_tile(jnp.maximum(tile - 1, 0))
                rows = tile_rows(tile)
                tok[rows, :] = (base(rows) + nn(src(rows), weight[...])).astype(BF16)

            norm_tile(tiles - 1)

        project_rows(take('in'), lambda rows: (h_ref[rows, :].astype(F32) * coef[0:1] + coef[1:2]).astype(BF16), lambda rows: 0.0, aux)
        start('cv0')

        def transposed(weight, src, dst, factor):
            @pl.loop(0, 2)
            def _(part):
                rows = pl.ds(pl.multiple_of(part * half, half), half)
                dst[rows, :] = (nt(weight[rows, :], src[...]).astype(BF16) * factor).astype(BF16) if factor != 1.0 else nt(weight[rows, :], src[...]).astype(BF16)

        transposed(take('q'), aux, q_t, scale)
        start('cv1')
        w_key = take('k')

        @pl.loop(0, tokens // 512)
        def _(part):
            rows = pl.ds(pl.multiple_of(part * 512, 512), 512)
            keys[rows, :] = nt(aux[rows, :], w_key[...]).astype(BF16)
        start('o')
        transposed(take('v'), aux, v_t, 1.0)
        start('cq')
        w_ck = take('ck0'), take('ck1')
        ctx_k[...] = (nt(ctx_ref[:, 0:ctx_half], w_ck[0][...]) + nt(ctx_ref[:, ctx_half:text_dim], w_ck[1][...])).astype(BF16)
        start('co')
        w_cv = take('cv0'), take('cv1')

        @pl.loop(0, chans // 256)
        def _(part):
            rows = pl.ds(pl.multiple_of(part * 256, 256), 256)
            ctx_v[rows, :] = (nt(w_cv[0][rows, :], ctx_ref[:, 0:ctx_half]) + nt(w_cv[1][rows, :], ctx_ref[:, ctx_half:text_dim])).astype(BF16)

        for copy in ff_copies(0, 0):
            copy.start()

        row_head = lax.broadcasted_iota(jnp.int32, (pair, 1), 0) < head_dim

        def query_of(hp, first, wide, head):
            both = q_t[pl.ds(pl.multiple_of(hp * pair, pair), pair), pl.ds(first, wide)]
            keep = row_head if head == 0 else jnp.logical_not(row_head)
            return jnp.where(keep, both, jnp.zeros_like(both))

        def pair_cols(hp):
            return pl.ds(pl.multiple_of(hp * pair, pair), pair)

        halves = tokens // qw
        blocks = pairs * halves
        scores = [acc.at[:, pl.ds(h * qw, qw)] for h in range(2)]
        probs = [out_ref.at[:, pl.ds(h * qw, qw)] for h in range(2)]
        parts = tokens // kb

        def place(block):
            hp = lax.div(block, halves)
            return hp, pl.multiple_of((block - hp * halves) * qw, qw)

        def fold(vals, func):
            return func(vals.reshape(-1, 8, vals.shape[-1]), axis=0)

        def score_part(block, head, part):
            hp, first = place(block)
            query = query_of(hp, first, qw, head)
            vals = nn(keys[part * kb:(part + 1) * kb, pair_cols(hp)], query)
            scores[head][part * kb:(part + 1) * kb, :] = vals
            return fold(vals, jnp.max)

        def exp_part(head, part, top):
            vals = jnp.exp(scores[head][part * kb:(part + 1) * kb, :] - top)
            probs[head][part * kb:(part + 1) * kb, :] = vals.astype(BF16)
            return fold(vals, jnp.sum)

        def value_of(block, head, denom):
            hp, _ = place(block)
            vals = v_t[pl.ds(pl.multiple_of(hp * pair + head * head_dim, head_dim), head_dim), :]
            return nn(vals, probs[head][...]) / denom

        def softmax_stage(score_block, score_head, exp_head, top):
            tops, sums = [], []
            for part in range(parts):
                tops.append(score_part(score_block, score_head, part))
                sums.append(exp_part(exp_head, part, top))
            new_top = jnp.max(functools.reduce(jnp.maximum, tops), axis=0, keepdims=True)
            return new_top, jnp.sum(functools.reduce(jnp.add, sums), axis=0, keepdims=True)

        def emit(block, low, high):
            hp, first = place(block)
            aux[pl.ds(first, qw), pair_cols(hp)] = jnp.concatenate([low, high], axis=0).T.astype(BF16)

        top_first = jnp.max(functools.reduce(jnp.maximum, [score_part(0, 0, part) for part in range(parts)]), axis=0, keepdims=True)
        zero_row = jnp.ones((1, qw), F32)
        zero_out = jnp.zeros((head_dim, qw), F32)

        def attend_block(block, carry):
            top0, denom1, low = carry
            before = jnp.maximum(block - 1, 0)
            high = value_of(before, 1, denom1)
            emit(before, low, high)
            top1, denom0 = softmax_stage(block, 1, 0, top0)
            after = jnp.minimum(block + 1, blocks - 1)
            low = value_of(block, 0, denom0)
            top0, denom1 = softmax_stage(after, 0, 1, top1)
            return top0, denom1, low

        _, denom1, low = lax.fori_loop(0, blocks, attend_block, (top_first, zero_row, zero_out))
        emit(blocks - 1, low, value_of(blocks - 1, 1, denom1))

        project_rows(take('o'), lambda rows: aux[rows, :], lambda rows: tok[rows, :].astype(F32), keys)
        transposed(take('cq'), keys, q_t, scale)

        text_valid = lax.broadcasted_iota(jnp.int32, (text_rows, 1), 0) < text

        @pl.loop(0, pairs // 2)
        def _(step):
            for sub in range(2):
                hp = step * 2 + sub
                outs = []
                for head in range(2):
                    vals = nn(ctx_k[:, pair_cols(hp)], query_of(hp, 0, tokens, head))
                    vals = jnp.where(text_valid, vals, -jnp.inf)
                    weights = jnp.exp(vals - jnp.max(vals, axis=0, keepdims=True))
                    denom = jnp.sum(weights, axis=0, keepdims=True)
                    text_vals = ctx_v[pl.ds(pl.multiple_of(hp * pair + head * head_dim, head_dim), head_dim), :]
                    outs.append(nn(text_vals, weights.astype(BF16)) / denom)
                aux[:, pair_cols(hp)] = jnp.concatenate(outs, axis=0).T.astype(BF16)

        project_rows(take('co'), lambda rows: aux[rows, :], lambda rows: tok[rows, :].astype(F32), keys)
        for copy in ff_copies(1, 1):
            copy.start()
        acc[...] = jnp.zeros_like(acc)

        @pl.loop(0, ff_steps)
        def _(step):
            group = lax.rem(step, 2)
            for copy in ff_copies(step, group):
                copy.wait()

            @pl.loop(0, tiles)
            def _(tile):
                rows = tile_rows(tile)
                src = keys[rows, :]
                value = nn(src, ring[group, 0])
                gate = nn(src, ring[group, 1])
                gated = (value * (0.5 * gate * (1.0 + lax.erf(gate * (0.5 ** 0.5))))).astype(BF16)
                acc[rows, :] += nn(gated, ring[group, 2])

            @pl.when(step + 2 < ff_steps)
            def _():
                for copy in ff_copies(step + 2, group):
                    copy.start()

            @pl.when(step == ff_steps - 2)
            def _():
                start('out')

        w_fin = take('out')

        @pl.loop(0, tiles)
        def _(tile):
            rows = tile_rows(tile)
            t = (tok[rows, :].astype(F32) + acc[rows, :]).astype(BF16)
            out_ref[rows, :] = (h_ref[rows, :].astype(F32) + nn(t, w_fin[...])).astype(BF16)

    vmem = pl.BlockSpec(memory_space=pltpu.VMEM)
    hbm = pl.BlockSpec(memory_space=pl.ANY)
    flops = 2 * tokens * chans * chans * (8 + 3 * ff_steps) + 4 * tokens * tokens * chans
    return pl.pallas_call(
        kernel,
        out_shape=jax.ShapeDtypeStruct(hidden.shape, BF16),
        in_specs=[vmem, vmem, vmem] + [hbm] * 8,
        out_specs=vmem,
        scratch_shapes=[
            pltpu.VMEM((2, 3, chans, chans), BF16),
            pltpu.VMEM((tokens, chans), BF16),
            pltpu.VMEM((tokens, chans), BF16),
            pltpu.VMEM((chans, tokens), BF16),
            pltpu.VMEM((tokens, chans), BF16),
            pltpu.VMEM((chans, tokens), BF16),
            pltpu.VMEM((tokens, chans), F32),
            pltpu.VMEM((text_rows, chans), BF16),
            pltpu.VMEM((chans, text_rows), BF16),
            pltpu.VMEM((8, chans), F32),
            pltpu.SemaphoreType.DMA((2, 3)),
        ],
        compiler_params=pltpu.CompilerParams(vmem_limit_bytes=VMEM_LIMIT),
        cost_estimate=pl.CostEstimate(flops=flops, bytes_accessed=80_000_000, transcendentals=tokens * tokens * heads),
        name='transformer',
    )(hidden, context, norms, proj_inout, qkv_t, self_out, cross_q_t, cross_kv_t, cross_out, ff_in, ff_out)


def solution(mesh):
    num_bands = mesh.shape['sp']

    def local_stage(latent, time_emb, context, res_conv, res_time, res_norm, attn_norm, proj_inout, self_qkv, self_out, cross_q, cross_kv, cross_out, ff_in, ff_out):
        images, band_rows, width, chans = latent.shape
        assert images == num_bands
        band = band_rows * width
        heads, head_dim = self_out.shape[:2]
        groups = res_norm.shape[3]
        text, text_dim = context.shape[1:]
        me = lax.axis_index('sp')

        image = exchange(latent.reshape(images, band, chans), 0).reshape(images * band, chans)
        time_row = lax.dynamic_slice_in_dim(time_emb, me, 1, 0)
        time_act = jax.nn.silu(time_row.astype(F32)).astype(BF16)
        time_proj = jnp.einsum('tc,bcd->btd', time_act, res_time, preferred_element_type=F32)
        norms = res_norm.astype(F32).reshape(2, 4, chans)
        ctx_rows = -(-text // 16) * 16
        ctx = lax.dynamic_index_in_dim(context, me, 0, keepdims=False)
        ctx = jnp.pad(ctx, ((0, ctx_rows - text), (0, 0)))

        first = res_block(image, res_conv, norms[0], time_proj[0], 0, width, groups)
        middle = transformer(
            first, ctx, attn_norm.astype(F32).reshape(2, chans), proj_inout,
            jnp.transpose(self_qkv, (0, 2, 3, 1)).reshape(3, chans, chans),
            self_out.reshape(chans, chans),
            jnp.transpose(cross_q, (1, 2, 0)).reshape(chans, chans),
            jnp.transpose(cross_kv, (0, 2, 3, 1)).reshape(2, chans, text_dim),
            cross_out.reshape(chans, chans), ff_in, ff_out, groups, heads, text)
        last = res_block(middle, res_conv, norms[1], time_proj[1], 1, width, groups)
        out = exchange(last.reshape(num_bands, band, chans), 1)
        return out.reshape(latent.shape)

    band_spec = P('dp', 'sp', None, None)
    shared = P()
    in_specs = (band_spec, P('dp', None), P('dp', None, None)) + (shared,) * 12
    return jax.shard_map(local_stage, mesh=mesh, in_specs=in_specs, out_specs=band_spec, check_vma=False)
```

```python
import functools

import jax
import jax.numpy as jnp
from jax import lax
from jax.experimental import pallas as pl
from jax.experimental.pallas import tpu as pltpu
from jax.sharding import PartitionSpec as P

BF16 = jnp.bfloat16
F32 = jnp.float32
MESH = pl.DeviceIdType.MESH
GN_EPS = 1e-6
LN_EPS = 1e-5
TM = 256
CK = 256
VMEM_LIMIT = 67_000_000


def nn(lhs, rhs):
    return lax.dot_general(lhs, rhs, (((1,), (0,)), ((), ())), preferred_element_type=F32)


def nt(lhs, rhs):
    return lax.dot_general(lhs, rhs, (((1,), (1,)), ((), ())), preferred_element_type=F32)


def split3(vals):
    high = vals.astype(BF16).astype(F32)
    rest = vals - high
    mid = rest.astype(BF16).astype(F32)
    return [high, mid, rest - mid]


def channel_sums(src, rows, chans):
    def step(idx, carry):
        tot, sqr = carry
        vals = src[pl.ds(pl.multiple_of(idx * 64, 64), 64), :].astype(F32).reshape(8, 8, chans)
        return tot + jnp.sum(vals, axis=0), sqr + jnp.sum(vals * vals, axis=0)

    zero = jnp.zeros((8, chans), F32)
    return lax.fori_loop(0, rows // 64, step, (zero, zero))


def group_affine(tot, sqr, gain, shift, groups, count, coef, factor):
    chans = tot.shape[1]
    width = chans // groups
    terms = split3(jnp.sum(tot, axis=0, keepdims=True)) + split3(jnp.sum(sqr, axis=0, keepdims=True))
    rows = jnp.concatenate(terms + [jnp.zeros((2, chans), F32)], axis=0).astype(BF16)
    chan = lax.broadcasted_iota(jnp.int32, (chans, 128), 0)
    low = lax.broadcasted_iota(jnp.int32, (chans, 128), 1) * width
    member = jnp.where((chan >= low) & (chan < low + width), 1.0, 0.0).astype(BF16)
    sums = nn(rows, member)
    mean = (sums[0:1] + sums[1:2] + sums[2:3]) / count
    msq = (sums[3:4] + sums[4:5] + sums[5:6]) / count
    rstd = lax.rsqrt(msq - mean * mean + GN_EPS)
    back = jnp.concatenate(split3(mean) + split3(rstd) + [jnp.zeros((2, 128), F32)], axis=0).astype(BF16)
    wide = nt(back, member)
    scale = (wide[3:4] + wide[4:5] + wide[5:6]) * gain
    coef[0:1, :] = factor * scale
    coef[1:2, :] = factor * (shift - (wide[0:1] + wide[1:2] + wide[2:3]) * scale)


def layer_norm(tokens):
    centred = tokens - jnp.mean(tokens, axis=-1, keepdims=True)
    return (centred * lax.rsqrt(jnp.mean(centred * centred, axis=-1, keepdims=True) + LN_EPS)).astype(BF16)


def meet(peers, me):
    barrier = pltpu.get_barrier_semaphore()

    @pl.loop(1, peers)
    def _(step):
        pl.semaphore_signal(barrier, inc=1, device_id={'sp': lax.rem(me + step, peers)}, device_id_type=MESH)


def await_peers(peers):
    pl.semaphore_wait(pltpu.get_barrier_semaphore(), peers - 1)


def drain(ref, sem):
    pltpu.make_async_copy(ref, ref, sem).wait()


def chunk_cols(chunk):
    return pl.ds(pl.multiple_of(chunk * CK, CK), CK)


def tile_rows(tile):
    return pl.ds(pl.multiple_of(tile * TM, TM), TM)


def activate(src, act, coef, chunk, tile, width):
    cols = chunk_cols(chunk)
    half = src[tile_rows(tile), cols].astype(F32) * coef[0:1, cols] + coef[1:2, cols]
    vals = half + half * jnp.tanh(half)
    column = lax.rem(lax.broadcasted_iota(jnp.int32, (TM, CK), 0), width)
    put = pl.ds(pl.multiple_of(tile * TM + width, width), TM)
    act[0, put, cols] = jnp.where(column == 0, 0.0, pltpu.roll(vals, 1, 0)).astype(BF16)
    act[1, put, cols] = vals.astype(BF16)
    act[2, put, cols] = jnp.where(column == width - 1, 0.0, pltpu.roll(vals, TM - 1, 0)).astype(BF16)


def clear_edges(act, tokens, width):
    edge = jnp.zeros((width, act.shape[2]), BF16)
    for shift in range(3):
        act[shift, 0:width, :] = edge
        act[shift, width + tokens:2 * width + tokens, :] = edge


def shifted(act, shift, tile, row, width, cols):
    return act[shift, pl.ds(pl.multiple_of(tile * TM + row * width, width), TM), cols]


def fetch_rows(kern, which, conv, chunk, wbuf, slot, sem):
    return [pltpu.make_async_copy(kern.at[which, conv, dy, dx, chunk_cols(chunk), :], wbuf.at[slot, dy, pl.ds(dx * CK, CK), :], sem.at[slot])
            for dy in range(3) for dx in range(3)]


def fetch_cols(kern, which, conv, chunk, wbuf, slot, sem):
    return [pltpu.make_async_copy(kern.at[which, conv, dy, dx, :, chunk_cols(chunk)], wbuf.at[slot, 3 * dy + dx], sem.at[slot])
            for dy in range(3) for dx in range(3)]


def rows_product(act, wbuf, slot, chunk, tile, width):
    cols = chunk_cols(chunk)
    part = None
    for dy in range(3):
        for dx in range(3):
            term = nn(shifted(act, dx, tile, dy, width, cols), wbuf[slot, dy, dx * CK:(dx + 1) * CK, :])
            part = term if part is None else part + term
    return part


def conv_rows(kern, which, conv, src, act, wbuf, wsem, coef, acc, tokens, width, ready):
    tiles = tokens // TM
    chunks = act.shape[2] // CK
    acc[...] = jnp.zeros_like(acc)
    if ready is None:
        @pl.loop(0, tiles)
        def _(tile):
            activate(src, act, coef, 0, tile, width)

    @pl.loop(0, chunks)
    def _(chunk):
        slot = lax.rem(chunk, 2)

        @pl.when(chunk + 1 < chunks)
        def _():
            for copy in fetch_rows(kern, which, conv, chunk + 1, wbuf, 1 - slot, wsem):
                copy.start()

        for copy in fetch_rows(kern, which, conv, chunk, wbuf, slot, wsem):
            copy.wait()
        if ready is not None:
            ready(chunk)

            @pl.loop(0, tiles)
            def _(tile):
                activate(src, act, coef, chunk, tile, width)

        @pl.loop(0, tiles)
        def _(tile):
            acc[tile_rows(tile), :] += rows_product(act, wbuf, slot, chunk, tile, width)
            if ready is None:
                activate(src, act, coef, lax.rem(chunk + 1, chunks), tile, width)


def add_rows(dst, src, other):
    @pl.loop(0, src.shape[0] // 64)
    def _(idx):
        rows = pl.ds(pl.multiple_of(idx * 64, 64), 64)
        dst[rows, :] = (src[rows, :] + (other[0:1, :] if other.shape[0] == 1 else other[rows, :]).astype(F32)).astype(BF16)


def res_block_in(latent, res_conv, norms, time_proj, which, width, groups):
    peers, band, chans = latent.shape
    tokens = peers * band
    chunks = chans // CK
    count = float(tokens * (chans // groups))

    def kernel(lat, kern, norm_ref, time_ref, out_ref, own, image, mid, act, wbuf, acc, mine, stats, coef, wsem, own_sem, send_sem, recv_sem, stat_send, stat_recv):
        me = lax.axis_index('sp')
        load = pltpu.make_async_copy(lat, own, own_sem)
        load.start()
        for copy in fetch_rows(kern, which, 0, 0, wbuf, 0, wsem):
            copy.start()
        meet(peers, me)
        clear_edges(act, tokens, width)
        load.wait()

        @pl.loop(0, peers)
        def _(peer):
            vals = own[peer].astype(F32)
            mine[peer, 0:1, :] = jnp.sum(vals, axis=0, keepdims=True)
            mine[peer, 1:2, :] = jnp.sum(vals * vals, axis=0, keepdims=True)

        await_peers(peers)

        def peer_of(step):
            return lax.rem(me + step, peers)

        @pl.loop(1, peers)
        def _(step):
            peer = peer_of(step)
            pltpu.make_async_remote_copy(mine.at[peer], stats.at[me], stat_send, stat_recv, device_id={'sp': peer}, device_id_type=MESH).start()

        for chunk in range(chunks):
            @pl.loop(1, peers)
            def _(step):
                peer = peer_of(step)
                cols = pl.ds(chunk * CK, CK)
                pltpu.make_async_remote_copy(
                    own.at[peer, :, cols], image.at[pl.ds(pl.multiple_of(me * band, band), band), cols], send_sem.at[chunk], recv_sem.at[chunk],
                    device_id={'sp': peer}, device_id_type=MESH).start()

        image[pl.ds(pl.multiple_of(me * band, band), band), :] = own[me]
        stats[me] = mine[me]
        others = pl.ds(0, tokens - band)
        drain(stats.at[pl.ds(0, peers - 1)], stat_recv)
        tot, sqr = stats[0, 0:1, :], stats[0, 1:2, :]
        for peer in range(1, peers):
            tot, sqr = tot + stats[peer, 0:1, :], sqr + stats[peer, 1:2, :]
        group_affine(tot, sqr, norm_ref[0:1], norm_ref[1:2], groups, count, coef, 0.5)
        conv_rows(kern, which, 0, image, act, wbuf, wsem, coef, acc, tokens, width,
                  lambda chunk: drain(image.at[others, chunk_cols(chunk)], recv_sem.at[chunk]))
        for copy in fetch_rows(kern, which, 1, 0, wbuf, 0, wsem):
            copy.start()
        add_rows(mid, acc, time_ref)
        tot, sqr = channel_sums(mid, tokens, chans)
        group_affine(tot, sqr, norm_ref[2:3], norm_ref[3:4], groups, count, coef, 0.5)
        conv_rows(kern, which, 1, mid, act, wbuf, wsem, coef, acc, tokens, width, None)
        add_rows(out_ref, acc, image)
        drain(stats.at[pl.ds(0, peers - 1)], stat_send)
        for chunk in range(chunks):
            drain(image.at[others, chunk_cols(chunk)], send_sem.at[chunk])

    vmem = pl.BlockSpec(memory_space=pltpu.VMEM)
    hbm = pl.BlockSpec(memory_space=pl.ANY)
    return pl.pallas_call(
        kernel,
        out_shape=jax.ShapeDtypeStruct((tokens, chans), BF16),
        in_specs=[hbm, hbm, vmem, vmem],
        out_specs=vmem,
        scratch_shapes=[
            pltpu.VMEM(latent.shape, BF16),
            pltpu.VMEM((tokens, chans), BF16),
            pltpu.VMEM((tokens, chans), BF16),
            pltpu.VMEM((3, tokens + 2 * width, chans), BF16),
            pltpu.VMEM((2, 3, 3 * CK, chans), BF16),
            pltpu.VMEM((tokens, chans), F32),
            pltpu.VMEM((peers, 2, chans), F32),
            pltpu.VMEM((peers, 2, chans), F32),
            pltpu.VMEM((8, chans), F32),
            pltpu.SemaphoreType.DMA((2,)),
            pltpu.SemaphoreType.DMA,
            pltpu.SemaphoreType.DMA((chunks,)),
            pltpu.SemaphoreType.DMA((chunks,)),
            pltpu.SemaphoreType.DMA,
            pltpu.SemaphoreType.DMA,
        ],
        compiler_params=pltpu.CompilerParams(vmem_limit_bytes=VMEM_LIMIT, collective_id=0, has_side_effects=True),
        cost_estimate=pl.CostEstimate(flops=36 * tokens * chans * chans, bytes_accessed=36 * chans * chans, transcendentals=0),
        name='res_block_in',
    )(latent, res_conv, norms, time_proj)


def res_block_out(hidden, res_conv, norms, time_proj, which, width, groups, peers):
    tokens, chans = hidden.shape
    band = tokens // peers
    chunks = chans // CK
    tiles = tokens // TM
    per_tile = TM // band
    count = float(tokens * (chans // groups))

    def kernel(x_ref, kern, norm_ref, time_ref, out_ref, mid, act, wbuf, cbuf, acc, result, coef, wsem, csem, own_sem, send_sem, recv_sem):
        me = lax.axis_index('sp')
        for copy in fetch_rows(kern, which, 0, 0, wbuf, 0, wsem):
            copy.start()
        meet(peers, me)
        clear_edges(act, tokens, width)
        tot, sqr = channel_sums(x_ref, tokens, chans)
        group_affine(tot, sqr, norm_ref[0:1], norm_ref[1:2], groups, count, coef, 0.5)
        conv_rows(kern, which, 0, x_ref, act, wbuf, wsem, coef, acc, tokens, width, None)
        for copy in fetch_cols(kern, which, 1, 0, cbuf, 0, csem):
            copy.start()
        add_rows(mid, acc, time_ref)
        tot, sqr = channel_sums(mid, tokens, chans)
        group_affine(tot, sqr, norm_ref[2:3], norm_ref[3:4], groups, count, coef, 0.5)

        @pl.loop(0, chunks)
        def _(chunk):
            @pl.loop(0, tiles)
            def _(tile):
                activate(mid, act, coef, chunk, tile, width)

        await_peers(peers)
        turn = lax.div(me, per_tile) + tiles // 2

        @pl.loop(0, chunks)
        def _(chunk):
            slot = lax.rem(chunk, 2)
            cols = chunk_cols(chunk)

            @pl.when(chunk + 1 < chunks)
            def _():
                for copy in fetch_cols(kern, which, 1, chunk + 1, cbuf, 1 - slot, csem):
                    copy.start()

            for copy in fetch_cols(kern, which, 1, chunk, cbuf, slot, csem):
                copy.wait()

            @pl.loop(0, tiles)
            def _(step):
                tile = lax.rem(step + turn, tiles)
                part = None
                for dy in range(3):
                    for dx in range(3):
                        term = nn(shifted(act, dx, tile, dy, width, slice(None)), cbuf[slot, 3 * dy + dx])
                        part = term if part is None else part + term
                rows = tile_rows(tile)
                result[rows, cols] = (x_ref[rows, cols].astype(F32) + part).astype(BF16)
                for idx in range(per_tile):
                    peer = tile * per_tile + idx
                    block = result.at[pl.ds(pl.multiple_of(peer * band, band), band), cols]

                    @pl.when(peer == me)
                    def _():
                        pltpu.make_async_copy(block, out_ref.at[me, :, cols], own_sem).start()

                    @pl.when(peer != me)
                    def _():
                        pltpu.make_async_remote_copy(block, out_ref.at[me, :, cols], send_sem, recv_sem, device_id={'sp': peer}, device_id_type=MESH).start()

        pltpu.make_async_copy(result.at[pl.ds(0, band), :], out_ref.at[me], own_sem).wait()
        drain(result.at[pl.ds(0, tokens - band), :], send_sem)
        drain(out_ref.at[pl.ds(0, peers - 1)], recv_sem)

    vmem = pl.BlockSpec(memory_space=pltpu.VMEM)
    hbm = pl.BlockSpec(memory_space=pl.ANY)
    return pl.pallas_call(
        kernel,
        out_shape=jax.ShapeDtypeStruct((peers, band, chans), BF16),
        in_specs=[vmem, hbm, vmem, vmem],
        out_specs=hbm,
        scratch_shapes=[
            pltpu.VMEM((tokens, chans), BF16),
            pltpu.VMEM((3, tokens + 2 * width, chans), BF16),
            pltpu.VMEM((2, 3, 3 * CK, chans), BF16),
            pltpu.VMEM((2, 9, chans, CK), BF16),
            pltpu.VMEM((tokens, chans), F32),
            pltpu.VMEM((tokens, chans), BF16),
            pltpu.VMEM((8, chans), F32),
            pltpu.SemaphoreType.DMA((2,)),
            pltpu.SemaphoreType.DMA((2,)),
            pltpu.SemaphoreType.DMA,
            pltpu.SemaphoreType.DMA,
            pltpu.SemaphoreType.DMA,
        ],
        compiler_params=pltpu.CompilerParams(vmem_limit_bytes=VMEM_LIMIT, collective_id=1, has_side_effects=True),
        cost_estimate=pl.CostEstimate(flops=36 * tokens * chans * chans, bytes_accessed=36 * chans * chans, transcendentals=0),
        name='res_block_out',
    )(hidden, res_conv, norms, time_proj)


def transformer(hidden, context, norms, proj_inout, qkv_t, self_out, cross_q_t, cross_kv_t, cross_out, ff_in, ff_out, groups, heads, text):
    tokens, chans = hidden.shape
    text_rows, text_dim = context.shape
    head_dim = chans // heads
    pairs = heads // 2
    pair = 2 * head_dim
    count = float(tokens * (chans // groups))
    tiles = tokens // TM
    ff_steps = ff_out.shape[0] // chans
    ctx_half = text_dim // 2
    qw = 512 if chans >= 1024 else 256
    kb = 256
    scale = head_dim ** -0.5
    half = chans // 2

    def kernel(h_ref, ctx_ref, norm_ref, pio, wqkv, wo, cq, ckv, co, f1, f2, out_ref,
               ring, tok, aux, q_t, keys, v_t, acc, ctx_k, ctx_v, coef, rsem):
        units = {
            'in': (pio.at[0], 0, 0), 'q': (wqkv.at[0], 0, 1), 'k': (wqkv.at[1], 1, 0), 'v': (wqkv.at[2], 1, 1),
            'ck0': (ckv.at[0, :, 0:ctx_half], 1, 2), 'ck1': (ckv.at[0, :, ctx_half:text_dim], 0, 2),
            'cv0': (ckv.at[1, :, 0:ctx_half], 0, 0), 'cv1': (ckv.at[1, :, ctx_half:text_dim], 0, 1),
            'o': (wo, 1, 0), 'cq': (cq, 1, 1), 'co': (co, 1, 2), 'out': (pio.at[1], 0, 0),
        }

        def spot(group, place, wide):
            return ring.at[group, place] if wide == chans else ring.at[group, place, :, 0:wide]

        def copy_of(name):
            src, group, place = units[name]
            return pltpu.make_async_copy(src, spot(group, place, src.shape[1]), rsem.at[group, place])

        def start(*names):
            for name in names:
                copy_of(name).start()

        def take(name):
            copy_of(name).wait()
            src, group, place = units[name]
            return spot(group, place, src.shape[1])

        def ff_copies(step, group):
            cols = pl.multiple_of(step * chans, chans)
            return [
                pltpu.make_async_copy(f1.at[:, pl.ds(cols, chans)], ring.at[group, 0], rsem.at[group, 0]),
                pltpu.make_async_copy(f1.at[:, pl.ds(cols + ff_steps * chans, chans)], ring.at[group, 1], rsem.at[group, 1]),
                pltpu.make_async_copy(f2.at[pl.ds(cols, chans), :], ring.at[group, 2], rsem.at[group, 2]),
            ]

        start('in', 'q', 'k', 'v', 'ck0', 'ck1')

        tot, sqr = channel_sums(h_ref, tokens, chans)
        group_affine(tot, sqr, norm_ref[0:1], norm_ref[1:2], groups, count, coef, 1.0)

        def project_rows(weight, src, base, normed_to):
            def norm_tile(tile):
                rows = tile_rows(tile)
                normed_to[rows, :] = layer_norm(tok[rows, :].astype(F32))

            @pl.loop(0, tiles)
            def _(tile):
                norm_tile(jnp.maximum(tile - 1, 0))
                rows = tile_rows(tile)
                tok[rows, :] = (base(rows) + nn(src(rows), weight[...])).astype(BF16)

            norm_tile(tiles - 1)

        project_rows(take('in'), lambda rows: (h_ref[rows, :].astype(F32) * coef[0:1] + coef[1:2]).astype(BF16), lambda rows: 0.0, aux)
        start('cv0')

        def transposed(weight, src, dst, factor):
            @pl.loop(0, 2)
            def _(part):
                rows = pl.ds(pl.multiple_of(part * half, half), half)
                dst[rows, :] = (nt(weight[rows, :], src[...]).astype(BF16) * factor).astype(BF16) if factor != 1.0 else nt(weight[rows, :], src[...]).astype(BF16)

        transposed(take('q'), aux, q_t, scale)
        start('cv1')
        w_key = take('k')

        @pl.loop(0, tokens // 512)
        def _(part):
            rows = pl.ds(pl.multiple_of(part * 512, 512), 512)
            keys[rows, :] = nt(aux[rows, :], w_key[...]).astype(BF16)
        start('o')
        transposed(take('v'), aux, v_t, 1.0)
        start('cq')
        w_ck = take('ck0'), take('ck1')
        ctx_k[...] = (nt(ctx_ref[:, 0:ctx_half], w_ck[0][...]) + nt(ctx_ref[:, ctx_half:text_dim], w_ck[1][...])).astype(BF16)
        start('co')
        w_cv = take('cv0'), take('cv1')

        @pl.loop(0, chans // 256)
        def _(part):
            rows = pl.ds(pl.multiple_of(part * 256, 256), 256)
            ctx_v[rows, :] = (nt(w_cv[0][rows, :], ctx_ref[:, 0:ctx_half]) + nt(w_cv[1][rows, :], ctx_ref[:, ctx_half:text_dim])).astype(BF16)

        for copy in ff_copies(0, 0):
            copy.start()

        row_head = lax.broadcasted_iota(jnp.int32, (pair, 1), 0) < head_dim

        def query_of(hp, first, wide, head):
            both = q_t[pl.ds(pl.multiple_of(hp * pair, pair), pair), pl.ds(first, wide)]
            keep = row_head if head == 0 else jnp.logical_not(row_head)
            return jnp.where(keep, both, jnp.zeros_like(both))

        def pair_cols(hp):
            return pl.ds(pl.multiple_of(hp * pair, pair), pair)

        halves = tokens // qw
        blocks = pairs * halves
        scores = [acc.at[:, pl.ds(h * qw, qw)] for h in range(2)]
        probs = [out_ref.at[:, pl.ds(h * qw, qw)] for h in range(2)]
        parts = tokens // kb

        def place(block):
            hp = lax.div(block, halves)
            return hp, pl.multiple_of((block - hp * halves) * qw, qw)

        def fold(vals, func):
            return func(vals.reshape(-1, 8, vals.shape[-1]), axis=0)

        def score_part(block, head, part):
            hp, first = place(block)
            query = query_of(hp, first, qw, head)
            vals = nn(keys[part * kb:(part + 1) * kb, pair_cols(hp)], query)
            scores[head][part * kb:(part + 1) * kb, :] = vals
            return fold(vals, jnp.max)

        def exp_part(head, part, top):
            vals = jnp.exp(scores[head][part * kb:(part + 1) * kb, :] - top)
            probs[head][part * kb:(part + 1) * kb, :] = vals.astype(BF16)
            return fold(vals, jnp.sum)

        def value_of(block, head, denom):
            hp, _ = place(block)
            vals = v_t[pl.ds(pl.multiple_of(hp * pair + head * head_dim, head_dim), head_dim), :]
            return nn(vals, probs[head][...]) / denom

        def softmax_stage(score_block, score_head, exp_head, top):
            tops, sums = [], []
            for part in range(parts):
                tops.append(score_part(score_block, score_head, part))
                sums.append(exp_part(exp_head, part, top))
            new_top = jnp.max(functools.reduce(jnp.maximum, tops), axis=0, keepdims=True)
            return new_top, jnp.sum(functools.reduce(jnp.add, sums), axis=0, keepdims=True)

        def emit(block, low, high):
            hp, first = place(block)
            aux[pl.ds(first, qw), pair_cols(hp)] = jnp.concatenate([low, high], axis=0).T.astype(BF16)

        top_first = jnp.max(functools.reduce(jnp.maximum, [score_part(0, 0, part) for part in range(parts)]), axis=0, keepdims=True)
        zero_row = jnp.ones((1, qw), F32)
        zero_out = jnp.zeros((head_dim, qw), F32)

        def attend_block(block, carry):
            top0, denom1, low = carry
            before = jnp.maximum(block - 1, 0)
            high = value_of(before, 1, denom1)
            emit(before, low, high)
            top1, denom0 = softmax_stage(block, 1, 0, top0)
            after = jnp.minimum(block + 1, blocks - 1)
            low = value_of(block, 0, denom0)
            top0, denom1 = softmax_stage(after, 0, 1, top1)
            return top0, denom1, low

        _, denom1, low = lax.fori_loop(0, blocks, attend_block, (top_first, zero_row, zero_out))
        emit(blocks - 1, low, value_of(blocks - 1, 1, denom1))

        project_rows(take('o'), lambda rows: aux[rows, :], lambda rows: tok[rows, :].astype(F32), keys)
        transposed(take('cq'), keys, q_t, scale)

        text_valid = lax.broadcasted_iota(jnp.int32, (text_rows, 1), 0) < text

        @pl.loop(0, pairs // 2)
        def _(step):
            for sub in range(2):
                hp = step * 2 + sub
                outs = []
                for head in range(2):
                    vals = nn(ctx_k[:, pair_cols(hp)], query_of(hp, 0, tokens, head))
                    vals = jnp.where(text_valid, vals, -jnp.inf)
                    weights = jnp.exp(vals - jnp.max(vals, axis=0, keepdims=True))
                    denom = jnp.sum(weights, axis=0, keepdims=True)
                    text_vals = ctx_v[pl.ds(pl.multiple_of(hp * pair + head * head_dim, head_dim), head_dim), :]
                    outs.append(nn(text_vals, weights.astype(BF16)) / denom)
                aux[:, pair_cols(hp)] = jnp.concatenate(outs, axis=0).T.astype(BF16)

        project_rows(take('co'), lambda rows: aux[rows, :], lambda rows: tok[rows, :].astype(F32), keys)
        for copy in ff_copies(1, 1):
            copy.start()
        acc[...] = jnp.zeros_like(acc)

        @pl.loop(0, ff_steps)
        def _(step):
            group = lax.rem(step, 2)
            for copy in ff_copies(step, group):
                copy.wait()

            @pl.loop(0, tiles)
            def _(tile):
                rows = tile_rows(tile)
                src = keys[rows, :]
                value = nn(src, ring[group, 0])
                gate = nn(src, ring[group, 1])
                gated = (value * (0.5 * gate * (1.0 + lax.erf(gate * (0.5 ** 0.5))))).astype(BF16)
                acc[rows, :] += nn(gated, ring[group, 2])

            @pl.when(step + 2 < ff_steps)
            def _():
                for copy in ff_copies(step + 2, group):
                    copy.start()

            @pl.when(step == ff_steps - 2)
            def _():
                start('out')

        w_fin = take('out')

        @pl.loop(0, tiles)
        def _(tile):
            rows = tile_rows(tile)
            t = (tok[rows, :].astype(F32) + acc[rows, :]).astype(BF16)
            out_ref[rows, :] = (h_ref[rows, :].astype(F32) + nn(t, w_fin[...])).astype(BF16)

    vmem = pl.BlockSpec(memory_space=pltpu.VMEM)
    hbm = pl.BlockSpec(memory_space=pl.ANY)
    flops = 2 * tokens * chans * chans * (8 + 3 * ff_steps) + 4 * tokens * tokens * chans
    return pl.pallas_call(
        kernel,
        out_shape=jax.ShapeDtypeStruct(hidden.shape, BF16),
        in_specs=[vmem, vmem, vmem] + [hbm] * 8,
        out_specs=vmem,
        scratch_shapes=[
            pltpu.VMEM((2, 3, chans, chans), BF16),
            pltpu.VMEM((tokens, chans), BF16),
            pltpu.VMEM((tokens, chans), BF16),
            pltpu.VMEM((chans, tokens), BF16),
            pltpu.VMEM((tokens, chans), BF16),
            pltpu.VMEM((chans, tokens), BF16),
            pltpu.VMEM((tokens, chans), F32),
            pltpu.VMEM((text_rows, chans), BF16),
            pltpu.VMEM((chans, text_rows), BF16),
            pltpu.VMEM((8, chans), F32),
            pltpu.SemaphoreType.DMA((2, 3)),
        ],
        compiler_params=pltpu.CompilerParams(vmem_limit_bytes=VMEM_LIMIT),
        cost_estimate=pl.CostEstimate(flops=flops, bytes_accessed=80_000_000, transcendentals=tokens * tokens * heads),
        name='transformer',
    )(hidden, context, norms, proj_inout, qkv_t, self_out, cross_q_t, cross_kv_t, cross_out, ff_in, ff_out)


def solution(mesh):
    num_bands = mesh.shape['sp']

    def local_stage(latent, time_emb, context, res_conv, res_time, res_norm, attn_norm, proj_inout, self_qkv, self_out, cross_q, cross_kv, cross_out, ff_in, ff_out):
        images, band_rows, width, chans = latent.shape
        assert images == num_bands
        band = band_rows * width
        heads, head_dim = self_out.shape[:2]
        groups = res_norm.shape[3]
        text, text_dim = context.shape[1:]
        me = lax.axis_index('sp')

        time_row = lax.dynamic_slice_in_dim(time_emb, me, 1, 0)
        time_act = jax.nn.silu(time_row.astype(F32)).astype(BF16)
        time_proj = jnp.einsum('tc,bcd->btd', time_act, res_time, preferred_element_type=F32)
        norms = res_norm.astype(F32).reshape(2, 4, chans)
        ctx_rows = -(-text // 16) * 16
        ctx = lax.dynamic_index_in_dim(context, me, 0, keepdims=False)
        ctx = jnp.pad(ctx, ((0, ctx_rows - text), (0, 0)))

        first = res_block_in(latent.reshape(images, band, chans), res_conv, norms[0], time_proj[0], 0, width, groups)
        middle = transformer(
            first, ctx, attn_norm.astype(F32).reshape(2, chans), proj_inout,
            jnp.transpose(self_qkv, (0, 2, 3, 1)).reshape(3, chans, chans),
            self_out.reshape(chans, chans),
            jnp.transpose(cross_q, (1, 2, 0)).reshape(chans, chans),
            jnp.transpose(cross_kv, (0, 2, 3, 1)).reshape(2, chans, text_dim),
            cross_out.reshape(chans, chans), ff_in, ff_out, groups, heads, text)
        out = res_block_out(middle, res_conv, norms[1], time_proj[1], 1, width, groups, num_bands)
        return out.reshape(latent.shape)

    band_spec = P('dp', 'sp', None, None)
    shared = P()
    in_specs = (band_spec, P('dp', None), P('dp', None, None)) + (shared,) * 12
    return jax.shard_map(local_stage, mesh=mesh, in_specs=in_specs, out_specs=band_spec, check_vma=False)
```

```python
import functools

import jax
import jax.numpy as jnp
from jax import lax
from jax.experimental import pallas as pl
from jax.experimental.pallas import tpu as pltpu
from jax.sharding import PartitionSpec as P

BF16 = jnp.bfloat16
F32 = jnp.float32
MESH = pl.DeviceIdType.MESH
GN_EPS = 1e-6
LN_EPS = 1e-5
TM = 256
CK = 256
VMEM_LIMIT = 67_000_000


def nn(lhs, rhs):
    return lax.dot_general(lhs, rhs, (((1,), (0,)), ((), ())), preferred_element_type=F32)


def nt(lhs, rhs):
    return lax.dot_general(lhs, rhs, (((1,), (1,)), ((), ())), preferred_element_type=F32)


def split3(vals):
    high = vals.astype(BF16).astype(F32)
    rest = vals - high
    mid = rest.astype(BF16).astype(F32)
    return [high, mid, rest - mid]


def channel_sums(src, rows, chans):
    def step(idx, carry):
        tot, sqr = carry
        vals = src[pl.ds(pl.multiple_of(idx * 64, 64), 64), :].astype(F32).reshape(8, 8, chans)
        return tot + jnp.sum(vals, axis=0), sqr + jnp.sum(vals * vals, axis=0)

    zero = jnp.zeros((8, chans), F32)
    return lax.fori_loop(0, rows // 64, step, (zero, zero))


def layer_norm(tokens):
    centred = tokens - jnp.mean(tokens, axis=-1, keepdims=True)
    return (centred * lax.rsqrt(jnp.mean(centred * centred, axis=-1, keepdims=True) + LN_EPS)).astype(BF16)


def meet(peers, me):
    barrier = pltpu.get_barrier_semaphore()

    @pl.loop(1, peers)
    def _(step):
        pl.semaphore_signal(barrier, inc=1, device_id={'sp': lax.rem(me + step, peers)}, device_id_type=MESH)


def await_peers(peers):
    pl.semaphore_wait(pltpu.get_barrier_semaphore(), peers - 1)


def drain(ref, sem):
    pltpu.make_async_copy(ref, ref, sem).wait()


def remote(src, dst, send_sem, recv_sem, peer):
    return pltpu.make_async_remote_copy(src, dst, send_sem, recv_sem, device_id={'sp': peer}, device_id_type=MESH)


def chunk_cols(chunk):
    return pl.ds(pl.multiple_of(chunk * CK, CK), CK)


def tile_rows(tile, first=0):
    return pl.ds(pl.multiple_of(first + tile * TM, 32), TM)


def members(chans, groups, offset=0):
    width = chans // groups
    chan = lax.broadcasted_iota(jnp.int32, (chans, 128), 0)
    low = (lax.broadcasted_iota(jnp.int32, (chans, 128), 1) - offset) * width
    return jnp.where((chan >= low) & (chan < low + width), 1.0, 0.0).astype(BF16)


def group_sums(rows, member):
    count = rows.shape[0]
    high, mid, low = split3(rows)
    sums = nn(jnp.concatenate([high, mid, low], axis=0).astype(BF16), member)
    return sums[0:count] + sums[count:2 * count] + sums[2 * count:3 * count]


def group_affine(sums, gain, shift, member, count, coef, factor):
    mean = sums[0:1] / count
    rstd = lax.rsqrt(sums[1:2] / count - mean * mean + GN_EPS)
    back = jnp.concatenate(split3(mean) + split3(rstd) + [jnp.zeros((2, 128), F32)], axis=0).astype(BF16)
    wide = nt(back, member)
    scale = (wide[3:4] + wide[4:5] + wide[5:6]) * gain
    coef[0:1, :] = factor * scale
    coef[1:2, :] = factor * (shift - (wide[0:1] + wide[1:2] + wide[2:3]) * scale)


def two_rows(tot, sqr):
    rows = [jnp.sum(tot, axis=0, keepdims=True), jnp.sum(sqr, axis=0, keepdims=True)]
    return jnp.concatenate(rows + [jnp.zeros((6, tot.shape[1]), F32)], axis=0)


def activate(src, first, act, put, count, coef, chunk, width):
    cols = chunk_cols(chunk)
    half = src[pl.ds(pl.multiple_of(first, width), count), cols].astype(F32) * coef[0:1, cols] + coef[1:2, cols]
    vals = half + half * jnp.tanh(half)
    column = lax.rem(lax.broadcasted_iota(jnp.int32, (count, CK), 0), width)
    rows = pl.ds(pl.multiple_of(put, width), count)
    act[0, rows, cols] = jnp.where(column == 0, 0.0, pltpu.roll(vals, 1, 0)).astype(BF16)
    act[1, rows, cols] = vals.astype(BF16)
    act[2, rows, cols] = jnp.where(column == width - 1, 0.0, pltpu.roll(vals, count - 1, 0)).astype(BF16)


def clear_edges(act, width):
    edge = jnp.zeros((width, act.shape[2]), BF16)
    for shift in range(3):
        act[shift, 0:width, :] = edge
        act[shift, act.shape[1] - width:act.shape[1], :] = edge


def shifted(act, shift, tile, row, width, cols):
    return act[shift, tile_rows(tile, row * width), cols]


def fetch_rows(kern, which, conv, chunk, wbuf, sem):
    slot = lax.rem(chunk, 2)
    return [pltpu.make_async_copy(kern.at[which, conv, dy, dx, chunk_cols(chunk), :], wbuf.at[slot, dy, pl.ds(dx * CK, CK), :], sem.at[slot])
            for dy in range(3) for dx in range(3)]


def fetch_cols(kern, which, conv, chunk, wbuf, sem):
    slot = lax.rem(chunk, 2)
    return [pltpu.make_async_copy(kern.at[which, conv, dy, dx, :, chunk_cols(chunk)], wbuf.at[slot, 3 * dy + dx], sem.at[slot])
            for dy in range(3) for dx in range(3)]


def start_all(copies):
    for copy in copies:
        copy.start()


def wait_all(copies):
    for copy in copies:
        copy.wait()


def conv_rows(fetch, parts, act, wbuf, coef, acc, width, ready):
    tokens, chans = acc.shape
    tiles = tokens // TM
    chunks = chans // CK
    (src, first, put, _), (halo, halo_first, halo_put, halo_rows) = parts
    acc[...] = jnp.zeros_like(acc)

    def build_tile(chunk, tile):
        activate(src, first + tile * TM, act, put + tile * TM, TM, coef, chunk, width)

    def build_halo(chunk):
        activate(halo, halo_first, act, halo_put, halo_rows, coef, chunk, width)

    if ready is None:
        build_halo(0)

        @pl.loop(0, tiles)
        def _(tile):
            build_tile(0, tile)

    @pl.loop(0, chunks)
    def _(chunk):
        slot = lax.rem(chunk, 2)

        @pl.when(chunk + 1 < chunks)
        def _():
            start_all(fetch(chunk + 1))

        wait_all(fetch(chunk))
        if ready is None:
            build_halo(lax.rem(chunk + 1, chunks))
        else:
            ready(chunk)
            build_halo(chunk)

            @pl.loop(0, tiles)
            def _(tile):
                build_tile(chunk, tile)

        @pl.loop(0, tiles)
        def _(tile):
            cols = chunk_cols(chunk)
            part = None
            for dy in range(3):
                for dx in range(3):
                    term = nn(shifted(act, dx, tile, dy, width, cols), wbuf[slot, dy, dx * CK:(dx + 1) * CK, :])
                    part = term if part is None else part + term
            acc[tile_rows(tile), :] += part
            if ready is None:
                build_tile(lax.rem(chunk + 1, chunks), tile)


def add_rows(dst, acc, src, first):
    @pl.loop(0, acc.shape[0] // 64)
    def _(idx):
        rows = pl.ds(pl.multiple_of(idx * 64, 64), 64)
        other = src if first is None else src[pl.ds(pl.multiple_of(first + idx * 64, 32), 64), :].astype(F32)
        dst[rows, :] = (other + acc[rows, :]).astype(BF16)


def time_rows(time_ref, weight, out):
    emb = time_ref[...].astype(F32)
    act = (emb / (1.0 + jnp.exp(-emb))).astype(BF16)
    total = None
    for place, first, count in time_pieces(act.shape[1], weight.shape[1]):
        term = nn(act[:, first:first + count], weight[place, 0:count])
        total = term if total is None else total + term
    out[...] = total


def time_pieces(depth, rows):
    return [(place, first, min(rows, depth - first)) for place, first in enumerate(range(0, depth, rows))]


def time_copies(res_time, which, weight, sem):
    return [pltpu.make_async_copy(res_time.at[which, pl.ds(first, count), :], weight.at[place, pl.ds(0, count), :], sem)
            for place, first, count in time_pieces(res_time.shape[1], weight.shape[1])]


def half_places(core, half_tokens, width):
    return core * width, (1 - core) * half_tokens, width, (1 - core) * (half_tokens + width)


def middle_norm(mid, acc, time_row, halo, sums, core, partner, member, gain, shift, count, coef, send_sem, recv_sem, width):
    half_tokens, chans = acc.shape
    add_rows(mid, acc, time_row, None)
    tot, sqr = channel_sums(mid, half_tokens, chans)
    edge = remote(mid.at[pl.ds(pl.multiple_of((1 - core) * (half_tokens - width), width), width), :], halo, send_sem.at[0], recv_sem.at[0], partner)
    edge.start()
    sums[0] = group_sums(two_rows(tot, sqr), member)
    swap = remote(sums.at[0], sums.at[1], send_sem.at[1], recv_sem.at[1], partner)
    swap.start()
    swap.wait()
    group_affine(sums[0, 0:2] + sums[1, 0:2], gain, shift, member, count, coef, 0.5)
    edge.wait()


def res_block_in(latent, time_emb, res_conv, res_time, norms, which, width, groups):
    peers, band, chans = latent.shape
    chips = peers // 2
    half_tokens = chips * band
    chunks = chans // CK
    count = float(peers * band * (chans // groups))

    def kernel(lat, time_ref, kern, wtime, norm_ref, out_ref, own, image, mid, halo, act, wbuf, acc, tproj, result, mine, stats, sums, swaps, coef,
               wsem, tsem, own_sem, send_sem, side_send, recv_sem, stat_send, stat_recv, swap_send, swap_recv, done_send, done_recv):
        me = lax.axis_index('sp')
        chip, core = lax.div(me, 2), lax.rem(me, 2)
        partner = me + 1 - 2 * core
        load = pltpu.make_async_copy(lat, own, own_sem)
        load.start()
        start_all(fetch_rows(kern, which, 0, 0, wbuf, wsem))
        start_all(time_copies(wtime, which, wbuf.at[1], tsem))
        meet(peers, me)
        clear_edges(act, width)
        member = members(chans, groups)
        side = lax.div(me, chips)
        place = lax.rem(me, chips) * band
        await_peers(peers)

        def send_to(src, dst, sent, index, chunk, peer):
            @pl.when(peer == me)
            def _():
                pltpu.make_async_copy(src, dst, recv_sem.at[index, chunk]).start()

            @pl.when(peer != me)
            def _():
                remote(src, dst, sent.at[index, chunk], recv_sem.at[index, chunk], peer).start()

        def send_chunk(index, chunk):
            cols = pl.ds(chunk * CK, CK)

            @pl.loop(0, chips)
            def _(step):
                target = lax.rem(chip + step + chips // 2, chips)
                source = lat.at[index * chips + target]
                send_to(source.at[:, cols], image.at[index, pl.ds(pl.multiple_of(side * width + place, 32), band), cols], send_sem, index, chunk, 2 * target + side)

                @pl.when(me == chips - 1)
                def _():
                    send_to(source.at[pl.ds(band - width, width), cols], image.at[index, pl.ds(0, width), cols], side_send, index, chunk, 2 * target + 1)

                @pl.when(me == chips)
                def _():
                    send_to(source.at[pl.ds(0, width), cols], image.at[index, pl.ds(half_tokens, width), cols], side_send, index, chunk, 2 * target)

        def drain_sends(index, chunk):
            cols = chunk_cols(chunk)
            extra = (me == chips - 1) | (me == chips)
            inside = side == core

            @pl.when(inside)
            def _():
                drain(image.at[index, pl.ds(0, half_tokens - band), cols], send_sem.at[index, chunk])

            @pl.when(jnp.logical_not(inside))
            def _():
                drain(image.at[index, pl.ds(0, half_tokens), cols], send_sem.at[index, chunk])

            @pl.when(extra)
            def _():
                drain(image.at[index, pl.ds(0, (chips - 1) * width), cols], side_send.at[index, chunk])

        send_chunk(0, 0)
        load.wait()

        @pl.loop(0, chips)
        def _(target):
            rows = []
            for index in range(2):
                vals = own[index * chips + target].astype(F32)
                rows += [jnp.sum(vals, axis=0, keepdims=True), jnp.sum(vals * vals, axis=0, keepdims=True)]
            mine[target] = group_sums(jnp.concatenate(rows + [jnp.zeros((4, chans), F32)], axis=0), member)

        @pl.loop(1, peers)
        def _(step):
            peer = lax.rem(me + step, peers)
            remote(mine.at[lax.div(peer, 2)], stats.at[me], stat_send, stat_recv, peer).start()

        for index in range(2):
            for chunk in range(chunks):
                if (index, chunk) != (0, 0):
                    send_chunk(index, chunk)
        wait_all(time_copies(wtime, which, wbuf.at[1], tsem))
        time_rows(time_ref, wbuf.at[1], tproj)
        stats[me] = mine[chip]
        drain(stats.at[pl.ds(0, peers - 1)], stat_recv)
        drain(stats.at[pl.ds(0, peers - 1)], stat_send)
        both = jnp.sum(stats[...], axis=0)
        sums[0] = both
        sums[1] = pltpu.roll(both, 6, 0)
        half_at, halo_at, put, halo_put = half_places(core, half_tokens, width)
        norm = [norm_ref[4 * which + row:4 * which + row + 1] for row in range(4)]

        @pl.loop(0, 2)
        def _(index):
            group_affine(sums[index, 0:2], norm[0], norm[1], member, count, coef, 0.5)
            conv_rows(lambda chunk: fetch_rows(kern, which, 0, chunk, wbuf, wsem),
                      [(image.at[index], half_at, put, half_tokens), (image.at[index], halo_at, halo_put, width)],
                      act, wbuf, coef, acc, width, lambda chunk: drain(image.at[index, :, chunk_cols(chunk)], recv_sem.at[index, chunk]))
            start_all(fetch_rows(kern, which, 1, 0, wbuf, wsem))
            middle_norm(mid, acc, tproj[pl.ds(index * chips + chip, 1), :], halo.at[index], swaps.at[index], core, partner, member, norm[2], norm[3], count, coef, swap_send.at[index], swap_recv.at[index], width)
            conv_rows(lambda chunk: fetch_rows(kern, which, 1, chunk, wbuf, wsem),
                      [(mid, 0, put, half_tokens), (halo.at[index], 0, halo_put, width)], act, wbuf, coef, acc, width, None)

            @pl.when(index == 0)
            def _():
                start_all(fetch_rows(kern, which, 0, 0, wbuf, wsem))

            add_rows(result.at[index], acc, image.at[index], half_at)
            mine_rows = pl.ds(pl.multiple_of(core * half_tokens, half_tokens), half_tokens)

            @pl.when(index == core)
            def _():
                out_ref[mine_rows, :] = result[index]

            @pl.when(index != core)
            def _():
                remote(result.at[index], out_ref.at[mine_rows, :], done_send, done_recv, partner).start()

        drain(result.at[0], done_recv)
        drain(result.at[0], done_send)
        for index in range(2):
            @pl.loop(0, chunks)
            def _(chunk):
                drain_sends(index, chunk)

    vmem = pl.BlockSpec(memory_space=pltpu.VMEM)
    hbm = pl.BlockSpec(memory_space=pl.ANY)
    dma = pltpu.SemaphoreType.DMA
    return pl.pallas_call(
        kernel,
        out_shape=jax.ShapeDtypeStruct((2 * half_tokens, chans), BF16),
        in_specs=[hbm, vmem, hbm, hbm, vmem],
        out_specs=vmem,
        scratch_shapes=[
            pltpu.VMEM(latent.shape, BF16),
            pltpu.VMEM((2, half_tokens + width, chans), BF16),
            pltpu.VMEM((half_tokens, chans), BF16),
            pltpu.VMEM((2, width, chans), BF16),
            pltpu.VMEM((3, half_tokens + 2 * width, chans), BF16),
            pltpu.VMEM((2, 3, 3 * CK, chans), BF16),
            pltpu.VMEM((half_tokens, chans), F32),
            pltpu.VMEM((peers, chans), F32),
            pltpu.VMEM((2, half_tokens, chans), BF16),
            pltpu.VMEM((chips, 8, 128), F32),
            pltpu.VMEM((peers, 8, 128), F32),
            pltpu.VMEM((2, 8, 128), F32),
            pltpu.VMEM((2, 2, 8, 128), F32),
            pltpu.VMEM((8, chans), F32),
            dma((2,)), dma, dma, dma((2, chunks)), dma((2, chunks)), dma((2, chunks)), dma, dma, dma((2, 2)), dma((2, 2)), dma, dma,
        ],
        compiler_params=pltpu.CompilerParams(vmem_limit_bytes=52000000, collective_id=0, has_side_effects=True),
        cost_estimate=pl.CostEstimate(flops=72 * half_tokens * chans * chans, bytes_accessed=72 * chans * chans, transcendentals=0),
        name='res_block_in',
    )(latent, time_emb, res_conv, res_time, norms)


def res_block_out(hidden, time_emb, res_conv, res_time, norms, which, width, groups, peers):
    tokens, chans = hidden.shape
    chips = peers // 2
    band = tokens // peers
    half_tokens = tokens // 2
    chunks = chans // CK
    tiles = half_tokens // TM
    per_tile = TM // band
    count = float(tokens * (chans // groups))

    def kernel(hid, time_ref, kern, wtime, norm_ref, out_ref, image, mid, halo, act, wbuf, cbuf, acc, tproj, result, sums, swaps, coef,
       wsem, csem, tsem, give_send, give_recv, swap_send, swap_recv, send_sem, recv_sem):
        me = lax.axis_index('sp')
        chip, core = lax.div(me, 2), lax.rem(me, 2)
        partner = me + 1 - 2 * core
        span = half_tokens + width

        def window(part):
            return pl.ds(pl.multiple_of(part * (half_tokens - width), width), span)

        start_all(fetch_rows(kern, which, 0, 0, wbuf, wsem))
        start_all(time_copies(wtime, which, wbuf.at[1], tsem))
        meet(peers, me)
        clear_edges(act, width)
        member = members(chans, groups)
        await_peers(peers)
        give = remote(hid.at[window(1 - core), :], image.at[core], give_send.at[0], give_recv.at[0], partner)
        give.start()
        image[core] = hid[window(core), :]
        tot, sqr = channel_sums(hid, tokens, chans)
        sums[core] = group_sums(two_rows(tot, sqr), member)
        wait_all(time_copies(wtime, which, wbuf.at[1], tsem))
        time_rows(time_ref, wbuf.at[1], tproj)
        tell = remote(sums.at[core], sums.at[core], give_send.at[1], give_recv.at[1], partner)
        tell.start()
        tell.wait()
        give.wait()
        half_at, halo_at, put, halo_put = half_places(core, half_tokens, width)
        norm = [norm_ref[4 * which + row:4 * which + row + 1] for row in range(4)]

        @pl.loop(0, 2)
        def _(index):
            group_affine(sums[index, 0:2], norm[0], norm[1], member, count, coef, 0.5)
            conv_rows(lambda chunk: fetch_rows(kern, which, 0, chunk, wbuf, wsem),
                      [(image.at[index], half_at, put, half_tokens), (image.at[index], halo_at, halo_put, width)],
                      act, wbuf, coef, acc, width, None)
            start_all(fetch_cols(kern, which, 1, 0, cbuf, csem))

            @pl.when(index == 0)
            def _():
                start_all(fetch_rows(kern, which, 0, 0, wbuf, wsem))

            middle_norm(mid, acc, tproj[pl.ds(index * chips + chip, 1), :], halo.at[index], swaps.at[index], core, partner, member, norm[2], norm[3], count, coef, swap_send.at[index], swap_recv.at[index], width)

            @pl.loop(0, chunks)
            def _(chunk):
                activate(halo.at[index], 0, act, halo_put, width, coef, chunk, width)

                @pl.loop(0, tiles)
                def _(tile):
                    activate(mid, tile * TM, act, put + tile * TM, TM, coef, chunk, width)

            slab = index * chips + chip

            @pl.loop(0, chunks)
            def _(chunk):
                slot = lax.rem(chunk, 2)
                cols = chunk_cols(chunk)

                @pl.when(chunk + 1 < chunks)
                def _():
                    start_all(fetch_cols(kern, which, 1, chunk + 1, cbuf, csem))

                wait_all(fetch_cols(kern, which, 1, chunk, cbuf, csem))

                @pl.loop(0, tiles)
                def _(step):
                    tile = lax.rem(step + lax.div(chip, 2), tiles)
                    part = None
                    for dy in range(3):
                        for dx in range(3):
                            term = nn(shifted(act, dx, tile, dy, width, slice(None)), cbuf[slot, 3 * dy + dx])
                            part = term if part is None else part + term
                    rows = tile_rows(tile)
                    result[index, rows, cols] = (image[index, tile_rows(tile, half_at), cols].astype(F32) + part).astype(BF16)
                    for idx in range(per_tile):
                        here = tile * per_tile + idx
                        peer = core * chips + here
                        block = result.at[index, pl.ds(pl.multiple_of(here * band, band), band), cols]

                        @pl.when(peer == me)
                        def _():
                            out_ref[slab, :, cols] = block[...]

                        @pl.when(peer != me)
                        def _():
                            remote(block, out_ref.at[slab, :, cols], send_sem, recv_sem, peer).start()

        inside = lax.div(me, chips) == core

        @pl.when(inside)
        def _():
            drain(out_ref.at[pl.ds(0, peers - 2)], send_sem)
            drain(out_ref.at[pl.ds(0, peers - 2)], recv_sem)

        @pl.when(jnp.logical_not(inside))
        def _():
            drain(out_ref, send_sem)
            drain(out_ref, recv_sem)

    vmem = pl.BlockSpec(memory_space=pltpu.VMEM)
    hbm = pl.BlockSpec(memory_space=pl.ANY)
    dma = pltpu.SemaphoreType.DMA
    return pl.pallas_call(
        kernel,
        out_shape=jax.ShapeDtypeStruct((peers, band, chans), BF16),
        in_specs=[vmem, vmem, hbm, hbm, vmem],
        out_specs=vmem,
        scratch_shapes=[
            pltpu.VMEM((2, half_tokens + width, chans), BF16),
            pltpu.VMEM((half_tokens, chans), BF16),
            pltpu.VMEM((2, width, chans), BF16),
            pltpu.VMEM((3, half_tokens + 2 * width, chans), BF16),
            pltpu.VMEM((2, 3, 3 * CK, chans), BF16),
            pltpu.VMEM((2, 9, chans, CK), BF16),
            pltpu.VMEM((half_tokens, chans), F32),
            pltpu.VMEM((peers, chans), F32),
            pltpu.VMEM((2, half_tokens, chans), BF16),
            pltpu.VMEM((2, 8, 128), F32),
            pltpu.VMEM((2, 2, 8, 128), F32),
            pltpu.VMEM((8, chans), F32),
            dma((2,)), dma((2,)), dma, dma((2,)), dma((2,)), dma((2, 2)), dma((2, 2)), dma, dma,
        ],
        compiler_params=pltpu.CompilerParams(vmem_limit_bytes=49000000, collective_id=1, has_side_effects=True),
        cost_estimate=pl.CostEstimate(flops=72 * half_tokens * chans * chans, bytes_accessed=72 * chans * chans, transcendentals=0),
        name='res_block_out',
    )(hidden, time_emb, res_conv, res_time, norms)


def transformer(hidden, context, norms, norm_row, proj_inout, qkv_t, self_out, cross_q_t, cross_kv_t, cross_out, ff_in, ff_out, groups, heads, text):
    tokens, chans = hidden.shape
    text_dim = context.shape[1]
    images = context.shape[0] // text
    text_rows = -(-text // 16) * 16
    head_dim = chans // heads
    pairs = heads // 2
    pair = 2 * head_dim
    count = float(tokens * (chans // groups))
    tiles = tokens // TM
    ff_steps = ff_out.shape[0] // chans
    ctx_half = text_dim // 2
    qw = 512 if chans >= 1024 else 256
    kb = 256
    scale = head_dim ** -0.5
    half = chans // 2

    def kernel(h_ref, ctx_ref, norm_ref, pio, wqkv, wo, cq, ckv, co, f1, f2, out_ref,
               ring, tok, aux, q_t, keys, v_t, acc, ctx_mine, ctx_k, ctx_v, coef, rsem):
        units = {
            'in': (pio.at[0], 0, 0), 'q': (wqkv.at[0], 0, 1), 'k': (wqkv.at[1], 1, 0), 'v': (wqkv.at[2], 1, 1),
            'ck0': (ckv.at[0, :, 0:ctx_half], 1, 2), 'ck1': (ckv.at[0, :, ctx_half:text_dim], 0, 2),
            'cv0': (ckv.at[1, :, 0:ctx_half], 0, 0), 'cv1': (ckv.at[1, :, ctx_half:text_dim], 0, 1),
            'o': (wo, 1, 0), 'cq': (cq, 1, 1), 'co': (co, 1, 2), 'out': (pio.at[1], 0, 0),
        }

        def spot(group, place, wide):
            return ring.at[group, place] if wide == chans else ring.at[group, place, :, 0:wide]

        def copy_of(name):
            src, group, place = units[name]
            return pltpu.make_async_copy(src, spot(group, place, src.shape[1]), rsem.at[group, place])

        def start(*names):
            for name in names:
                copy_of(name).start()

        def take(name):
            copy_of(name).wait()
            src, group, place = units[name]
            return spot(group, place, src.shape[1])

        def ff_copies(step, group):
            cols = pl.multiple_of(step * chans, chans)
            return [
                pltpu.make_async_copy(f1.at[:, pl.ds(cols, chans)], ring.at[group, 0], rsem.at[group, 0]),
                pltpu.make_async_copy(f1.at[:, pl.ds(cols + ff_steps * chans, chans)], ring.at[group, 1], rsem.at[group, 1]),
                pltpu.make_async_copy(f2.at[pl.ds(cols, chans), :], ring.at[group, 2], rsem.at[group, 2]),
            ]

        me = lax.axis_index('sp')
        ctx_rows = text * images
        assert ctx_rows <= chans and ctx_half <= chans
        ctx_copies = [
            pltpu.make_async_copy(ctx_ref.at[:, pl.ds(part * ctx_half, ctx_half)], ring.at[1 - part, 2, 0:ctx_rows, 0:ctx_half], rsem.at[1 - part, 2])
            for part in range(2)
        ]
        start_all(ctx_copies)
        start('in', 'q', 'k', 'v')

        tot, sqr = channel_sums(h_ref, tokens, chans)
        member = members(chans, groups)
        sums = group_sums(two_rows(tot, sqr), member)
        group_affine(sums, norm_ref[norm_row:norm_row + 1], norm_ref[norm_row + 1:norm_row + 2], member, count, coef, 1.0)

        def project_rows(weight, src, base, normed_to):
            def norm_tile(tile):
                rows = tile_rows(tile)
                normed_to[rows, :] = layer_norm(tok[rows, :].astype(F32))

            @pl.loop(0, tiles)
            def _(tile):
                norm_tile(jnp.maximum(tile - 1, 0))
                rows = tile_rows(tile)
                tok[rows, :] = (base(rows) + nn(src(rows), weight[...])).astype(BF16)

            norm_tile(tiles - 1)

        place = (text_rows, ctx_rows)
        wanted = lax.broadcasted_iota(jnp.int32, place, 0) * images + (lax.rem(me, 2) * (images // 2) + lax.div(me, 2))
        pick = jnp.where(lax.broadcasted_iota(jnp.int32, place, 1) == wanted, 1.0, 0.0).astype(BF16)
        wait_all(ctx_copies)
        for part in range(2):
            ctx_mine[part] = nn(pick, ring[1 - part, 2, 0:ctx_rows, 0:ctx_half]).astype(BF16)
        start('ck0', 'ck1')
        project_rows(take('in'), lambda rows: (h_ref[rows, :].astype(F32) * coef[0:1] + coef[1:2]).astype(BF16), lambda rows: 0.0, aux)
        start('cv0')

        def transposed(weight, src, dst, factor):
            @pl.loop(0, 2)
            def _(part):
                rows = pl.ds(pl.multiple_of(part * half, half), half)
                dst[rows, :] = (nt(weight[rows, :], src[...]).astype(BF16) * factor).astype(BF16) if factor != 1.0 else nt(weight[rows, :], src[...]).astype(BF16)

        transposed(take('q'), aux, q_t, scale)
        start('cv1')
        w_key = take('k')

        @pl.loop(0, tokens // 512)
        def _(part):
            rows = pl.ds(pl.multiple_of(part * 512, 512), 512)
            keys[rows, :] = nt(aux[rows, :], w_key[...]).astype(BF16)
        start('o')
        transposed(take('v'), aux, v_t, 1.0)
        start('cq')
        w_ck = take('ck0'), take('ck1')
        ctx_k[...] = (nt(ctx_mine[0], w_ck[0][...]) + nt(ctx_mine[1], w_ck[1][...])).astype(BF16)
        start('co')
        w_cv = take('cv0'), take('cv1')

        @pl.loop(0, chans // 256)
        def _(part):
            rows = pl.ds(pl.multiple_of(part * 256, 256), 256)
            ctx_v[rows, :] = (nt(w_cv[0][rows, :], ctx_mine[0]) + nt(w_cv[1][rows, :], ctx_mine[1])).astype(BF16)

        for copy in ff_copies(0, 0):
            copy.start()

        row_head = lax.broadcasted_iota(jnp.int32, (pair, 1), 0) < head_dim

        def query_of(hp, first, wide, head):
            both = q_t[pl.ds(pl.multiple_of(hp * pair, pair), pair), pl.ds(first, wide)]
            keep = row_head if head == 0 else jnp.logical_not(row_head)
            return jnp.where(keep, both, jnp.zeros_like(both))

        def pair_cols(hp):
            return pl.ds(pl.multiple_of(hp * pair, pair), pair)

        halves = tokens // qw
        blocks = pairs * halves
        scores = [acc.at[:, pl.ds(h * qw, qw)] for h in range(2)]
        probs = [out_ref.at[:, pl.ds(h * qw, qw)] for h in range(2)]
        parts = tokens // kb

        def place(block):
            hp = lax.div(block, halves)
            return hp, pl.multiple_of((block - hp * halves) * qw, qw)

        def fold(vals, func):
            return func(vals.reshape(-1, 8, vals.shape[-1]), axis=0)

        def score_part(block, head, part):
            hp, first = place(block)
            query = query_of(hp, first, qw, head)
            vals = nn(keys[part * kb:(part + 1) * kb, pair_cols(hp)], query)
            scores[head][part * kb:(part + 1) * kb, :] = vals
            return fold(vals, jnp.max)

        def exp_part(head, part, top):
            vals = jnp.exp(scores[head][part * kb:(part + 1) * kb, :] - top)
            probs[head][part * kb:(part + 1) * kb, :] = vals.astype(BF16)
            return fold(vals, jnp.sum)

        def value_of(block, head, denom):
            hp, _ = place(block)
            vals = v_t[pl.ds(pl.multiple_of(hp * pair + head * head_dim, head_dim), head_dim), :]
            return nn(vals, probs[head][...]) / denom

        def softmax_stage(score_block, score_head, exp_head, top):
            tops, sums = [], []
            for part in range(parts):
                tops.append(score_part(score_block, score_head, part))
                sums.append(exp_part(exp_head, part, top))
            new_top = jnp.max(functools.reduce(jnp.maximum, tops), axis=0, keepdims=True)
            return new_top, jnp.sum(functools.reduce(jnp.add, sums), axis=0, keepdims=True)

        def emit(block, low, high):
            hp, first = place(block)
            aux[pl.ds(first, qw), pair_cols(hp)] = jnp.concatenate([low, high], axis=0).T.astype(BF16)

        top_first = jnp.max(functools.reduce(jnp.maximum, [score_part(0, 0, part) for part in range(parts)]), axis=0, keepdims=True)
        zero_row = jnp.ones((1, qw), F32)
        zero_out = jnp.zeros((head_dim, qw), F32)

        def attend_block(block, carry):
            top0, denom1, low = carry
            before = jnp.maximum(block - 1, 0)
            high = value_of(before, 1, denom1)
            emit(before, low, high)
            top1, denom0 = softmax_stage(block, 1, 0, top0)
            after = jnp.minimum(block + 1, blocks - 1)
            low = value_of(block, 0, denom0)
            top0, denom1 = softmax_stage(after, 0, 1, top1)
            return top0, denom1, low

        _, denom1, low = lax.fori_loop(0, blocks, attend_block, (top_first, zero_row, zero_out))
        emit(blocks - 1, low, value_of(blocks - 1, 1, denom1))

        project_rows(take('o'), lambda rows: aux[rows, :], lambda rows: tok[rows, :].astype(F32), keys)
        transposed(take('cq'), keys, q_t, scale)

        text_valid = lax.broadcasted_iota(jnp.int32, (text_rows, 1), 0) < text

        @pl.loop(0, pairs // 2)
        def _(step):
            for sub in range(2):
                hp = step * 2 + sub
                outs = []
                for head in range(2):
                    vals = nn(ctx_k[:, pair_cols(hp)], query_of(hp, 0, tokens, head))
                    vals = jnp.where(text_valid, vals, -jnp.inf)
                    weights = jnp.exp(vals - jnp.max(vals, axis=0, keepdims=True))
                    denom = jnp.sum(weights, axis=0, keepdims=True)
                    text_vals = ctx_v[pl.ds(pl.multiple_of(hp * pair + head * head_dim, head_dim), head_dim), :]
                    outs.append(nn(text_vals, weights.astype(BF16)) / denom)
                aux[:, pair_cols(hp)] = jnp.concatenate(outs, axis=0).T.astype(BF16)

        project_rows(take('co'), lambda rows: aux[rows, :], lambda rows: tok[rows, :].astype(F32), keys)
        for copy in ff_copies(1, 1):
            copy.start()
        acc[...] = jnp.zeros_like(acc)

        @pl.loop(0, ff_steps)
        def _(step):
            group = lax.rem(step, 2)
            for copy in ff_copies(step, group):
                copy.wait()

            @pl.loop(0, tiles)
            def _(tile):
                rows = tile_rows(tile)
                src = keys[rows, :]
                value = nn(src, ring[group, 0])
                gate = nn(src, ring[group, 1])
                gated = (value * (0.5 * gate * (1.0 + lax.erf(gate * (0.5 ** 0.5))))).astype(BF16)
                acc[rows, :] += nn(gated, ring[group, 2])

            @pl.when(step + 2 < ff_steps)
            def _():
                for copy in ff_copies(step + 2, group):
                    copy.start()

            @pl.when(step == ff_steps - 2)
            def _():
                start('out')

        w_fin = take('out')

        @pl.loop(0, tiles)
        def _(tile):
            rows = tile_rows(tile)
            t = (tok[rows, :].astype(F32) + acc[rows, :]).astype(BF16)
            out_ref[rows, :] = (h_ref[rows, :].astype(F32) + nn(t, w_fin[...])).astype(BF16)

    vmem = pl.BlockSpec(memory_space=pltpu.VMEM)
    hbm = pl.BlockSpec(memory_space=pl.ANY)
    flops = 2 * tokens * chans * chans * (8 + 3 * ff_steps) + 4 * tokens * tokens * chans
    return pl.pallas_call(
        kernel,
        out_shape=jax.ShapeDtypeStruct(hidden.shape, BF16),
        in_specs=[vmem, hbm, vmem] + [hbm] * 8,
        out_specs=vmem,
        scratch_shapes=[
            pltpu.VMEM((2, 3, chans, chans), BF16),
            pltpu.VMEM((tokens, chans), BF16),
            pltpu.VMEM((tokens, chans), BF16),
            pltpu.VMEM((chans, tokens), BF16),
            pltpu.VMEM((tokens, chans), BF16),
            pltpu.VMEM((chans, tokens), BF16),
            pltpu.VMEM((tokens, chans), F32),
            pltpu.VMEM((2, text_rows, ctx_half), BF16),
            pltpu.VMEM((text_rows, chans), BF16),
            pltpu.VMEM((chans, text_rows), BF16),
            pltpu.VMEM((8, chans), F32),
            pltpu.SemaphoreType.DMA((2, 3)),
        ],
        compiler_params=pltpu.CompilerParams(vmem_limit_bytes=49000000),
        cost_estimate=pl.CostEstimate(flops=flops, bytes_accessed=80_000_000, transcendentals=tokens * tokens * heads),
        name='transformer',
    )(hidden, context, norms, proj_inout, qkv_t, self_out, cross_q_t, cross_kv_t, cross_out, ff_in, ff_out)


def solution(mesh):
    num_bands = mesh.shape['sp']

    def local_stage(latent, time_emb, context, res_conv, res_time, res_norm, attn_norm, proj_inout, self_qkv, self_out, cross_q, cross_kv, cross_out, ff_in, ff_out):
        images, band_rows, width, chans = latent.shape
        assert images == num_bands
        band = band_rows * width
        heads, head_dim = self_out.shape[:2]
        groups = res_norm.shape[3]
        text, text_dim = context.shape[1:]
        norms = jnp.concatenate([res_norm.reshape(8, chans), attn_norm.reshape(2, chans)], axis=0).astype(F32)
        first = res_block_in(latent.reshape(images, band, chans), time_emb, res_conv, res_time, norms, 0, width, groups)
        middle = transformer(
            first, jnp.transpose(context, (1, 0, 2)).reshape(text * images, text_dim), norms, 8, proj_inout,
            jnp.transpose(self_qkv, (0, 2, 3, 1)).reshape(3, chans, chans),
            self_out.reshape(chans, chans),
            jnp.transpose(cross_q, (1, 2, 0)).reshape(chans, chans),
            jnp.transpose(cross_kv, (0, 2, 3, 1)).reshape(2, chans, text_dim),
            cross_out.reshape(chans, chans), ff_in, ff_out, groups, heads, text)
        out = res_block_out(middle, time_emb, res_conv, res_time, norms, 1, width, groups, num_bands)
        return out.reshape(latent.shape)

    band_spec = P('dp', 'sp', None, None)
    shared = P()
    in_specs = (band_spec, P('dp', None), P('dp', None, None)) + (shared,) * 12
    return jax.shard_map(local_stage, mesh=mesh, in_specs=in_specs, out_specs=band_spec, check_vma=False)
```

```python
import functools

import jax
import jax.numpy as jnp
from jax import lax
from jax.experimental import pallas as pl
from jax.experimental.pallas import tpu as pltpu
from jax.sharding import PartitionSpec as P

BF16 = jnp.bfloat16
F32 = jnp.float32
MESH = pl.DeviceIdType.MESH
GN_EPS = 1e-6
LN_EPS = 1e-5
TM = 256
CK = 256
VMEM_LIMIT = 67_000_000


def nn(lhs, rhs):
    return lax.dot_general(lhs, rhs, (((1,), (0,)), ((), ())), preferred_element_type=F32)


def nt(lhs, rhs):
    return lax.dot_general(lhs, rhs, (((1,), (1,)), ((), ())), preferred_element_type=F32)


def split3(vals):
    high = vals.astype(BF16).astype(F32)
    rest = vals - high
    mid = rest.astype(BF16).astype(F32)
    return [high, mid, rest - mid]


def channel_sums(src, rows, chans):
    def step(idx, carry):
        tot, sqr = carry
        vals = src[pl.ds(pl.multiple_of(idx * 64, 64), 64), :].astype(F32).reshape(8, 8, chans)
        return tot + jnp.sum(vals, axis=0), sqr + jnp.sum(vals * vals, axis=0)

    zero = jnp.zeros((8, chans), F32)
    return lax.fori_loop(0, rows // 64, step, (zero, zero))


def layer_norm(tokens):
    centred = tokens - jnp.mean(tokens, axis=-1, keepdims=True)
    return (centred * lax.rsqrt(jnp.mean(centred * centred, axis=-1, keepdims=True) + LN_EPS)).astype(BF16)


def meet(peers, me):
    barrier = pltpu.get_barrier_semaphore()

    @pl.loop(1, peers)
    def _(step):
        pl.semaphore_signal(barrier, inc=1, device_id={'sp': lax.rem(me + step, peers)}, device_id_type=MESH)


def await_peers(peers):
    pl.semaphore_wait(pltpu.get_barrier_semaphore(), peers - 1)


def drain(ref, sem):
    pltpu.make_async_copy(ref, ref, sem).wait()


def remote(src, dst, send_sem, recv_sem, peer):
    return pltpu.make_async_remote_copy(src, dst, send_sem, recv_sem, device_id={'sp': peer}, device_id_type=MESH)


def chunk_cols(chunk):
    return pl.ds(pl.multiple_of(chunk * CK, CK), CK)


def tile_rows(tile, first=0):
    return pl.ds(pl.multiple_of(first + tile * TM, 32), TM)


def members(chans, groups, offset=0):
    width = chans // groups
    chan = lax.broadcasted_iota(jnp.int32, (chans, 128), 0)
    low = (lax.broadcasted_iota(jnp.int32, (chans, 128), 1) - offset) * width
    return jnp.where((chan >= low) & (chan < low + width), 1.0, 0.0).astype(BF16)


def group_sums(rows, member):
    count = rows.shape[0]
    high, mid, low = split3(rows)
    sums = nn(jnp.concatenate([high, mid, low], axis=0).astype(BF16), member)
    return sums[0:count] + sums[count:2 * count] + sums[2 * count:3 * count]


def group_affine(sums, gain, shift, member, count, coef, factor):
    mean = sums[0:1] / count
    rstd = lax.rsqrt(sums[1:2] / count - mean * mean + GN_EPS)
    back = jnp.concatenate(split3(mean) + split3(rstd) + [jnp.zeros((2, 128), F32)], axis=0).astype(BF16)
    wide = nt(back, member)
    scale = (wide[3:4] + wide[4:5] + wide[5:6]) * gain
    coef[0:1, :] = factor * scale
    coef[1:2, :] = factor * (shift - (wide[0:1] + wide[1:2] + wide[2:3]) * scale)


def two_rows(tot, sqr):
    rows = [jnp.sum(tot, axis=0, keepdims=True), jnp.sum(sqr, axis=0, keepdims=True)]
    return jnp.concatenate(rows + [jnp.zeros((6, tot.shape[1]), F32)], axis=0)


def activate(src, act, coef, first, wide, tile, width):
    cols = pl.ds(first, wide)
    half = src[tile_rows(tile), cols].astype(F32) * coef[0:1, cols] + coef[1:2, cols]
    vals = half + half * jnp.tanh(half)
    column = lax.rem(lax.broadcasted_iota(jnp.int32, (TM, wide), 0), width)
    put = tile_rows(tile, width)
    act[0, put, cols] = jnp.where(column == 0, 0.0, pltpu.roll(vals, 1, 0)).astype(BF16)
    act[1, put, cols] = vals.astype(BF16)
    act[2, put, cols] = jnp.where(column == width - 1, 0.0, pltpu.roll(vals, TM - 1, 0)).astype(BF16)


def clear_edges(act, width):
    edge = jnp.zeros((width, act.shape[2]), BF16)
    for shift in range(3):
        act[shift, 0:width, :] = edge
        act[shift, act.shape[1] - width:act.shape[1], :] = edge


def shifted(act, shift, tile, row, width, cols):
    return act[shift, tile_rows(tile, row * width), cols]


def taps():
    return [(dy, dx) for dy in range(3) for dx in range(3)]


def fetch_rows(kern, which, conv, chunk, wbuf, sem):
    slot = lax.rem(chunk, 2)
    return [pltpu.make_async_copy(kern.at[which, conv, dy, dx, chunk_cols(chunk), :], wbuf.at[slot, pl.ds(tap * CK, CK), :], sem.at[slot])
            for tap, (dy, dx) in enumerate(taps())]


def fetch_halves(kern, which, conv, chunk, wbuf, sem):
    slot, half, count = lax.rem(chunk, 2), CK // 2, len(taps())
    return [pltpu.make_async_copy(kern.at[which, conv, dy, dx, pl.ds(chunk * CK + part * half, half), :], wbuf.at[slot, pl.ds((part * count + tap) * half, half), :], sem.at[slot])
            for part in range(2) for tap, (dy, dx) in enumerate(taps())]


def fetch_cols(kern, which, conv, chunk, wbuf, sem):
    slot = lax.rem(chunk, 2)
    return [pltpu.make_async_copy(kern.at[which, conv, dy, dx, :, chunk_cols(chunk)], wbuf.at[slot, tap], sem.at[slot])
            for tap, (dy, dx) in enumerate(taps())]


def start_all(copies):
    for copy in copies:
        copy.start()


def wait_all(copies):
    for copy in copies:
        copy.wait()


def chunk_product(act, wbuf, slot, chunk, tile, width):
    cols = chunk_cols(chunk)
    return sum(nn(shifted(act, dx, tile, dy, width, cols), wbuf[slot, tap * CK:(tap + 1) * CK, :]) for tap, (dy, dx) in enumerate(taps()))


def half_product(act, wbuf, slot, first, part, tile, width):
    depth = len(taps()) * (CK // 2)
    rows = jnp.concatenate([shifted(act, dx, tile, dy, width, pl.ds(first, CK // 2)) for dy, dx in taps()], axis=1)
    return nn(rows, wbuf[slot, pl.ds(pl.multiple_of(part * depth, depth), depth), :])


def conv_rows(fetch, src, act, wbuf, coef, acc, width):
    tokens, chans = acc.shape
    chunks = chans // CK
    acc[...] = jnp.zeros_like(acc)

    def build(chunk, tile):
        activate(src, act, coef, pl.multiple_of(chunk * CK, CK), CK, tile, width)

    @pl.loop(0, tokens // TM)
    def _(tile):
        build(0, tile)

    @pl.loop(0, chunks)
    def _(chunk):
        @pl.when(chunk + 1 < chunks)
        def _():
            start_all(fetch(chunk + 1))

        wait_all(fetch(chunk))

        @pl.loop(0, tokens // TM)
        def _(tile):
            acc[tile_rows(tile), :] += chunk_product(act, wbuf, lax.rem(chunk, 2), chunk, tile, width)
            build(lax.rem(chunk + 1, chunks), tile)


def add_rows(dst, acc, other):
    @pl.loop(0, acc.shape[0] // 64)
    def _(idx):
        rows = pl.ds(pl.multiple_of(idx * 64, 64), 64)
        dst[rows, :] = ((other if other.shape[0] == 1 else other[rows, :].astype(F32)) + acc[rows, :]).astype(BF16)


def time_copy(res_time, which, wbuf, sem):
    depth = res_time.shape[1]
    return pltpu.make_async_copy(res_time.at[which], wbuf.at[1, pl.ds(0, depth), :], sem)


def time_row(time_ref, wbuf, tproj, image):
    emb = time_ref[...].astype(F32)
    act = (emb / (1.0 + jnp.exp(-emb))).astype(BF16)
    tproj[...] = nn(act, wbuf[1, 0:act.shape[1], :])
    return tproj[pl.ds(image, 1), :]


def norm_from(src, member, norm_ref, row, count, coef):
    tot, sqr = channel_sums(src, src.shape[0], src.shape[1])
    group_affine(group_sums(two_rows(tot, sqr), member), norm_ref[row:row + 1], norm_ref[row + 1:row + 2], member, count, coef, 0.5)


def res_block_in(latent, time_emb, res_conv, res_time, norms, which, width, groups):
    peers, band, chans = latent.shape
    tokens = peers * band
    last = chans // CK - 1
    half = CK // 2
    pieces = [(chunk * CK, CK) for chunk in range(last)] + [(last * CK, half), (last * CK + half, half)]
    count = float(tokens * (chans // groups))
    tiles = tokens // TM

    def kernel(lat, time_ref, kern, wtime, norm_ref, out_ref, own, image, mid, act, wbuf, acc, tproj, rows, mine, stats, coef,
               wsem, tsem, own_sem, send_sem, recv_sem, stat_send, stat_recv):
        me = lax.axis_index('sp')
        load = pltpu.make_async_copy(lat, own, own_sem)
        load.start()
        start_all(fetch_rows(kern, which, 0, 0, wbuf, wsem))
        weight = time_copy(wtime, which, wbuf, tsem)
        weight.start()
        meet(peers, me)
        clear_edges(act, width)
        member = members(chans, groups)
        own_rows = pl.ds(pl.multiple_of(me * band, band), band)
        await_peers(peers)

        def send(index):
            first, wide = pieces[index]

            @pl.loop(1, peers)
            def _(step):
                peer = lax.rem(me + step, peers)
                remote(lat.at[peer, :, pl.ds(first, wide)], image.at[own_rows, pl.ds(first, wide)], send_sem.at[index], recv_sem.at[index], peer).start()

        send(0)
        load.wait()

        @pl.loop(0, peers)
        def _(peer):
            vals = own[peer].astype(F32).reshape(band // 8, 8, chans)
            rows[pl.ds(peer, 1), :] = jnp.sum(jnp.sum(vals, axis=0), axis=0, keepdims=True)
            rows[pl.ds(peers + peer, 1), :] = jnp.sum(jnp.sum(vals * vals, axis=0), axis=0, keepdims=True)

        sums = group_sums(rows[...], member)
        for peer in range(peers):
            mine[peer, 0:1, :] = sums[peer:peer + 1]
            mine[peer, 1:2, :] = sums[peers + peer:peers + peer + 1]

        @pl.loop(1, peers)
        def _(step):
            peer = lax.rem(me + step, peers)
            remote(mine.at[peer], stats.at[me], stat_send, stat_recv, peer).start()

        for index in range(1, len(pieces)):
            send(index)
        image[own_rows, :] = own[me]
        stats[me] = mine[me]
        weight.wait()
        bias = time_row(time_ref, wbuf, tproj, me)
        acc[...] = jnp.zeros_like(acc)
        drain(stats.at[pl.ds(0, peers - 1)], stat_recv)
        drain(stats.at[pl.ds(0, peers - 1)], stat_send)
        row = 4 * which
        group_affine(jnp.sum(stats[...], axis=0), norm_ref[row:row + 1], norm_ref[row + 1:row + 2], member, count, coef, 0.5)

        def landed(index):
            first, wide = pieces[index]
            return image.at[pl.ds(0, tokens - band), pl.ds(first, wide)]

        @pl.loop(0, last)
        def _(chunk):
            @pl.when(chunk + 1 < last)
            def _():
                start_all(fetch_rows(kern, which, 0, chunk + 1, wbuf, wsem))

            @pl.when(chunk + 1 == last)
            def _():
                start_all(fetch_halves(kern, which, 0, last, wbuf, wsem))

            wait_all(fetch_rows(kern, which, 0, chunk, wbuf, wsem))
            drain(image.at[pl.ds(0, tokens - band), chunk_cols(chunk)], recv_sem.at[chunk])

            @pl.loop(0, tiles)
            def _(tile):
                activate(image, act, coef, pl.multiple_of(chunk * CK, CK), CK, tile, width)

            @pl.loop(0, tiles)
            def _(tile):
                acc[tile_rows(tile), :] += chunk_product(act, wbuf, lax.rem(chunk, 2), chunk, tile, width)

        wait_all(fetch_halves(kern, which, 0, last, wbuf, wsem))

        @pl.loop(0, 2)
        def _(part):
            first = pl.multiple_of(last * CK + part * half, half)
            drain(image.at[pl.ds(0, tokens - band), pl.ds(first, half)], recv_sem.at[last + part])

            @pl.loop(0, tiles)
            def _(tile):
                activate(image, act, coef, first, half, tile, width)

            @pl.loop(0, tiles)
            def _(tile):
                acc[tile_rows(tile), :] += half_product(act, wbuf, last % 2, first, part, tile, width)

        start_all(fetch_rows(kern, which, 1, 0, wbuf, wsem))
        add_rows(mid, acc, bias)
        norm_from(mid, member, norm_ref, row + 2, count, coef)
        conv_rows(lambda chunk: fetch_rows(kern, which, 1, chunk, wbuf, wsem), mid, act, wbuf, coef, acc, width)
        add_rows(out_ref, acc, image)
        for index in range(len(pieces)):
            drain(landed(index), send_sem.at[index])

    vmem = pl.BlockSpec(memory_space=pltpu.VMEM)
    hbm = pl.BlockSpec(memory_space=pl.ANY)
    dma = pltpu.SemaphoreType.DMA
    return pl.pallas_call(
        kernel,
        out_shape=jax.ShapeDtypeStruct((tokens, chans), BF16),
        in_specs=[hbm, vmem, hbm, hbm, vmem],
        out_specs=vmem,
        scratch_shapes=[
            pltpu.VMEM(latent.shape, BF16),
            pltpu.VMEM((tokens, chans), BF16),
            pltpu.VMEM((tokens, chans), BF16),
            pltpu.VMEM((3, tokens + 2 * width, chans), BF16),
            pltpu.VMEM((2, len(taps()) * CK, chans), BF16),
            pltpu.VMEM((tokens, chans), F32),
            pltpu.VMEM((peers, chans), F32),
            pltpu.VMEM((2 * peers, chans), F32),
            pltpu.VMEM((peers, 8, 128), F32),
            pltpu.VMEM((peers, 8, 128), F32),
            pltpu.VMEM((8, chans), F32),
            dma((2,)), dma, dma, dma((len(pieces),)), dma((len(pieces),)), dma, dma,
        ],
        compiler_params=pltpu.CompilerParams(vmem_limit_bytes=52000000, collective_id=0, has_side_effects=True),
        cost_estimate=cost_of(36 * tokens * chans * chans, 36 * chans * chans),
        name='res_block_in',
    )(latent, time_emb, res_conv, res_time, norms)


def res_block_out(hidden, time_emb, res_conv, res_time, norms, which, width, groups, peers):
    tokens, chans = hidden.shape
    band = tokens // peers
    chunks = chans // CK
    tiles = tokens // TM
    per_tile = TM // band
    count = float(tokens * (chans // groups))

    def kernel(x_ref, time_ref, kern, wtime, norm_ref, out_ref, mid, act, wbuf, cbuf, acc, tproj, coef, wsem, csem, tsem, send_sem, recv_sem):
        me = lax.axis_index('sp')
        start_all(fetch_rows(kern, which, 0, 0, wbuf, wsem))
        weight = time_copy(wtime, which, wbuf, tsem)
        weight.start()
        meet(peers, me)
        clear_edges(act, width)
        member = members(chans, groups)
        row = 4 * which
        norm_from(x_ref, member, norm_ref, row, count, coef)
        weight.wait()
        bias = time_row(time_ref, wbuf, tproj, me)
        conv_rows(lambda chunk: fetch_rows(kern, which, 0, chunk, wbuf, wsem), x_ref, act, wbuf, coef, acc, width)
        start_all(fetch_cols(kern, which, 1, 0, cbuf, csem))
        add_rows(mid, acc, bias)
        norm_from(mid, member, norm_ref, row + 2, count, coef)

        @pl.loop(0, chunks)
        def _(chunk):
            @pl.loop(0, tiles)
            def _(tile):
                activate(mid, act, coef, pl.multiple_of(chunk * CK, CK), CK, tile, width)

        await_peers(peers)
        turn = lax.div(me, per_tile) + tiles // 2
        result = mid

        @pl.loop(0, chunks)
        def _(chunk):
            slot = lax.rem(chunk, 2)
            cols = chunk_cols(chunk)

            @pl.when(chunk + 1 < chunks)
            def _():
                start_all(fetch_cols(kern, which, 1, chunk + 1, cbuf, csem))

            wait_all(fetch_cols(kern, which, 1, chunk, cbuf, csem))

            @pl.loop(0, tiles)
            def _(step):
                tile = lax.rem(step + turn, tiles)
                part = sum(nn(shifted(act, dx, tile, dy, width, slice(None)), cbuf[slot, tap]) for tap, (dy, dx) in enumerate(taps()))
                rows = tile_rows(tile)
                result[rows, cols] = (x_ref[rows, cols].astype(F32) + part).astype(BF16)
                for idx in range(per_tile):
                    peer = tile * per_tile + idx
                    block = result.at[pl.ds(pl.multiple_of(peer * band, band), band), cols]

                    @pl.when(peer == me)
                    def _():
                        out_ref[me, :, cols] = block[...]

                    @pl.when(peer != me)
                    def _():
                        remote(block, out_ref.at[me, :, cols], send_sem, recv_sem, peer).start()

        others = out_ref.at[pl.ds(0, peers - 1)]
        drain(others, send_sem)
        drain(others, recv_sem)

    vmem = pl.BlockSpec(memory_space=pltpu.VMEM)
    hbm = pl.BlockSpec(memory_space=pl.ANY)
    dma = pltpu.SemaphoreType.DMA
    return pl.pallas_call(
        kernel,
        out_shape=jax.ShapeDtypeStruct((peers, band, chans), BF16),
        in_specs=[vmem, vmem, hbm, hbm, vmem],
        out_specs=vmem,
        scratch_shapes=[
            pltpu.VMEM((tokens, chans), BF16),
            pltpu.VMEM((3, tokens + 2 * width, chans), BF16),
            pltpu.VMEM((2, len(taps()) * CK, chans), BF16),
            pltpu.VMEM((2, len(taps()), chans, CK), BF16),
            pltpu.VMEM((tokens, chans), F32),
            pltpu.VMEM((peers, chans), F32),
            pltpu.VMEM((8, chans), F32),
            dma((2,)), dma((2,)), dma, dma, dma,
        ],
        compiler_params=pltpu.CompilerParams(vmem_limit_bytes=49000000, collective_id=1, has_side_effects=True),
        cost_estimate=cost_of(36 * tokens * chans * chans, 36 * chans * chans),
        name='res_block_out',
    )(hidden, time_emb, res_conv, res_time, norms)


def cost_of(flops, nbytes):
    return pl.CostEstimate(flops=flops, bytes_accessed=nbytes, transcendentals=0)


def transformer(hidden, context, norms, norm_row, proj_inout, qkv_t, self_out, cross_q_t, cross_kv_t, cross_out, ff_in, ff_out, groups, heads, text):
    tokens, chans = hidden.shape
    text_dim = context.shape[1]
    images = context.shape[0] // text
    text_rows = -(-text // 16) * 16
    head_dim = chans // heads
    pairs = heads // 2
    pair = 2 * head_dim
    count = float(tokens * (chans // groups))
    tiles = tokens // TM
    ff_steps = ff_out.shape[0] // chans
    ctx_half = text_dim // 2
    qw = 512 if chans >= 1024 else 256
    kb = 256
    scale = head_dim ** -0.5
    half = chans // 2

    def kernel(h_ref, ctx_ref, norm_ref, pio, wqkv, wo, cq, ckv, co, f1, f2, out_ref,
               ring, tok, aux, q_t, keys, v_t, acc, ctx_mine, ctx_k, ctx_v, coef, rsem):
        units = {
            'in': (pio.at[0], 0, 0), 'q': (wqkv.at[0], 0, 1), 'k': (wqkv.at[1], 1, 0), 'v': (wqkv.at[2], 1, 1),
            'ck0': (ckv.at[0, :, 0:ctx_half], 1, 2), 'ck1': (ckv.at[0, :, ctx_half:text_dim], 0, 2),
            'cv0': (ckv.at[1, :, 0:ctx_half], 0, 0), 'cv1': (ckv.at[1, :, ctx_half:text_dim], 0, 1),
            'o': (wo, 1, 0), 'cq': (cq, 1, 1), 'co': (co, 1, 2), 'out': (pio.at[1], 0, 0),
        }

        def spot(group, place, wide):
            return ring.at[group, place] if wide == chans else ring.at[group, place, :, 0:wide]

        def copy_of(name):
            src, group, place = units[name]
            return pltpu.make_async_copy(src, spot(group, place, src.shape[1]), rsem.at[group, place])

        def start(*names):
            for name in names:
                copy_of(name).start()

        def take(name):
            copy_of(name).wait()
            src, group, place = units[name]
            return spot(group, place, src.shape[1])

        def ff_copies(step, group):
            cols = pl.multiple_of(step * chans, chans)
            return [
                pltpu.make_async_copy(f1.at[:, pl.ds(cols, chans)], ring.at[group, 0], rsem.at[group, 0]),
                pltpu.make_async_copy(f1.at[:, pl.ds(cols + ff_steps * chans, chans)], ring.at[group, 1], rsem.at[group, 1]),
                pltpu.make_async_copy(f2.at[pl.ds(cols, chans), :], ring.at[group, 2], rsem.at[group, 2]),
            ]

        me = lax.axis_index('sp')
        ctx_rows = text * images
        assert ctx_rows <= chans and ctx_half <= chans
        ctx_copies = [
            pltpu.make_async_copy(ctx_ref.at[:, pl.ds(part * ctx_half, ctx_half)], ring.at[1 - part, 2, 0:ctx_rows, 0:ctx_half], rsem.at[1 - part, 2])
            for part in range(2)
        ]
        start_all(ctx_copies)
        start('in', 'q', 'k', 'v')

        tot, sqr = channel_sums(h_ref, tokens, chans)
        member = members(chans, groups)
        sums = group_sums(two_rows(tot, sqr), member)
        group_affine(sums, norm_ref[norm_row:norm_row + 1], norm_ref[norm_row + 1:norm_row + 2], member, count, coef, 1.0)

        def project_rows(weight, src, base, normed_to):
            def norm_tile(tile):
                rows = tile_rows(tile)
                normed_to[rows, :] = layer_norm(tok[rows, :].astype(F32))

            @pl.loop(0, tiles)
            def _(tile):
                norm_tile(jnp.maximum(tile - 1, 0))
                rows = tile_rows(tile)
                tok[rows, :] = (base(rows) + nn(src(rows), weight[...])).astype(BF16)

            norm_tile(tiles - 1)

        place = (text_rows, ctx_rows)
        wanted = lax.broadcasted_iota(jnp.int32, place, 0) * images + me
        pick = jnp.where(lax.broadcasted_iota(jnp.int32, place, 1) == wanted, 1.0, 0.0).astype(BF16)
        wait_all(ctx_copies)
        for part in range(2):
            ctx_mine[part] = nn(pick, ring[1 - part, 2, 0:ctx_rows, 0:ctx_half]).astype(BF16)
        start('ck0', 'ck1')
        project_rows(take('in'), lambda rows: (h_ref[rows, :].astype(F32) * coef[0:1] + coef[1:2]).astype(BF16), lambda rows: 0.0, aux)
        start('cv0')

        def transposed(weight, src, dst, factor):
            @pl.loop(0, 2)
            def _(part):
                rows = pl.ds(pl.multiple_of(part * half, half), half)
                dst[rows, :] = (nt(weight[rows, :], src[...]).astype(BF16) * factor).astype(BF16) if factor != 1.0 else nt(weight[rows, :], src[...]).astype(BF16)

        transposed(take('q'), aux, q_t, scale)
        start('cv1')
        w_key = take('k')

        @pl.loop(0, tokens // 512)
        def _(part):
            rows = pl.ds(pl.multiple_of(part * 512, 512), 512)
            keys[rows, :] = nt(aux[rows, :], w_key[...]).astype(BF16)
        start('o')
        transposed(take('v'), aux, v_t, 1.0)
        start('cq')
        w_ck = take('ck0'), take('ck1')
        ctx_k[...] = (nt(ctx_mine[0], w_ck[0][...]) + nt(ctx_mine[1], w_ck[1][...])).astype(BF16)
        start('co')
        w_cv = take('cv0'), take('cv1')

        @pl.loop(0, chans // 256)
        def _(part):
            rows = pl.ds(pl.multiple_of(part * 256, 256), 256)
            ctx_v[rows, :] = (nt(w_cv[0][rows, :], ctx_mine[0]) + nt(w_cv[1][rows, :], ctx_mine[1])).astype(BF16)

        for copy in ff_copies(0, 0):
            copy.start()

        row_head = lax.broadcasted_iota(jnp.int32, (pair, 1), 0) < head_dim

        def query_of(hp, first, wide, head):
            both = q_t[pl.ds(pl.multiple_of(hp * pair, pair), pair), pl.ds(first, wide)]
            keep = row_head if head == 0 else jnp.logical_not(row_head)
            return jnp.where(keep, both, jnp.zeros_like(both))

        def pair_cols(hp):
            return pl.ds(pl.multiple_of(hp * pair, pair), pair)

        halves = tokens // qw
        blocks = pairs * halves
        scores = [acc.at[:, pl.ds(h * qw, qw)] for h in range(2)]
        probs = [out_ref.at[:, pl.ds(h * qw, qw)] for h in range(2)]
        parts = tokens // kb

        def place(block):
            hp = lax.div(block, halves)
            return hp, pl.multiple_of((block - hp * halves) * qw, qw)

        def fold(vals, func):
            return func(vals.reshape(-1, 8, vals.shape[-1]), axis=0)

        def score_part(block, query, head, part):
            hp, _ = place(block)
            vals = nn(keys[part * kb:(part + 1) * kb, pair_cols(hp)], query)
            scores[head][part * kb:(part + 1) * kb, :] = vals
            return fold(vals, jnp.max)

        def exp_part(head, part, top):
            vals = jnp.exp(scores[head][part * kb:(part + 1) * kb, :] - top)
            probs[head][part * kb:(part + 1) * kb, :] = vals.astype(BF16)
            return fold(vals, jnp.sum)

        def value_of(block, head, denom):
            hp, _ = place(block)
            vals = v_t[pl.ds(pl.multiple_of(hp * pair + head * head_dim, head_dim), head_dim), :]
            return nn(vals, probs[head][...]) * (1.0 / denom)

        def block_query(block, head):
            hp, first = place(block)
            return query_of(hp, first, qw, head)

        def softmax_stage(score_block, score_head, exp_head, top):
            tops, sums = [], []
            query = block_query(score_block, score_head)
            for part in range(parts):
                tops.append(score_part(score_block, query, score_head, part))
                sums.append(exp_part(exp_head, part, top))
            new_top = jnp.max(functools.reduce(jnp.maximum, tops), axis=0, keepdims=True)
            return new_top, jnp.sum(functools.reduce(jnp.add, sums), axis=0, keepdims=True)

        def emit(block, low, high):
            hp, first = place(block)
            aux[pl.ds(first, qw), pair_cols(hp)] = jnp.concatenate([low, high], axis=0).T.astype(BF16)

        top_first = jnp.max(functools.reduce(jnp.maximum, [score_part(0, block_query(0, 0), 0, part) for part in range(parts)]), axis=0, keepdims=True)
        zero_row = jnp.ones((1, qw), F32)
        zero_out = jnp.zeros((head_dim, qw), F32)

        def attend_block(block, carry):
            top0, denom1, low = carry
            before = jnp.maximum(block - 1, 0)
            high = value_of(before, 1, denom1)
            emit(before, low, high)
            top1, denom0 = softmax_stage(block, 1, 0, top0)
            after = jnp.minimum(block + 1, blocks - 1)
            low = value_of(block, 0, denom0)
            top0, denom1 = softmax_stage(after, 0, 1, top1)
            return top0, denom1, low

        def attend_blocks(step, carry):
            for sub in range(4):
                carry = attend_block(step * 4 + sub, carry)
            return carry

        _, denom1, low = lax.fori_loop(0, blocks // 4, attend_blocks, (top_first, zero_row, zero_out))
        emit(blocks - 1, low, value_of(blocks - 1, 1, denom1))

        project_rows(take('o'), lambda rows: aux[rows, :], lambda rows: tok[rows, :].astype(F32), keys)
        transposed(take('cq'), keys, q_t, scale)

        text_valid = lax.broadcasted_iota(jnp.int32, (text_rows, 1), 0) < text

        @pl.loop(0, pairs // 2)
        def _(step):
            for sub in range(2):
                hp = step * 2 + sub
                outs = []
                for head in range(2):
                    vals = nn(ctx_k[:, pair_cols(hp)], query_of(hp, 0, tokens, head))
                    vals = jnp.where(text_valid, vals, -jnp.inf)
                    weights = jnp.exp(vals - jnp.max(vals, axis=0, keepdims=True))
                    denom = jnp.sum(weights, axis=0, keepdims=True)
                    text_vals = ctx_v[pl.ds(pl.multiple_of(hp * pair + head * head_dim, head_dim), head_dim), :]
                    outs.append(nn(text_vals, weights.astype(BF16)) * (1.0 / denom))
                aux[:, pair_cols(hp)] = jnp.concatenate(outs, axis=0).T.astype(BF16)

        project_rows(take('co'), lambda rows: aux[rows, :], lambda rows: tok[rows, :].astype(F32), keys)
        for copy in ff_copies(1, 1):
            copy.start()
        acc[...] = jnp.zeros_like(acc)

        @pl.loop(0, ff_steps)
        def _(step):
            group = lax.rem(step, 2)
            for copy in ff_copies(step, group):
                copy.wait()

            @pl.loop(0, tiles, unroll=2)
            def _(tile):
                rows = tile_rows(tile)
                src = keys[rows, :]
                value = nn(src, ring[group, 0])
                gate = nn(src, ring[group, 1])
                gated = (value * (0.5 * gate * (1.0 + lax.erf(gate * (0.5 ** 0.5))))).astype(BF16)
                acc[rows, :] += nn(gated, ring[group, 2])

            @pl.when(step + 2 < ff_steps)
            def _():
                for copy in ff_copies(step + 2, group):
                    copy.start()

            @pl.when(step == ff_steps - 2)
            def _():
                start('out')

        w_fin = take('out')

        @pl.loop(0, tiles)
        def _(tile):
            rows = tile_rows(tile)
            t = (tok[rows, :].astype(F32) + acc[rows, :]).astype(BF16)
            out_ref[rows, :] = (h_ref[rows, :].astype(F32) + nn(t, w_fin[...])).astype(BF16)

    vmem = pl.BlockSpec(memory_space=pltpu.VMEM)
    hbm = pl.BlockSpec(memory_space=pl.ANY)
    flops = 2 * tokens * chans * chans * (8 + 3 * ff_steps) + 4 * tokens * tokens * chans
    return pl.pallas_call(
        kernel,
        out_shape=jax.ShapeDtypeStruct(hidden.shape, BF16),
        in_specs=[vmem, hbm, vmem] + [hbm] * 8,
        out_specs=vmem,
        scratch_shapes=[
            pltpu.VMEM((2, 3, chans, chans), BF16),
            pltpu.VMEM((tokens, chans), BF16),
            pltpu.VMEM((tokens, chans), BF16),
            pltpu.VMEM((chans, tokens), BF16),
            pltpu.VMEM((tokens, chans), BF16),
            pltpu.VMEM((chans, tokens), BF16),
            pltpu.VMEM((tokens, chans), F32),
            pltpu.VMEM((2, text_rows, ctx_half), BF16),
            pltpu.VMEM((text_rows, chans), BF16),
            pltpu.VMEM((chans, text_rows), BF16),
            pltpu.VMEM((8, chans), F32),
            pltpu.SemaphoreType.DMA((2, 3)),
        ],
        compiler_params=pltpu.CompilerParams(vmem_limit_bytes=49000000),
        cost_estimate=cost_of(flops, 50 * chans * chans),
        name='transformer',
    )(hidden, context, norms, proj_inout, qkv_t, self_out, cross_q_t, cross_kv_t, cross_out, ff_in, ff_out)


def solution(mesh):
    num_bands = mesh.shape['sp']

    def local_stage(latent, time_emb, context, res_conv, res_time, res_norm, attn_norm, proj_inout, self_qkv, self_out, cross_q, cross_kv, cross_out, ff_in, ff_out):
        images, band_rows, width, chans = latent.shape
        assert images == num_bands
        band = band_rows * width
        heads, head_dim = self_out.shape[:2]
        groups = res_norm.shape[3]
        text, text_dim = context.shape[1:]
        norms = jnp.concatenate([res_norm.reshape(8, chans), attn_norm.reshape(2, chans)], axis=0).astype(F32)
        first = res_block_in(latent.reshape(images, band, chans), time_emb, res_conv, res_time, norms, 0, width, groups)
        middle = transformer(
            first, jnp.transpose(context, (1, 0, 2)).reshape(text * images, text_dim), norms, 8, proj_inout,
            jnp.transpose(self_qkv, (0, 2, 3, 1)).reshape(3, chans, chans),
            self_out.reshape(chans, chans),
            jnp.transpose(cross_q, (1, 2, 0)).reshape(chans, chans),
            jnp.transpose(cross_kv, (0, 2, 3, 1)).reshape(2, chans, text_dim),
            cross_out.reshape(chans, chans), ff_in, ff_out, groups, heads, text)
        out = res_block_out(middle, time_emb, res_conv, res_time, norms, 1, width, groups, num_bands)
        return out.reshape(latent.shape)

    band_spec = P('dp', 'sp', None, None)
    shared = P()
    in_specs = (band_spec, P('dp', None), P('dp', None, None)) + (shared,) * 12
    return jax.shard_map(local_stage, mesh=mesh, in_specs=in_specs, out_specs=band_spec, check_vma=False)
```

```python
import functools

import jax
import jax.numpy as jnp
from jax import lax
from jax.experimental import pallas as pl
from jax.experimental.pallas import tpu as pltpu
from jax.sharding import PartitionSpec as P

BF16 = jnp.bfloat16
F32 = jnp.float32
MESH = pl.DeviceIdType.MESH
GN_EPS = 1e-6
LN_EPS = 1e-5
TM = 256
CK = 256
CROSS_PAIRS = 5
VMEM_LIMIT = 67_000_000


def nn(lhs, rhs):
    return jnp.dot(lhs, rhs, preferred_element_type=F32)


def nt(lhs, rhs):
    return lax.dot_general(lhs, rhs, (((1,), (1,)), ((), ())), preferred_element_type=F32)


def split3(vals):
    high = vals.astype(BF16).astype(F32)
    rest = vals - high
    mid = rest.astype(BF16).astype(F32)
    return [high, mid, rest - mid]


def channel_sums(src, rows, chans):
    def step(idx, carry):
        tot, sqr = carry
        vals = src[pl.ds(pl.multiple_of(idx * 64, 64), 64), :].astype(F32).reshape(8, 8, chans)
        return tot + jnp.sum(vals, axis=0), sqr + jnp.sum(vals * vals, axis=0)

    zero = jnp.zeros((8, chans), F32)
    return lax.fori_loop(0, rows // 64, step, (zero, zero))


def layer_norm(tokens):
    centred = tokens - jnp.mean(tokens, axis=-1, keepdims=True)
    return (centred * lax.rsqrt(jnp.mean(centred * centred, axis=-1, keepdims=True) + LN_EPS)).astype(BF16)


def meet(peers, me):
    barrier = pltpu.get_barrier_semaphore()

    @pl.loop(1, peers)
    def _(step):
        pl.semaphore_signal(barrier, inc=1, device_id={'sp': lax.rem(me + step, peers)}, device_id_type=MESH)


def await_peers(peers):
    pl.semaphore_wait(pltpu.get_barrier_semaphore(), peers - 1)


def drain(ref, sem):
    pltpu.make_async_copy(ref, ref, sem).wait()


def remote(src, dst, send_sem, recv_sem, peer):
    return pltpu.make_async_remote_copy(src, dst, send_sem, recv_sem, device_id={'sp': peer}, device_id_type=MESH)


def chunk_cols(chunk):
    return pl.ds(pl.multiple_of(chunk * CK, CK), CK)


def tile_rows(tile, first=0):
    return pl.ds(pl.multiple_of(first + tile * TM, 32), TM)


def members(chans, groups, offset=0):
    width = chans // groups
    chan = lax.broadcasted_iota(jnp.int32, (chans, 128), 0)
    low = (lax.broadcasted_iota(jnp.int32, (chans, 128), 1) - offset) * width
    return jnp.where((chan >= low) & (chan < low + width), 1.0, 0.0).astype(BF16)


def group_sums(rows, member):
    count = rows.shape[0]
    high, mid, low = split3(rows)
    sums = nn(jnp.concatenate([high, mid, low], axis=0).astype(BF16), member)
    return sums[0:count] + sums[count:2 * count] + sums[2 * count:3 * count]


def group_affine(sums, gain, shift, member, count, coef, factor):
    mean = sums[0:1] / count
    rstd = lax.rsqrt(sums[1:2] / count - mean * mean + GN_EPS)
    back = jnp.concatenate(split3(mean) + split3(rstd) + [jnp.zeros((2, 128), F32)], axis=0).astype(BF16)
    wide = nt(back, member)
    scale = jnp.sum(wide[3:6], axis=0, keepdims=True) * gain
    coef[0:1, :] = factor * scale
    coef[1:2, :] = factor * (shift - jnp.sum(wide[:3], axis=0, keepdims=True) * scale)


def two_rows(tot, sqr):
    rows = [jnp.sum(tot, axis=0, keepdims=True), jnp.sum(sqr, axis=0, keepdims=True)]
    return jnp.concatenate(rows + [jnp.zeros((6, tot.shape[1]), F32)], axis=0)


def activate(src, act, coef, first, wide, row, count, width):
    cols = pl.ds(first, wide)
    half = src[pl.ds(pl.multiple_of(row, width), count), cols].astype(F32) * coef[0:1, cols] + coef[1:2, cols]
    vals = half + half * jnp.tanh(half)
    column = lax.rem(lax.broadcasted_iota(jnp.int32, (count, wide), 0), width)
    put = pl.ds(pl.multiple_of(row + width, width), count)
    act[0, put, cols] = jnp.where(column == 0, 0.0, pltpu.roll(vals, 1, 0)).astype(BF16)
    act[1, put, cols] = vals.astype(BF16)
    act[2, put, cols] = jnp.where(column == width - 1, 0.0, pltpu.roll(vals, count - 1, 0)).astype(BF16)


def clear_edges(act, width):
    edge = jnp.zeros((width, act.shape[2]), BF16)
    for shift in range(3):
        act[shift, 0:width, :] = edge
        act[shift, act.shape[1] - width:act.shape[1], :] = edge


def shifted(act, shift, tile, row, width, cols):
    return act[shift, tile_rows(tile, row * width), cols]


def taps():
    return [(dy, dx) for dy in range(3) for dx in range(3)]


def fetch_rows(kern, which, conv, chunk, wbuf, sem):
    slot = lax.rem(chunk, 2)
    return [pltpu.make_async_copy(kern.at[which, conv, dy, dx, chunk_cols(chunk), :], wbuf.at[slot, pl.ds(tap * CK, CK), :], sem.at[slot])
            for tap, (dy, dx) in enumerate(taps())]


def fetch_halves(kern, which, conv, chunk, wbuf, sem):
    slot, half, count = lax.rem(chunk, 2), CK // 2, len(taps())
    return [pltpu.make_async_copy(kern.at[which, conv, dy, dx, pl.ds(chunk * CK + part * half, half), :], wbuf.at[slot, pl.ds((part * count + tap) * half, half), :], sem.at[slot])
            for part in range(2) for tap, (dy, dx) in enumerate(taps())]


def fetch_cols(kern, which, conv, chunk, wbuf, sem):
    slot = lax.rem(chunk, 2)
    return [pltpu.make_async_copy(kern.at[which, conv, dy, dx, :, chunk_cols(chunk)], wbuf.at[slot, tap], sem.at[slot])
            for tap, (dy, dx) in enumerate(taps())]


def start_all(copies):
    for copy in copies:
        copy.start()


def wait_all(copies):
    for copy in copies:
        copy.wait()


def chunk_product(act, wbuf, slot, chunk, tile, width):
    cols = chunk_cols(chunk)
    return sum(nn(shifted(act, dx, tile, dy, width, cols), wbuf[slot, tap * CK:(tap + 1) * CK, :]) for tap, (dy, dx) in enumerate(taps()))


def half_product(act, wbuf, slot, first, part, tile, width):
    depth = len(taps()) * (CK // 2)
    rows = jnp.concatenate([shifted(act, dx, tile, dy, width, pl.ds(first, CK // 2)) for dy, dx in taps()], axis=1)
    return nn(rows, wbuf[slot, pl.ds(pl.multiple_of(part * depth, depth), depth), :])


def conv_rows(fetch, src, act, wbuf, coef, acc, width):
    tokens, chans = acc.shape
    chunks = chans // CK
    acc[...] = jnp.zeros_like(acc)

    def build(chunk, tile):
        activate(src, act, coef, pl.multiple_of(chunk * CK, CK), CK, tile * TM, TM, width)

    @pl.loop(0, tokens // TM)
    def _(tile):
        build(0, tile)

    @pl.loop(0, chunks)
    def _(chunk):
        @pl.when(chunk + 1 < chunks)
        def _():
            start_all(fetch(chunk + 1))

        wait_all(fetch(chunk))

        @pl.loop(0, tokens // TM)
        def _(tile):
            acc[tile_rows(tile), :] += chunk_product(act, wbuf, lax.rem(chunk, 2), chunk, tile, width)
            build(lax.rem(chunk + 1, chunks), tile)


def add_rows(dst, acc, other):
    @pl.loop(0, acc.shape[0] // 64)
    def _(idx):
        rows = pl.ds(pl.multiple_of(idx * 64, 64), 64)
        dst[rows, :] = (other[rows, :].astype(F32) + acc[rows, :]).astype(BF16)


def time_copy(res_time, which, wbuf, sem):
    return pltpu.make_async_copy(res_time.at[which], wbuf.at[1, pl.ds(0, res_time.shape[1]), :], sem)


def time_row(time_ref, wbuf, tproj, image):
    emb = time_ref[...].astype(F32)
    act = (emb / (1.0 + jnp.exp(-emb))).astype(BF16)
    tproj[...] = nn(act, wbuf[1, 0:act.shape[1], :])
    return tproj[pl.ds(image, 1), :]


def widen(param, chans):
    groups, width = param.shape
    group = lax.broadcasted_iota(jnp.int32, (groups, chans), 0) * width
    chan = lax.broadcasted_iota(jnp.int32, (groups, chans), 1)
    spread = jnp.where((chan >= group) & (chan < group + width), 1.0, 0.0).astype(BF16)
    wide = lax.dot_general(param, spread, (((0,), (0,)), ((), ())), preferred_element_type=F32)
    place = lax.broadcasted_iota(jnp.int32, (width, chans), 0)
    inside = lax.rem(lax.broadcasted_iota(jnp.int32, (width, chans), 1), width)
    return jnp.sum(jnp.where(place == inside, wide, 0.0), axis=0, keepdims=True)


def norm_from(src, member, norm_ref, row, count, coef):
    tot, sqr = channel_sums(src, src.shape[0], src.shape[1])
    group_affine(group_sums(two_rows(tot, sqr), member), norm_ref[row:row + 1], norm_ref[row + 1:row + 2], member, count, coef, 0.5)


def add_and_norm(mid, acc, bias, member, norm_ref, row, count, coef):
    def step(idx, carry):
        rows = pl.ds(pl.multiple_of(idx * 64, 64), 64)
        rounded = (acc[rows, :] + bias).astype(BF16)
        mid[rows, :] = rounded
        vals = rounded.astype(F32).reshape(8, 8, acc.shape[1])
        return carry[0] + jnp.sum(vals, axis=0), carry[1] + jnp.sum(vals * vals, axis=0)

    zero = jnp.zeros((8, acc.shape[1]), F32)
    tot, sqr = lax.fori_loop(0, acc.shape[0] // 64, step, (zero, zero))
    group_affine(group_sums(two_rows(tot, sqr), member), norm_ref[row:row + 1], norm_ref[row + 1:row + 2], member, count, coef, 0.5)


def res_block_in(latent, time_emb, context, res_conv, res_time, res_norm, attn_norm, cross_kv, text, width):
    which, other = 0, 1
    peers, band, chans = latent.shape
    groups = res_norm.shape[1]
    text_dim = context.shape[1]
    text_rows = -(-text // 16) * 16
    block_norms = res_norm.shape[0]
    tokens = peers * band
    last = chans // CK - 1
    half = CK // 2
    pieces = [(chunk * CK, CK) for chunk in range(last)] + [(last * CK, half), (last * CK + half, half)]
    count = float(tokens * (chans // groups))
    tiles = tokens // TM

    def kernel(lat, time_hbm, ctx_hbm, kern, wtime, norm_hbm, attn_hbm, ckv, out_ref, norm_ref, bias_ref, ctx_k, ctx_v,
               image, own, act, wbuf, acc, time_ref, tproj, rows, mine, stats, coef, norm_raw, attn_raw, ctx_raw, ctx_mine, ckv_buf,
               wsem, tsem, own_sem, small_sem, ctx_sem, send_sem, recv_sem, stat_send, stat_recv):
        me = lax.axis_index('sp')
        mid = own
        load = [pltpu.make_async_copy(lat.at[peer], own.at[pl.ds(peer * band, band), :], own_sem) for peer in range(peers)]
        start_all(load)
        small = [pltpu.make_async_copy(src, dst, small_sem.at[index]) for index, (src, dst) in enumerate(((time_hbm, time_ref), (norm_hbm, norm_raw), (attn_hbm, attn_raw)))]
        start_all(small)
        weight = time_copy(wtime, which, wbuf, tsem)
        weight.start()
        start_all(fetch_rows(kern, which, 0, 0, wbuf, wsem))
        ctx_copies = [pltpu.make_async_copy(ctx_hbm, ctx_raw, ctx_sem.at[0]), pltpu.make_async_copy(ckv, ckv_buf, ctx_sem.at[1])]
        start_all(ctx_copies)
        meet(peers, me)
        clear_edges(act, width)
        member = members(chans, groups)
        own_rows = pl.ds(pl.multiple_of(me * band, band), band)
        await_peers(peers)

        def send(index):
            first, wide = pieces[index]

            @pl.loop(1, peers)
            def _(step):
                peer = lax.rem(me + step, peers)
                remote(lat.at[peer, :, pl.ds(first, wide)], image.at[own_rows, pl.ds(first, wide)], send_sem.at[index], recv_sem.at[index], peer).start()

        send(0)
        wait_all(load)

        @pl.loop(0, peers)
        def _(peer):
            vals = own[pl.ds(pl.multiple_of(peer * band, band), band), :].astype(F32).reshape(band // 8, 8, chans)
            rows[pl.ds(peer, 1), :] = jnp.sum(jnp.sum(vals, axis=0), axis=0, keepdims=True)
            rows[pl.ds(peers + peer, 1), :] = jnp.sum(jnp.sum(vals * vals, axis=0), axis=0, keepdims=True)

        sums = group_sums(rows[...], member)
        for peer in range(peers):
            mine[peer, 0:1, :] = sums[peer:peer + 1]
            mine[peer, 1:2, :] = sums[peers + peer:peers + peer + 1]

        @pl.loop(1, peers)
        def _(step):
            peer = lax.rem(me + step, peers)
            remote(mine.at[peer], stats.at[me], stat_send, stat_recv, peer).start()

        for index in range(1, len(pieces)):
            send(index)
        image[own_rows, :] = own[own_rows, :]
        stats[me] = mine[me]
        wait_all(small)
        for index in range(block_norms):
            norm_ref[index:index + 1, :] = widen(norm_raw[index], chans)
        for index in range(2):
            norm_ref[block_norms + index:block_norms + index + 1, :] = widen(attn_raw[index], chans)
        weight.wait()
        rows[0:1, :] = time_row(time_ref, wbuf, tproj, me)
        weight = time_copy(wtime, other, wbuf, tsem)
        weight.start()
        acc[...] = jnp.zeros_like(acc)
        ctx_copies[0].wait()
        place = (text_rows, text * peers)
        wanted = lax.broadcasted_iota(jnp.int32, place, 0) * peers + me
        pick = jnp.where(lax.broadcasted_iota(jnp.int32, place, 1) == wanted, 1.0, 0.0).astype(BF16)
        ctx_mine[...] = nn(pick, ctx_raw[...]).astype(BF16)
        ctx_copies[1].wait()
        ctx_k[...] = nt(ctx_mine[...], ckv_buf[0]).astype(BF16)

        @pl.loop(0, chans // 256)
        def _(part):
            part_rows = pl.ds(pl.multiple_of(part * 256, 256), 256)
            ctx_v[part_rows, :] = nt(ckv_buf[1, part_rows, :], ctx_mine[...]).astype(BF16)

        weight.wait()
        bias_ref[...] = time_row(time_ref, wbuf, tproj, me)
        drain(stats.at[pl.ds(0, peers - 1)], stat_recv)
        drain(stats.at[pl.ds(0, peers - 1)], stat_send)
        row = 4 * which
        group_affine(jnp.sum(stats[...], axis=0), norm_ref[row:row + 1], norm_ref[row + 1:row + 2], member, count, coef, 0.5)

        def landed(index):
            first, wide = pieces[index]
            return image.at[pl.ds(0, tokens - band), pl.ds(first, wide)]

        @pl.loop(0, last)
        def _(chunk):
            @pl.when(chunk + 1 < last)
            def _():
                start_all(fetch_rows(kern, which, 0, chunk + 1, wbuf, wsem))

            @pl.when(chunk + 1 == last)
            def _():
                start_all(fetch_halves(kern, which, 0, last, wbuf, wsem))

            wait_all(fetch_rows(kern, which, 0, chunk, wbuf, wsem))
            drain(image.at[pl.ds(0, tokens - band), chunk_cols(chunk)], recv_sem.at[chunk])

            @pl.loop(0, tiles)
            def _(tile):
                activate(image, act, coef, pl.multiple_of(chunk * CK, CK), CK, tile * TM, TM, width)

            @pl.loop(0, tiles)
            def _(tile):
                acc[tile_rows(tile), :] += chunk_product(act, wbuf, lax.rem(chunk, 2), chunk, tile, width)

        wait_all(fetch_halves(kern, which, 0, last, wbuf, wsem))

        @pl.loop(0, 2)
        def _(part):
            first = pl.multiple_of(last * CK + part * half, half)
            drain(image.at[pl.ds(0, tokens - band), pl.ds(first, half)], recv_sem.at[last + part])

            @pl.loop(0, tiles)
            def _(tile):
                activate(image, act, coef, first, half, tile * TM, TM, width)

            @pl.loop(0, tiles)
            def _(tile):
                acc[tile_rows(tile), :] += half_product(act, wbuf, last % 2, first, part, tile, width)

        start_all(fetch_rows(kern, which, 1, 0, wbuf, wsem))
        add_and_norm(mid, acc, rows[0:1, :], member, norm_ref, row + 2, count, coef)
        conv_rows(lambda chunk: fetch_rows(kern, which, 1, chunk, wbuf, wsem), mid, act, wbuf, coef, acc, width)
        add_rows(out_ref, acc, image)
        for index in range(len(pieces)):
            drain(landed(index), send_sem.at[index])

    vmem = pl.BlockSpec(memory_space=pltpu.VMEM)
    hbm = pl.BlockSpec(memory_space=pl.ANY)
    dma = pltpu.SemaphoreType.DMA
    return pl.pallas_call(
        kernel,
        out_shape=[
            jax.ShapeDtypeStruct((tokens, chans), BF16),
            jax.ShapeDtypeStruct((block_norms + 8, chans), F32),
            jax.ShapeDtypeStruct((1, chans), F32),
            jax.ShapeDtypeStruct((text_rows, chans), BF16),
            jax.ShapeDtypeStruct((chans, text_rows), BF16),
        ],
        in_specs=[hbm] * 8,
        out_specs=[vmem] * 5,
        scratch_shapes=[
            pltpu.VMEM((tokens, chans), BF16),
            pltpu.VMEM((tokens, chans), BF16),
            pltpu.VMEM((3, tokens + 2 * width, chans), BF16),
            pltpu.VMEM((2, len(taps()) * CK, chans), BF16),
            pltpu.VMEM((tokens, chans), F32),
            pltpu.VMEM(time_emb.shape, BF16),
            pltpu.VMEM((peers, chans), F32),
            pltpu.VMEM((2 * peers, chans), F32),
            pltpu.VMEM((peers, 8, 128), F32),
            pltpu.VMEM((peers, 8, 128), F32),
            pltpu.VMEM((8, chans), F32),
            pltpu.VMEM(res_norm.shape, BF16),
            pltpu.VMEM(attn_norm.shape, BF16),
            pltpu.VMEM(context.shape, BF16),
            pltpu.VMEM((text_rows, text_dim), BF16),
            pltpu.VMEM(cross_kv.shape, BF16),
            dma((2,)), dma, dma, dma((3,)), dma((2,)), dma((len(pieces),)), dma((len(pieces),)), dma, dma,
        ],
        compiler_params=pltpu.CompilerParams(vmem_limit_bytes=53000000, collective_id=0, has_side_effects=True),
        cost_estimate=cost_of(36 * tokens * chans * chans, 36 * chans * chans),
        name='res_block_in',
    )(latent, time_emb, context, res_conv, res_time, res_norm, attn_norm, cross_kv)


def res_block_out(hidden, bias, res_conv, norms, width, groups, peers):
    which = 1
    tokens, chans = hidden.shape
    band = tokens // peers
    chunks = chans // CK
    tiles = tokens // TM
    per_tile = TM // band
    count = float(tokens * (chans // groups))

    def kernel(x_ref, bias_ref, kern, norm_ref, out_ref, mid, result, act, wbuf, cbuf, acc, coef, wsem, csem, send_sem, recv_sem):
        me = lax.axis_index('sp')
        start_all(fetch_rows(kern, which, 0, 0, wbuf, wsem))
        meet(peers, me)
        clear_edges(act, width)
        member = members(chans, groups)
        row = 4 * which
        norm_from(x_ref, member, norm_ref, row, count, coef)
        conv_rows(lambda chunk: fetch_rows(kern, which, 0, chunk, wbuf, wsem), x_ref, act, wbuf, coef, acc, width)
        start_all(fetch_cols(kern, which, 1, 0, cbuf, csem))
        add_and_norm(mid, acc, bias_ref[...], member, norm_ref, row + 2, count, coef)

        def build(row, rows):
            @pl.loop(0, chunks)
            def _(chunk):
                activate(mid, act, coef, pl.multiple_of(chunk * CK, CK), CK, row, rows, width)

        def build_tile(tile):
            build(tile * TM, TM)

            @pl.when(tile + 1 < tiles)
            def _():
                build((tile + 1) * TM, width)

        turn = lax.rem(lax.div(me, per_tile) + tiles // 2, tiles)
        build_tile(turn)

        @pl.when(turn > 0)
        def _():
            build(turn * TM - width, width)

        await_peers(peers)

        @pl.loop(0, chunks)
        def _(chunk):
            slot = lax.rem(chunk, 2)
            cols = chunk_cols(chunk)

            @pl.when(chunk + 1 < chunks)
            def _():
                start_all(fetch_cols(kern, which, 1, chunk + 1, cbuf, csem))

            wait_all(fetch_cols(kern, which, 1, chunk, cbuf, csem))

            @pl.loop(0, tiles)
            def _(step):
                tile = lax.rem(step + turn, tiles)
                part = sum(nn(shifted(act, dx, tile, dy, width, slice(None)), cbuf[slot, tap]) for tap, (dy, dx) in enumerate(taps()))
                rows = tile_rows(tile)
                result[rows, cols] = (x_ref[rows, cols].astype(F32) + part).astype(BF16)
                for idx in range(per_tile):
                    peer = tile * per_tile + idx
                    block = result.at[pl.ds(pl.multiple_of(peer * band, band), band), cols]

                    @pl.when(peer == me)
                    def _():
                        out_ref[me, :, cols] = block[...]

                    @pl.when(peer != me)
                    def _():
                        remote(block, out_ref.at[me, :, cols], send_sem, recv_sem, peer).start()

                @pl.when((chunk == 0) & (step + 1 < tiles))
                def _():
                    build_tile(lax.rem(step + 1 + turn, tiles))

        others = out_ref.at[pl.ds(0, peers - 1)]
        drain(others, send_sem)
        drain(others, recv_sem)

    vmem = pl.BlockSpec(memory_space=pltpu.VMEM)
    hbm = pl.BlockSpec(memory_space=pl.ANY)
    dma = pltpu.SemaphoreType.DMA
    return pl.pallas_call(
        kernel,
        out_shape=jax.ShapeDtypeStruct((peers, band, chans), BF16),
        in_specs=[vmem, vmem, hbm, vmem],
        out_specs=vmem,
        scratch_shapes=[
            pltpu.VMEM((tokens, chans), BF16),
            pltpu.VMEM((tokens, chans), BF16),
            pltpu.VMEM((3, tokens + 2 * width, chans), BF16),
            pltpu.VMEM((2, len(taps()) * CK, chans), BF16),
            pltpu.VMEM((2, len(taps()), chans, CK), BF16),
            pltpu.VMEM((tokens, chans), F32),
            pltpu.VMEM((8, chans), F32),
            dma((2,)), dma((2,)), dma, dma,
        ],
        compiler_params=pltpu.CompilerParams(vmem_limit_bytes=48000000, collective_id=1, has_side_effects=True),
        cost_estimate=cost_of(36 * tokens * chans * chans, 36 * chans * chans),
        name='res_block_out',
    )(hidden, bias, res_conv, norms)


def cost_of(flops, nbytes):
    return pl.CostEstimate(flops=flops, bytes_accessed=nbytes, transcendentals=0)


def transformer(hidden, ctx_keys, ctx_vals, norms, norm_row, proj_inout, qkv_t, self_out, cross_q_t, cross_out, ff_in, ff_out, groups, heads, text):
    tokens, chans = hidden.shape
    text_rows = ctx_keys.shape[0]
    head_dim = chans // heads
    pairs = heads // 2
    pair = 2 * head_dim
    count = float(tokens * (chans // groups))
    tiles = tokens // TM
    ff_steps = ff_out.shape[0] // chans
    qw = 512 if chans >= 1024 else 256
    kb = 256
    scale = head_dim ** -0.5
    half = chans // 2

    def kernel(h_ref, ctx_k, ctx_v, norm_ref, pio, wqkv, wo, cq, co, f1, f2, out_ref, ring, tok, aux, both, keys, acc, coef, rsem):
        units = {
            'in': (pio.at[0], 0, 0), 'q': (wqkv.at[0], 0, 1), 'k': (wqkv.at[1], 1, 0), 'v': (wqkv.at[2], 1, 1),
            'o': (wo, 1, 0), 'cq': (cq, 1, 1), 'co': (co, 1, 2), 'out': (pio.at[1], 0, 0),
        }

        def copy_of(name):
            src, group, place = units[name]
            return pltpu.make_async_copy(src, ring.at[group, place], rsem.at[group, place])

        def start(*names):
            for name in names:
                copy_of(name).start()

        def take(name):
            copy_of(name).wait()
            _, group, place = units[name]
            return ring.at[group, place]

        def ff_copies(step, group):
            cols = pl.multiple_of(step * chans, chans)
            return [
                pltpu.make_async_copy(f1.at[:, pl.ds(cols, chans)], ring.at[group, 0], rsem.at[group, 0]),
                pltpu.make_async_copy(f1.at[:, pl.ds(cols + ff_steps * chans, chans)], ring.at[group, 1], rsem.at[group, 1]),
                pltpu.make_async_copy(f2.at[pl.ds(cols, chans), :], ring.at[group, 2], rsem.at[group, 2]),
            ]

        start('in', 'q', 'k', 'v', 'co')

        tot, sqr = channel_sums(h_ref, tokens, chans)
        member = members(chans, groups)
        sums = group_sums(two_rows(tot, sqr), member)
        group_affine(sums, norm_ref[norm_row:norm_row + 1], norm_ref[norm_row + 1:norm_row + 2], member, count, coef, 1.0)

        def project_rows(weight, src, base, normed_to):
            def norm_tile(tile):
                rows = tile_rows(tile)
                normed_to[rows, :] = layer_norm(tok[rows, :].astype(F32))

            @pl.loop(0, tiles)
            def _(tile):
                norm_tile(jnp.maximum(tile - 1, 0))
                rows = tile_rows(tile)
                tok[rows, :] = (base(rows) + nn(src(rows), weight[...])).astype(BF16)

            norm_tile(tiles - 1)

        project_rows(take('in'), lambda rows: (h_ref[rows, :].astype(F32) * coef[0:1] + coef[1:2]).astype(BF16), lambda rows: 0.0, aux)

        q_t, v_t = both.at[0], both.at[1]

        def transposed(weight, src, dst, factor):
            @pl.loop(0, 2)
            def _(part):
                rows = pl.ds(pl.multiple_of(part * half, half), half)
                dst[rows, :] = (nt(weight[rows, :], src[...]).astype(BF16) * factor).astype(BF16)

        w_key = take('k')

        @pl.loop(0, tokens // 512)
        def _(part):
            rows = pl.ds(pl.multiple_of(part * 512, 512), 512)
            keys[rows, :] = nt(aux[rows, :], w_key[...]).astype(BF16)
        start('o')

        @pl.loop(0, 2)
        def _(which):
            pltpu.make_async_copy(wqkv.at[2 * which], ring.at[which, 1], rsem.at[which, 1]).wait()
            transposed(ring.at[which, 1], aux, both.at[which], jnp.where(which == 0, scale, 1.0))
        start('cq')
        for copy in ff_copies(0, 0):
            copy.start()

        row_head = lax.broadcasted_iota(jnp.int32, (pair, 1), 0) < head_dim

        def query_of(hp, first, wide, head):
            both = q_t[pl.ds(pl.multiple_of(hp * pair, pair), pair), pl.ds(first, wide)]
            keep = row_head if head == 0 else jnp.logical_not(row_head)
            return jnp.where(keep, both, jnp.zeros_like(both))

        def pair_cols(hp):
            return pl.ds(pl.multiple_of(hp * pair, pair), pair)

        halves = tokens // qw
        blocks = pairs * halves
        scores = [acc.at[:, pl.ds(h * qw, qw)] for h in range(2)]
        probs = [out_ref.at[:, pl.ds(h * qw, qw)] for h in range(2)]
        parts = tokens // kb

        def place(block):
            hp = lax.div(block, halves)
            return hp, pl.multiple_of((block - hp * halves) * qw, qw)

        def fold(vals, func):
            return func(vals.reshape(-1, 8, vals.shape[-1]), axis=0)

        def score_part(block, query, head, part):
            hp, _ = place(block)
            vals = nn(keys[part * kb:(part + 1) * kb, pair_cols(hp)], query)
            scores[head][part * kb:(part + 1) * kb, :] = vals
            return fold(vals, jnp.max)

        def exp_part(head, part, top):
            vals = jnp.exp(scores[head][part * kb:(part + 1) * kb, :] - top)
            probs[head][part * kb:(part + 1) * kb, :] = vals.astype(BF16)
            return fold(vals, jnp.sum)

        def value_of(block, head, denom):
            hp, _ = place(block)
            vals = v_t[pl.ds(pl.multiple_of(hp * pair + head * head_dim, head_dim), head_dim), :]
            return nn(vals, probs[head][...]) * (1.0 / denom)

        def block_query(block, head):
            hp, first = place(block)
            return query_of(hp, first, qw, head)

        def softmax_stage(score_block, score_head, exp_head, top):
            tops, sums = [], []
            query = block_query(score_block, score_head)
            for part in range(parts):
                tops.append(score_part(score_block, query, score_head, part))
                sums.append(exp_part(exp_head, part, top))
            new_top = jnp.max(functools.reduce(jnp.maximum, tops), axis=0, keepdims=True)
            return new_top, jnp.sum(functools.reduce(jnp.add, sums), axis=0, keepdims=True)

        def emit(block, low, high):
            hp, first = place(block)
            aux[pl.ds(first, qw), pair_cols(hp)] = jnp.concatenate([low, high], axis=0).T.astype(BF16)

        top_first = jnp.max(functools.reduce(jnp.maximum, [score_part(0, block_query(0, 0), 0, part) for part in range(parts)]), axis=0, keepdims=True)
        zero_row = jnp.ones((1, qw), F32)
        zero_out = jnp.zeros((head_dim, qw), F32)

        def attend_block(block, carry):
            top0, denom1, low = carry
            before = jnp.maximum(block - 1, 0)
            high = value_of(before, 1, denom1)
            emit(before, low, high)
            top1, denom0 = softmax_stage(block, 1, 0, top0)
            after = jnp.minimum(block + 1, blocks - 1)
            low = value_of(block, 0, denom0)
            top0, denom1 = softmax_stage(after, 0, 1, top1)
            return top0, denom1, low

        def attend_blocks(step, carry):
            for sub in range(4):
                carry = attend_block(step * 4 + sub, carry)
            return carry

        _, denom1, low = lax.fori_loop(0, blocks // 4, attend_blocks, (top_first, zero_row, zero_out))
        emit(blocks - 1, low, value_of(blocks - 1, 1, denom1))

        project_rows(take('o'), lambda rows: aux[rows, :], lambda rows: tok[rows, :].astype(F32), keys)
        transposed(take('cq'), keys, q_t, scale)

        text_valid = lax.broadcasted_iota(jnp.int32, (text_rows, 1), 0) < text

        wide_step = max(count for count in (CROSS_PAIRS, 2, 1) if pairs % count == 0)

        @pl.loop(0, pairs // wide_step)
        def _(step):
            for sub in range(wide_step):
                hp = step * wide_step + sub
                outs = []
                for head in range(2):
                    vals = nn(ctx_k[:, pair_cols(hp)], query_of(hp, 0, tokens, head))
                    vals = jnp.where(text_valid, vals, -jnp.inf)
                    weights = jnp.exp(vals - jnp.max(vals, axis=0, keepdims=True))
                    denom = jnp.sum(weights, axis=0, keepdims=True)
                    text_vals = ctx_v[pl.ds(pl.multiple_of(hp * pair + head * head_dim, head_dim), head_dim), :]
                    outs.append(nn(text_vals, weights.astype(BF16)) * (1.0 / denom))
                aux[:, pair_cols(hp)] = jnp.concatenate(outs, axis=0).T.astype(BF16)

        project_rows(take('co'), lambda rows: aux[rows, :], lambda rows: tok[rows, :].astype(F32), keys)
        for copy in ff_copies(1, 1):
            copy.start()
        acc[...] = jnp.zeros_like(acc)

        @pl.loop(0, ff_steps)
        def _(step):
            group = lax.rem(step, 2)
            for copy in ff_copies(step, group):
                copy.wait()

            @pl.loop(0, tiles, unroll=2)
            def _(tile):
                rows = tile_rows(tile)
                src = keys[rows, :]
                value = nn(src, ring[group, 0])
                gate = nn(src, ring[group, 1])
                gated = (value * (0.5 * gate * (1.0 + lax.erf(gate * (0.5 ** 0.5))))).astype(BF16)
                acc[rows, :] += nn(gated, ring[group, 2])

            @pl.when(step + 2 < ff_steps)
            def _():
                for copy in ff_copies(step + 2, group):
                    copy.start()

            @pl.when(step == ff_steps - 2)
            def _():
                start('out')

        w_fin = take('out')

        @pl.loop(0, tiles)
        def _(tile):
            rows = tile_rows(tile)
            t = (tok[rows, :].astype(F32) + acc[rows, :]).astype(BF16)
            out_ref[rows, :] = (h_ref[rows, :].astype(F32) + nn(t, w_fin[...])).astype(BF16)

    vmem = pl.BlockSpec(memory_space=pltpu.VMEM)
    hbm = pl.BlockSpec(memory_space=pl.ANY)
    flops = 2 * tokens * chans * chans * (8 + 3 * ff_steps) + 4 * tokens * tokens * chans
    return pl.pallas_call(
        kernel,
        out_shape=jax.ShapeDtypeStruct(hidden.shape, BF16),
        in_specs=[vmem] * 4 + [hbm] * 7,
        out_specs=vmem,
        scratch_shapes=[
            pltpu.VMEM((2, 3, chans, chans), BF16),
            pltpu.VMEM((tokens, chans), BF16),
            pltpu.VMEM((tokens, chans), BF16),
            pltpu.VMEM((2, chans, tokens), BF16),
            pltpu.VMEM((tokens, chans), BF16),
            pltpu.VMEM((tokens, chans), F32),
            pltpu.VMEM((8, chans), F32),
            pltpu.SemaphoreType.DMA((2, 3)),
        ],
        compiler_params=pltpu.CompilerParams(vmem_limit_bytes=49000000),
        cost_estimate=cost_of(flops, 50 * chans * chans),
        name='transformer',
    )(hidden, ctx_keys, ctx_vals, norms, proj_inout, qkv_t, self_out, cross_q_t, cross_out, ff_in, ff_out)


def solution(mesh):
    num_bands = mesh.shape['sp']

    def local_stage(latent, time_emb, context, res_conv, res_time, res_norm, attn_norm, proj_inout, self_qkv, self_out, cross_q, cross_kv, cross_out, ff_in, ff_out):
        images, band_rows, width, chans = latent.shape
        assert images == num_bands
        band = band_rows * width
        heads, head_dim = self_out.shape[:2]
        groups = res_norm.shape[3]
        text, text_dim = context.shape[1:]
        flat_kv = jnp.transpose(cross_kv, (0, 2, 3, 1)).reshape(2, chans, text_dim)
        first, norms, bias, ctx_keys, ctx_vals = res_block_in(
            latent.reshape(images, band, chans), time_emb, jnp.transpose(context, (1, 0, 2)).reshape(text * images, text_dim), res_conv, res_time,
            res_norm.reshape((-1,) + res_norm.shape[3:]), attn_norm, flat_kv, text, width)
        middle = transformer(
            first, ctx_keys, ctx_vals, norms, res_norm.shape[0] * res_norm.shape[1] * res_norm.shape[2], proj_inout,
            jnp.transpose(self_qkv, (0, 2, 3, 1)).reshape(3, chans, chans),
            self_out.reshape(chans, chans),
            jnp.transpose(cross_q, (1, 2, 0)).reshape(chans, chans),
            cross_out.reshape(chans, chans), ff_in, ff_out, groups, heads, text)
        out = res_block_out(middle, bias, res_conv, norms, width, groups, num_bands)
        return out.reshape(latent.shape)

    band_spec = P('dp', 'sp', None, None)
    shared = P()
    in_specs = (band_spec, P('dp', None), P('dp', None, None)) + (shared,) * 12
    return jax.shard_map(local_stage, mesh=mesh, in_specs=in_specs, out_specs=band_spec, check_vma=False)
```

```python
import functools

import jax
import jax.numpy as jnp
from jax import lax
from jax.experimental import pallas as pl
from jax.experimental.pallas import tpu as pltpu
from jax.sharding import PartitionSpec as P

BF16 = jnp.bfloat16
F32 = jnp.float32
MESH = pl.DeviceIdType.MESH
GN_EPS = 1e-6
LN_EPS = 1e-5
TM = 256
CK = 256
LANES = 128
ROWS = 8
STEP = 64
CROSS_PAIRS = 5
VMEM_LIMIT = 67_000_000


def loop(stop, **options):
    return pl.loop(0, stop, **options)


def one_hot(mask):
    return mask.astype(F32).astype(BF16)


def nn(lhs, rhs):
    return jnp.dot(lhs, rhs, preferred_element_type=F32)


def nt(lhs, rhs):
    return lax.dot_general(lhs, rhs, (((1,), (1,)), ((), ())), preferred_element_type=F32)


def split3(vals):
    high = vals.astype(BF16).astype(F32)
    rest = vals - high
    mid = rest.astype(BF16).astype(F32)
    return [high, mid, rest - mid]


def channel_sums(src, rows, chans):
    def step(idx, carry):
        tot, sqr = carry
        vals = src[pl.ds(pl.multiple_of(idx * STEP, STEP), STEP), :].astype(F32).reshape(ROWS, ROWS, chans)
        return tot + jnp.sum(vals, axis=0), sqr + jnp.sum(vals * vals, axis=0)

    zero = jnp.zeros((ROWS, chans), F32)
    return lax.fori_loop(0, rows // STEP, step, (zero, zero))


def layer_norm(tokens):
    centred = tokens - jnp.mean(tokens, axis=-1, keepdims=True)
    return (centred * lax.rsqrt(jnp.mean(centred * centred, axis=-1, keepdims=True) + LN_EPS)).astype(BF16)


def meet(peers, me):
    barrier = pltpu.get_barrier_semaphore()

    @pl.loop(1, peers)
    def _(step):
        pl.semaphore_signal(barrier, inc=1, device_id={'sp': lax.rem(me + step, peers)}, device_id_type=MESH)


def await_peers(peers):
    pl.semaphore_wait(pltpu.get_barrier_semaphore(), peers - 1)


def drain(ref, sem):
    pltpu.make_async_copy(ref, ref, sem).wait()


def remote(src, dst, send_sem, recv_sem, peer):
    return pltpu.make_async_remote_copy(src, dst, send_sem, recv_sem, device_id={'sp': peer}, device_id_type=MESH)


def chunk_cols(chunk):
    return pl.ds(pl.multiple_of(chunk * CK, CK), CK)


def tile_rows(tile, first=0):
    return pl.ds(pl.multiple_of(first + tile * TM, 32), TM)


def members(chans, groups, offset=0):
    width = chans // groups
    chan = lax.broadcasted_iota(jnp.int32, (chans, LANES), 0)
    low = (lax.broadcasted_iota(jnp.int32, (chans, LANES), 1) - offset) * width
    return one_hot((chan >= low) & (chan < low + width))


def group_sums(rows, member):
    count = rows.shape[0]
    high, mid, low = split3(rows)
    sums = nn(jnp.concatenate([high, mid, low], axis=0).astype(BF16), member)
    return sums[0:count] + sums[count:2 * count] + sums[2 * count:3 * count]


def group_affine(sums, gain, shift, member, count, coef, factor):
    mean = sums[0:1] / count
    rstd = lax.rsqrt(sums[1:2] / count - mean * mean + GN_EPS)
    back = jnp.concatenate(split3(mean) + split3(rstd) + [jnp.zeros((2, LANES), F32)], axis=0).astype(BF16)
    wide = nt(back, member)
    scale = jnp.sum(wide[3:6], axis=0, keepdims=True) * gain
    coef[0:1, :] = factor * scale
    coef[1:2, :] = factor * (shift - jnp.sum(wide[:3], axis=0, keepdims=True) * scale)


def row_sums(tot, sqr):
    return [jnp.sum(tot, axis=0, keepdims=True), jnp.sum(sqr, axis=0, keepdims=True)]


def eight_rows(rows):
    return jnp.concatenate(rows + [jnp.zeros((ROWS - len(rows), rows[0].shape[1]), F32)], axis=0)


class Pair:
    def __init__(self, peers, band, width):
        self.chips, self.band, self.width = peers // 2, band, width
        self.half, self.sub = self.chips // 2, 2 * band
        self.rows = self.half * self.sub
        self.me = lax.axis_index('sp')
        self.chip, self.core = lax.div(self.me, 2), lax.rem(self.me, 2)
        self.base, self.side, _ = self.seat(self.me)
        self.partner = self.device(self.base, 1 - self.side, self.core)
        self.owners = [self.device(self.base, slot, self.core) for slot in range(2)]

    def seat(self, device):
        chip, core = lax.div(device, 2), lax.rem(device, 2)
        side = lax.div(lax.rem(chip + self.chips - 2 * core, 4), 2)
        return lax.rem(chip - 2 * side + self.chips, self.chips), side, core

    def device(self, base, side, core):
        return 2 * lax.rem(base + 2 * side, self.chips) + core

    def first_chip(self, base, slot, side):
        return lax.rem(base + slot + 1 + (side + 1) * self.half, self.chips)

    def block_chip(self, slot, index, side=None):
        return lax.rem(self.first_chip(self.base, slot, self.side if side is None else side) + index, self.chips)

    def block_rows(self, index):
        return pl.ds(pl.multiple_of(self.width + index * self.sub, self.width), self.sub)

    def border(self, slot):
        return lax.rem(self.chips - self.block_chip(slot, 0), self.chips)

    def spot(self, slot, index):
        return self.width + index * self.sub + jnp.where(index >= self.border(slot), self.width, 0)

    def last_spot(self, slot):
        return self.width + self.rows + jnp.where(self.half >= self.border(slot), self.width, 0)

    def act_shape(self, chans):
        return (2, 3, self.rows + 3 * self.width, chans)

    def clear_border(self, act):
        for slot in range(2):
            @pl.when(self.half >= self.border(slot))
            def _():
                row = pl.ds(pl.multiple_of(self.width + self.border(slot) * self.sub, self.width), self.width)
                act[slot, :, row, :] = jnp.zeros((3, self.width, act.shape[3]), BF16)

    def build(self, src, act, coef, slot, first):
        def part(row, put, count):
            activate(src.at[slot], act.at[slot], coef.at[slot], pl.ds(first, CK), row, put, count, self.width)

        part(0, 0, self.width)
        part(self.width + self.rows, self.last_spot(slot), self.width)

        @loop(self.half)
        def _(index):
            part(self.width + index * self.sub, self.spot(slot, index), self.sub)

    def build_all(self, src, act, coef, slot):
        @loop(act.shape[3] // CK)
        def _(chunk):
            self.build(src, act, coef, slot, pl.multiple_of(chunk * CK, CK))

    def shifted(self, act, slot, tile, dy, dx, cols):
        blocks = TM // self.sub
        rows = [self.spot(slot, blocks * tile + index) + (dy - 1) * self.width for index in range(blocks)]
        return jnp.concatenate([act[slot, dx, pl.ds(pl.multiple_of(row, self.width), self.sub), cols] for row in rows], axis=0)

    def tiles(self, body, order=None):
        per = self.rows // TM

        @loop(2 * per if order is None else per)
        def _(step):
            body(lax.div(step, per) if order is None else order, lax.rem(step, per))

    def acc_rows(self, slot, tile):
        return pl.ds(pl.multiple_of(slot * self.rows + tile * TM, TM), TM)

    def swap_norm(self, mid, acc, bias, sums, member, norm_ref, row, count, coef, send_sem, recv_sem):
        copies, rows = [], []
        for slot in range(2):
            def step(idx, carry):
                first = pl.multiple_of(idx * STEP, STEP)
                rounded = (acc[pl.ds(first + slot * self.rows, STEP), :] + bias[slot:slot + 1, :]).astype(BF16)
                mid[slot, pl.ds(first + self.width, STEP), :] = rounded
                vals = rounded.astype(F32).reshape(ROWS, ROWS, acc.shape[1])
                return carry[0] + jnp.sum(vals, axis=0), carry[1] + jnp.sum(vals * vals, axis=0)

            zero = jnp.zeros((ROWS, acc.shape[1]), F32)
            rows += row_sums(*lax.fori_loop(0, self.rows // STEP, step, (zero, zero)))
            for here, there in ((self.width, self.width + self.rows), (self.rows, 0)):
                index = len(copies)
                copies.append(remote(mid.at[slot, pl.ds(here, self.width), :], mid.at[slot, pl.ds(there, self.width), :], send_sem.at[index], recv_sem.at[index], self.partner))
                copies[-1].start()
        sums[0] = group_sums(eight_rows(rows), member)
        copies.append(remote(sums.at[0], sums.at[1], send_sem.at[len(copies)], recv_sem.at[len(copies)], self.partner))
        copies[-1].start()
        wait_all(copies)
        total = sums[0] + sums[1]
        for slot in range(2):
            group_affine(total[2 * slot:2 * slot + 2], norm_ref[row:row + 1], norm_ref[row + 1:row + 2], member, count, coef.at[slot], 0.5)


def activate(src, act, coef, cols, row, put, count, width):
    half = src[pl.ds(pl.multiple_of(row, width), count), cols].astype(F32) * coef[0:1, cols] + coef[1:2, cols]
    vals = half + half * jnp.tanh(half)
    column = lax.rem(lax.broadcasted_iota(jnp.int32, vals.shape, 0), width)
    rows = pl.ds(pl.multiple_of(put, width), count)
    act[0, rows, cols] = jnp.where(column == 0, 0.0, pltpu.roll(vals, 1, 0)).astype(BF16)
    act[1, rows, cols] = vals.astype(BF16)
    act[2, rows, cols] = jnp.where(column == width - 1, 0.0, pltpu.roll(vals, count - 1, 0)).astype(BF16)


def taps():
    return [(dy, dx) for dy in range(3) for dx in range(3)]


def fetch_rows(kern, which, conv, chunk, wbuf, sem):
    slot = lax.rem(chunk, 2)
    return [pltpu.make_async_copy(kern.at[which, conv, dy, dx, chunk_cols(chunk), :], wbuf.at[slot, pl.ds(tap * CK, CK), :], sem.at[slot])
            for tap, (dy, dx) in enumerate(taps())]


def fetch_cols(kern, which, conv, chunk, wbuf, sem):
    slot = lax.rem(chunk, 2)
    return [pltpu.make_async_copy(kern.at[which, conv, dy, dx, :, chunk_cols(chunk)], wbuf.at[slot, tap], sem.at[slot])
            for tap, (dy, dx) in enumerate(taps())]


def start_all(copies):
    for copy in copies:
        copy.start()


def wait_all(copies):
    for copy in copies:
        copy.wait()


def chunk_product(pair, act, wbuf, chunk, slot, tile):
    cols = chunk_cols(chunk)
    return sum(nn(pair.shifted(act, slot, tile, dy, dx, cols), wbuf[lax.rem(chunk, 2), tap * CK:(tap + 1) * CK, :]) for tap, (dy, dx) in enumerate(taps()))


def column_product(pair, act, cbuf, chunk, slot, tile):
    return sum(nn(pair.shifted(act, slot, tile, dy, dx, slice(None)), cbuf[lax.rem(chunk, 2), tap]) for tap, (dy, dx) in enumerate(taps()))


def conv_columns(pair, kern, which, image, mid, act, cbuf, csem, coef, lead, emit):
    chunks = act.shape[3] // CK
    pair.build_all(mid, act, coef, lead)

    @loop(chunks)
    def _(chunk):
        @pl.when(chunk + 1 < chunks)
        def _():
            start_all(fetch_cols(kern, which, 1, chunk + 1, cbuf, csem))

        wait_all(fetch_cols(kern, which, 1, chunk, cbuf, csem))
        cols = chunk_cols(chunk)

        @loop(2)
        def _(turn):
            slot = lax.rem(lead + turn, 2)

            @pl.when((chunk == 0) & (turn == 1))
            def _():
                pair.build_all(mid, act, coef, slot)

            def body(slot, tile):
                rows = pl.ds(pl.multiple_of(pair.width + tile * TM, pair.width), TM)
                emit(slot, tile, rows, cols, (image[slot, rows, cols].astype(F32) + column_product(pair, act, cbuf, chunk, slot, tile)).astype(BF16))

            pair.tiles(body, slot)


def time_copy(res_time, which, wbuf, sem):
    return pltpu.make_async_copy(res_time.at[which], wbuf.at[1, pl.ds(0, res_time.shape[1]), :], sem)


def time_project(time_ref, wbuf, tproj):
    emb = time_ref[...].astype(F32)
    act = (emb / (1.0 + jnp.exp(-emb))).astype(BF16)
    tproj[...] = nn(act, wbuf[1, 0:act.shape[1], :])


def widen(param, chans):
    groups, width = param.shape
    group = lax.broadcasted_iota(jnp.int32, (groups, chans), 0) * width
    chan = lax.broadcasted_iota(jnp.int32, (groups, chans), 1)
    spread = one_hot((chan >= group) & (chan < group + width))
    wide = lax.dot_general(param, spread, (((0,), (0,)), ((), ())), preferred_element_type=F32)
    place = lax.broadcasted_iota(jnp.int32, (width, chans), 0)
    inside = lax.rem(lax.broadcasted_iota(jnp.int32, (width, chans), 1), width)
    return jnp.sum(jnp.where(place == inside, wide, 0.0), axis=0, keepdims=True)


def res_block_in(latent, time_emb, context, res_conv, res_time, res_norm, attn_norm, cross_kv, text, width):
    which, other = 0, 1
    peers, band, chans = latent.shape
    groups = res_norm.shape[1]
    text_dim = context.shape[1]
    text_rows = -(-text // 16) * 16
    block_norms = res_norm.shape[0]
    tokens = peers * band
    chunks = chans // CK
    count = float(tokens * (chans // groups))
    ctx_half = text_dim // 2

    def kernel(lat, time_hbm, ctx_hbm, kern, wtime, norm_hbm, attn_hbm, ckv, out_ref, norm_ref, bias_ref, ctx_k, ctx_v,
               image, mid, act, wbuf, cbuf, acc, time_ref, tproj, rows, bias, mine, stats, sums, coef, norm_raw, attn_raw, ctx_mine,
               wsem, csem, tsem, own_sem, small_sem, ctx_sem, send_sem, side_sem, recv_sem, stat_send, stat_recv, swap_send, swap_recv, give_send, give_recv):
        pair = Pair(peers, band, width)
        me = pair.me

        def own_rows(peer):
            return mid.at[lax.div(peer, pair.chips), pl.ds(pl.multiple_of(lax.rem(peer, pair.chips) * band, band), band), :]

        def load(peer):
            return pltpu.make_async_copy(lat.at[peer], own_rows(peer), own_sem)

        loop(peers)(lambda peer: load(peer).start())
        small = [pltpu.make_async_copy(src, dst, small_sem.at[index]) for index, (src, dst) in enumerate(((time_hbm, time_ref), (norm_hbm, norm_raw), (attn_hbm, attn_raw)))]
        start_all(small)
        weight = time_copy(wtime, which, wbuf, tsem)
        weight.start()
        start_all(fetch_rows(kern, which, 0, 0, wbuf, wsem))
        depth = act.shape[2]
        ctx_parts = [(part, piece, first, min(depth, text * peers - first)) for part in range(2) for piece, first in enumerate(range(0, text * peers, depth))]
        load_ctx = [pltpu.make_async_copy(ctx_hbm.at[pl.ds(first, size), pl.ds(part * ctx_half, ctx_half)], act.at[part, piece, pl.ds(0, size), pl.ds(0, ctx_half)], ctx_sem.at[0])
                    for part, piece, first, size in ctx_parts]
        start_all(load_ctx)
        load_kv = [pltpu.make_async_copy(ckv.at[index, :, pl.ds(part * CK, CK)], cbuf.at[index, part], ctx_sem.at[1]) for index in range(2) for part in range(text_dim // CK)]
        start_all(load_kv)
        meet(peers, me)
        member = members(chans, groups)
        await_peers(peers)

        def send(index):
            cols = chunk_cols(index)

            @loop(peers)
            def _(step):
                owner = lax.rem(me + step, peers)
                base, slot, core = pair.seat(owner)
                place = lax.rem(pair.chip - pair.first_chip(base, slot, 0) + pair.chips, pair.chips)
                side = lax.div(place, pair.half)
                place = place - side * pair.half
                near, far = pair.device(base, side, core), pair.device(base, 1 - side, core)
                src = lat.at[owner, :, cols]
                dst = image.at[slot, pl.ds(pl.multiple_of(width + place * pair.sub + pair.core * band, width), band), cols]

                @pl.when(near == me)
                def _():
                    pltpu.make_async_copy(src, dst, recv_sem.at[index]).start()

                @pl.when(near != me)
                def _():
                    remote(src, dst, send_sem, recv_sem.at[index], near).start()

                @pl.when((pair.core == 1) & (place == pair.half - 1))
                def _():
                    remote(lat.at[owner, pl.ds(band - width, width), cols], image.at[slot, pl.ds(0, width), cols], side_sem, recv_sem.at[index], far).start()

                @pl.when((pair.core == 0) & (place == 0))
                def _():
                    remote(lat.at[owner, pl.ds(0, width), cols], image.at[slot, pl.ds(width + pair.rows, width), cols], side_sem, recv_sem.at[index], far).start()

        send(0)
        loop(peers)(lambda peer: load(peer).wait())

        @loop(peers)
        def _(peer):
            vals = own_rows(peer)[...].astype(F32).reshape(band // ROWS, ROWS, chans)
            for part, total in enumerate((vals, vals * vals)):
                rows[pl.ds(part * peers + peer, 1), :] = jnp.sum(jnp.sum(total, axis=0), axis=0, keepdims=True)

        found = group_sums(rows[...], member)
        for peer in range(peers):
            mine[peer, 0:1, :] = found[peer:peer + 1]
            mine[peer, 1:2, :] = found[peers + peer:peers + peer + 1]

        @pl.loop(1, peers)
        def _(step):
            peer = lax.rem(me + step, peers)
            base, _, core = pair.seat(peer)
            for slot in range(2):
                remote(mine.at[pair.device(base, slot, core)], stats.at[me, slot], stat_send, stat_recv, peer).start()

        pl.loop(1, chunks)(send)
        for slot in range(2):
            stats[me, slot] = mine[pair.owners[slot]]
        wait_all(small)
        for index in range(block_norms):
            norm_ref[index:index + 1, :] = widen(norm_raw[index], chans)
        for index in range(2):
            norm_ref[block_norms + index:block_norms + index + 1, :] = widen(attn_raw[index], chans)

        def time_rows(dst, copy):
            copy.wait()
            time_project(time_ref, wbuf, tproj)
            for slot in range(2):
                dst[slot:slot + 1, :] = tproj[pl.ds(pair.owners[slot], 1), :]

        time_rows(bias, weight)
        weight = time_copy(wtime, other, wbuf, tsem)
        weight.start()
        acc[...] = jnp.zeros_like(acc)
        wait_all(load_ctx)
        for part in range(2):
            total = 0.0
            for this, piece, first, size in ctx_parts:
                if this == part:
                    place = (text_rows, size)
                    wanted = lax.broadcasted_iota(jnp.int32, place, 0) * peers + (me - first)
                    pick = one_hot(lax.broadcasted_iota(jnp.int32, place, 1) == wanted)
                    total += nn(pick, act[part, piece, 0:size, 0:ctx_half])
            ctx_mine[:, part * ctx_half:(part + 1) * ctx_half] = total.astype(BF16)
        wait_all(load_kv)
        ctx_k[...] = sum(nt(ctx_mine[:, part * CK:(part + 1) * CK], cbuf[0, part]) for part in range(text_dim // CK)).astype(BF16)

        @loop(chans // CK)
        def _(block):
            part_rows = pl.ds(pl.multiple_of(block * CK, CK), CK)
            ctx_v[part_rows, :] = sum(nt(cbuf[1, part, part_rows, :], ctx_mine[:, part * CK:(part + 1) * CK]) for part in range(text_dim // CK)).astype(BF16)

        time_rows(bias_ref, weight)
        pair.clear_border(act)
        others = stats.at[pl.ds(0, peers - 1)]
        drain(others, stat_recv)
        drain(others, stat_send)
        row = 4 * which
        for slot in range(2):
            group_affine(jnp.sum(stats[:, slot], axis=0), norm_ref[row:row + 1], norm_ref[row + 1:row + 2], member, count, coef.at[slot], 0.5)

        @loop(chunks)
        def _(chunk):
            @pl.when(chunk + 1 < chunks)
            def _():
                start_all(fetch_rows(kern, which, 0, chunk + 1, wbuf, wsem))

            wait_all(fetch_rows(kern, which, 0, chunk, wbuf, wsem))
            drain(image.at[:, :, chunk_cols(chunk)], recv_sem.at[chunk])

            @loop(2)
            def _(slot):
                pair.build(image, act, coef, slot, pl.multiple_of(chunk * CK, CK))

            def body(slot, tile):
                acc[pair.acc_rows(slot, tile), :] += chunk_product(pair, act, wbuf, chunk, slot, tile)

            pair.tiles(body)

        start_all(fetch_cols(kern, which, 1, 0, cbuf, csem))
        pair.swap_norm(mid, acc, bias, sums, member, norm_ref, row + 2, count, coef, swap_send, swap_recv)
        give = 1 - pair.side

        def emit(slot, tile, place, cols, vals):
            blocks = TM // pair.sub
            spots = [pl.ds(pl.multiple_of(pair.block_chip(slot, blocks * tile + index) * pair.sub, pair.sub), pair.sub) for index in range(blocks)]

            @pl.when(slot == give)
            def _():
                image[slot, place, cols] = vals
                for index, spot in enumerate(spots):
                    remote(image.at[slot, pair.block_rows(blocks * tile + index), cols], out_ref.at[spot, cols], give_send, give_recv, pair.partner).start()

            @pl.when(slot != give)
            def _():
                for index, spot in enumerate(spots):
                    out_ref[spot, cols] = vals[index * pair.sub:(index + 1) * pair.sub]

        conv_columns(pair, kern, which, image, mid, act, cbuf, csem, coef, give, emit)
        for sem in (give_send, give_recv):
            drain(out_ref.at[pl.ds(0, pair.rows)], sem)
        drain(lat.at[pl.ds(0, peers - 2)], send_sem)
        drain(lat.at[0:2], side_sem)

    vmem = pl.BlockSpec(memory_space=pltpu.VMEM)
    hbm = pl.BlockSpec(memory_space=pl.ANY)
    dma = pltpu.SemaphoreType.DMA
    rows = tokens // 2
    return pl.pallas_call(
        kernel,
        out_shape=[
            jax.ShapeDtypeStruct((tokens, chans), BF16),
            jax.ShapeDtypeStruct((block_norms + ROWS, chans), F32),
            jax.ShapeDtypeStruct((2, chans), F32),
            jax.ShapeDtypeStruct((text_rows, chans), BF16),
            jax.ShapeDtypeStruct((chans, text_rows), BF16),
        ],
        in_specs=[hbm] * ROWS,
        out_specs=[vmem] * 5,
        scratch_shapes=shared_scratch(rows, width, chans) + [
            pltpu.VMEM(time_emb.shape, BF16),
            pltpu.VMEM((peers, chans), F32),
            pltpu.VMEM((2 * peers, chans), F32),
            pltpu.VMEM((2, chans), F32),
            pltpu.VMEM((peers, 2, LANES), F32),
            pltpu.VMEM((peers, 2, 2, LANES), F32),
            pltpu.VMEM((2, ROWS, LANES), F32),
            pltpu.VMEM((2, ROWS, chans), F32),
            pltpu.VMEM(res_norm.shape, BF16),
            pltpu.VMEM(attn_norm.shape, BF16),
            pltpu.VMEM((text_rows, text_dim), BF16),
            dma((2,)), dma((2,)), dma, dma, dma((3,)), dma((2,)), dma, dma, dma((chunks,)), dma, dma, dma((5,)), dma((5,)), dma, dma,
        ],
        compiler_params=pltpu.CompilerParams(vmem_limit_bytes=53000000, collective_id=0, has_side_effects=True),
        cost_estimate=cost_of(36 * tokens * chans * chans, 36 * chans * chans),
        name='res_block_in',
    )(latent, time_emb, context, res_conv, res_time, res_norm, attn_norm, cross_kv)


def shared_scratch(rows, width, chans):
    beside = rows + 2 * width
    return [
        pltpu.VMEM((2, beside, chans), BF16),
        pltpu.VMEM((2, beside, chans), BF16),
        pltpu.VMEM((2, 3, beside + width, chans), BF16),
        pltpu.VMEM((2, len(taps()) * CK, chans), BF16),
        pltpu.VMEM((2, len(taps()), chans, CK), BF16),
        pltpu.VMEM((2 * rows, chans), F32),
    ]


def res_block_out(hidden, bias, res_conv, norms, width, groups, peers):
    which = 1
    tokens, chans = hidden.shape
    band = tokens // peers
    chunks = chans // CK
    count = float(tokens * (chans // groups))

    def kernel(hid, bias_ref, kern, norm_ref, out_ref, image, mid, act, wbuf, cbuf, acc, owned, sums, coef,
               wsem, csem, give_send, give_recv, tell_send, tell_recv, swap_send, swap_recv, send_sem, recv_sem):
        pair = Pair(peers, band, width)
        me, side = pair.me, pair.side
        start_all(fetch_rows(kern, which, 0, 0, wbuf, wsem))
        meet(peers, me)
        pair.clear_border(act)
        member = members(chans, groups)

        def pieces(holder):
            def image_rows(index, offset, size):
                return pl.ds(pl.multiple_of(lax.rem(pair.block_chip(side, index, holder) * pair.sub + offset, tokens), width), size)

            return [(image_rows(index, 0, pair.sub), pair.block_rows(index)) for index in range(pair.half)] + [
                (image_rows(0, tokens - width, width), pl.ds(0, width)), (image_rows(pair.half, 0, width), pl.ds(width + pair.rows, width))]

        await_peers(peers)

        @loop(chunks)
        def _(chunk):
            cols = chunk_cols(chunk)
            for src, dst in pieces(1 - side):
                remote(hid.at[src, cols], image.at[side, dst, cols], give_send, give_recv.at[chunk], pair.partner).start()

        owned[side] = group_sums(eight_rows(row_sums(*channel_sums(hid, tokens, chans))), member)
        tell = remote(owned.at[side], owned.at[side], tell_send, tell_recv, pair.partner)
        tell.start()
        for src, dst in pieces(side):
            image[side, dst, :] = hid[src, :]
        acc[...] = jnp.zeros_like(acc)
        tell.wait()
        row = 4 * which
        for slot in range(2):
            group_affine(owned[slot, 0:2], norm_ref[row:row + 1], norm_ref[row + 1:row + 2], member, count, coef.at[slot], 0.5)

        @loop(chunks)
        def _(chunk):
            @pl.when(chunk + 1 < chunks)
            def _():
                start_all(fetch_rows(kern, which, 0, chunk + 1, wbuf, wsem))

            wait_all(fetch_rows(kern, which, 0, chunk, wbuf, wsem))

            @loop(2)
            def _(turn):
                slot = lax.rem(side + turn, 2)

                @pl.when(turn == 1)
                def _():
                    drain(image.at[1 - side, :, chunk_cols(chunk)], give_recv.at[chunk])

                pair.build(image, act, coef, slot, pl.multiple_of(chunk * CK, CK))

                def body(slot, tile):
                    acc[pair.acc_rows(slot, tile), :] += chunk_product(pair, act, wbuf, chunk, slot, tile)

                pair.tiles(body, slot)

        start_all(fetch_cols(kern, which, 1, 0, cbuf, csem))
        pair.swap_norm(mid, acc, bias_ref, sums, member, norm_ref, row + 2, count, coef, swap_send, swap_recv)

        def emit(slot, tile, place, cols, vals):
            image[slot, place, cols] = vals
            slab = pair.device(pair.base, slot, pair.core)
            blocks = TM // pair.sub
            for index in range(blocks):
                block = blocks * tile + index
                for core in range(2):
                    peer = 2 * pair.block_chip(slot, block) + core
                    src = image.at[slot, pl.ds(pl.multiple_of(width + block * pair.sub + core * band, width), band), cols]

                    @pl.when(peer == me)
                    def _():
                        out_ref[slab, :, cols] = src[...]

                    @pl.when(peer != me)
                    def _():
                        remote(src, out_ref.at[slab, :, cols], send_sem, recv_sem, peer).start()

        conv_columns(pair, kern, which, image, mid, act, cbuf, csem, coef, side, emit)
        drain(image.at[0], give_send)
        others = out_ref.at[pl.ds(0, peers - 2)]
        drain(others, send_sem)
        drain(others, recv_sem)

    vmem = pl.BlockSpec(memory_space=pltpu.VMEM)
    hbm = pl.BlockSpec(memory_space=pl.ANY)
    dma = pltpu.SemaphoreType.DMA
    return pl.pallas_call(
        kernel,
        out_shape=jax.ShapeDtypeStruct((peers, band, chans), BF16),
        in_specs=[vmem, vmem, hbm, vmem],
        out_specs=vmem,
        scratch_shapes=shared_scratch(tokens // 2, width, chans) + [
            pltpu.VMEM((2, ROWS, LANES), F32),
            pltpu.VMEM((2, ROWS, LANES), F32),
            pltpu.VMEM((2, ROWS, chans), F32),
            dma((2,)), dma((2,)), dma, dma((chunks,)), dma, dma, dma((5,)), dma((5,)), dma, dma,
        ],
        compiler_params=pltpu.CompilerParams(vmem_limit_bytes=48000000, collective_id=1, has_side_effects=True),
        cost_estimate=cost_of(36 * tokens * chans * chans, 36 * chans * chans),
        name='res_block_out',
    )(hidden, bias, res_conv, norms)


def in_hbm(array):
    return pltpu.with_memory_space_constraint(array, pltpu.HBM)


def cost_of(flops, nbytes):
    return pl.CostEstimate(flops=flops, bytes_accessed=nbytes, transcendentals=0)


def transformer(hidden, ctx_keys, ctx_vals, norms, norm_row, proj_inout, qkv_t, self_out, cross_q_t, cross_out, ff_in, ff_out, groups, heads, text):
    tokens, chans = hidden.shape
    text_rows = ctx_keys.shape[0]
    head_dim = chans // heads
    pairs = heads // 2
    pair = 2 * head_dim
    count = float(tokens * (chans // groups))
    tiles = tokens // TM
    ff_steps = ff_out.shape[0] // chans
    qw = 512 if chans >= 1024 else CK
    kb = CK
    scale = head_dim ** -0.5
    half = chans // 2

    def kernel(h_ref, ctx_k, ctx_v, norm_ref, pio, wqkv, wo, cq, co, f1, f2, out_ref, ring, tok, aux, both, keys, acc, coef, rsem):
        units = {
            'in': (pio.at[0], 0, 0), 'q': (wqkv.at[0], 0, 1), 'k': (wqkv.at[1], 1, 0), 'v': (wqkv.at[2], 1, 1),
            'o': (wo, 1, 0), 'cq': (cq, 1, 1), 'co': (co, 1, 2), 'out': (pio.at[1], 0, 0),
        }

        def copy_of(name):
            src, group, place = units[name]
            return pltpu.make_async_copy(src, ring.at[group, place], rsem.at[group, place])

        def start(*names):
            for name in names:
                copy_of(name).start()

        def take(name):
            copy_of(name).wait()
            _, group, place = units[name]
            return ring.at[group, place]

        def ff_copies(step, group):
            cols = pl.multiple_of(step * chans, chans)
            return [
                pltpu.make_async_copy(f1.at[:, pl.ds(cols, chans)], ring.at[group, 0], rsem.at[group, 0]),
                pltpu.make_async_copy(f1.at[:, pl.ds(cols + ff_steps * chans, chans)], ring.at[group, 1], rsem.at[group, 1]),
                pltpu.make_async_copy(f2.at[pl.ds(cols, chans), :], ring.at[group, 2], rsem.at[group, 2]),
            ]

        start('in', 'q', 'k', 'v', 'co')

        tot, sqr = channel_sums(h_ref, tokens, chans)
        member = members(chans, groups)
        sums = group_sums(eight_rows(row_sums(tot, sqr)), member)
        group_affine(sums, norm_ref[norm_row:norm_row + 1], norm_ref[norm_row + 1:norm_row + 2], member, count, coef, 1.0)

        def project_rows(weight, src, base, normed_to):
            def norm_tile(tile):
                rows = tile_rows(tile)
                normed_to[rows, :] = layer_norm(tok[rows, :].astype(F32))

            @loop(tiles)
            def _(tile):
                norm_tile(jnp.maximum(tile - 1, 0))
                rows = tile_rows(tile)
                tok[rows, :] = (base(rows) + nn(src(rows), weight[...])).astype(BF16)

            norm_tile(tiles - 1)

        project_rows(take('in'), lambda rows: (h_ref[rows, :].astype(F32) * coef[0:1] + coef[1:2]).astype(BF16), lambda rows: 0.0, aux)

        q_t, v_t = both.at[0], both.at[1]

        def transposed(weight, src, dst, factor):
            @loop(2)
            def _(part):
                rows = pl.ds(pl.multiple_of(part * half, half), half)
                dst[rows, :] = (nt(weight[rows, :], src[...]).astype(BF16) * factor).astype(BF16)

        w_key = take('k')

        @loop(tokens // 512)
        def _(part):
            rows = pl.ds(pl.multiple_of(part * 512, 512), 512)
            keys[rows, :] = nt(aux[rows, :], w_key[...]).astype(BF16)
        start('o')

        @loop(2)
        def _(which):
            pltpu.make_async_copy(wqkv.at[2 * which], ring.at[which, 1], rsem.at[which, 1]).wait()
            transposed(ring.at[which, 1], aux, both.at[which], jnp.where(which == 0, scale, 1.0))
        start('cq')
        for copy in ff_copies(0, 0):
            copy.start()

        row_head = lax.broadcasted_iota(jnp.int32, (pair, 1), 0) < head_dim

        def query_of(hp, first, wide, head):
            both = q_t[pl.ds(pl.multiple_of(hp * pair, pair), pair), pl.ds(first, wide)]
            keep = row_head if head == 0 else jnp.logical_not(row_head)
            return jnp.where(keep, both, jnp.zeros_like(both))

        def pair_cols(hp):
            return pl.ds(pl.multiple_of(hp * pair, pair), pair)

        halves = tokens // qw
        blocks = pairs * halves
        scores = [acc.at[:, pl.ds(h * qw, qw)] for h in range(2)]
        probs = [out_ref.at[:, pl.ds(h * qw, qw)] for h in range(2)]
        parts = tokens // kb

        def place(block):
            hp = lax.div(block, halves)
            return hp, pl.multiple_of((block - hp * halves) * qw, qw)

        def fold(vals, func):
            return func(vals.reshape(-1, ROWS, vals.shape[-1]), axis=0)

        def score_part(block, query, head, part):
            hp, _ = place(block)
            vals = nn(keys[part * kb:(part + 1) * kb, pair_cols(hp)], query)
            scores[head][part * kb:(part + 1) * kb, :] = vals
            return fold(vals, jnp.max)

        def exp_part(head, part, top):
            vals = jnp.exp(scores[head][part * kb:(part + 1) * kb, :] - top)
            probs[head][part * kb:(part + 1) * kb, :] = vals.astype(BF16)
            return fold(vals, jnp.sum)

        def value_of(block, head, denom):
            hp, _ = place(block)
            vals = v_t[pl.ds(pl.multiple_of(hp * pair + head * head_dim, head_dim), head_dim), :]
            return nn(vals, probs[head][...]) * (1.0 / denom)

        def block_query(block, head):
            hp, first = place(block)
            return query_of(hp, first, qw, head)

        def softmax_stage(score_block, score_head, exp_head, top):
            tops, sums = [], []
            query = block_query(score_block, score_head)
            for part in range(parts):
                tops.append(score_part(score_block, query, score_head, part))
                sums.append(exp_part(exp_head, part, top))
            new_top = jnp.max(functools.reduce(jnp.maximum, tops), axis=0, keepdims=True)
            return new_top, jnp.sum(functools.reduce(jnp.add, sums), axis=0, keepdims=True)

        def emit(block, low, high):
            hp, first = place(block)
            aux[pl.ds(first, qw), pair_cols(hp)] = jnp.concatenate([low, high], axis=0).T.astype(BF16)

        top_first = jnp.max(functools.reduce(jnp.maximum, [score_part(0, block_query(0, 0), 0, part) for part in range(parts)]), axis=0, keepdims=True)
        zero_row = jnp.ones((1, qw), F32)
        zero_out = jnp.zeros((head_dim, qw), F32)

        def attend_block(block, carry):
            top0, denom1, low = carry
            before = jnp.maximum(block - 1, 0)
            high = value_of(before, 1, denom1)
            emit(before, low, high)
            top1, denom0 = softmax_stage(block, 1, 0, top0)
            after = jnp.minimum(block + 1, blocks - 1)
            low = value_of(block, 0, denom0)
            top0, denom1 = softmax_stage(after, 0, 1, top1)
            return top0, denom1, low

        def attend_blocks(step, carry):
            for sub in range(4):
                carry = attend_block(step * 4 + sub, carry)
            return carry

        _, denom1, low = lax.fori_loop(0, blocks // 4, attend_blocks, (top_first, zero_row, zero_out))
        emit(blocks - 1, low, value_of(blocks - 1, 1, denom1))

        project_rows(take('o'), lambda rows: aux[rows, :], lambda rows: tok[rows, :].astype(F32), keys)
        transposed(take('cq'), keys, q_t, scale)

        text_valid = lax.broadcasted_iota(jnp.int32, (text_rows, 1), 0) < text

        wide_step = max(count for count in (CROSS_PAIRS, 2, 1) if pairs % count == 0)

        @loop(pairs // wide_step)
        def _(step):
            for sub in range(wide_step):
                hp = step * wide_step + sub
                outs = []
                for head in range(2):
                    vals = nn(ctx_k[:, pair_cols(hp)], query_of(hp, 0, tokens, head))
                    vals = jnp.where(text_valid, vals, -jnp.inf)
                    weights = jnp.exp(vals - jnp.max(vals, axis=0, keepdims=True))
                    denom = jnp.sum(weights, axis=0, keepdims=True)
                    text_vals = ctx_v[pl.ds(pl.multiple_of(hp * pair + head * head_dim, head_dim), head_dim), :]
                    outs.append(nn(text_vals, weights.astype(BF16)) * (1.0 / denom))
                aux[:, pair_cols(hp)] = jnp.concatenate(outs, axis=0).T.astype(BF16)

        project_rows(take('co'), lambda rows: aux[rows, :], lambda rows: tok[rows, :].astype(F32), keys)
        for copy in ff_copies(1, 1):
            copy.start()
        acc[...] = jnp.zeros_like(acc)

        @loop(ff_steps)
        def _(step):
            group = lax.rem(step, 2)
            for copy in ff_copies(step, group):
                copy.wait()

            @loop(tiles, unroll=2)
            def _(tile):
                rows = tile_rows(tile)
                src = keys[rows, :]
                value = nn(src, ring[group, 0])
                gate = nn(src, ring[group, 1])
                gated = (value * (0.5 * gate * (1.0 + lax.erf(gate * (0.5 ** 0.5))))).astype(BF16)
                acc[rows, :] += nn(gated, ring[group, 2])

            @pl.when(step + 2 < ff_steps)
            def _():
                for copy in ff_copies(step + 2, group):
                    copy.start()

            @pl.when(step == ff_steps - 2)
            def _():
                start('out')

        w_fin = take('out')

        @loop(tiles)
        def _(tile):
            rows = tile_rows(tile)
            t = (tok[rows, :].astype(F32) + acc[rows, :]).astype(BF16)
            out_ref[rows, :] = (h_ref[rows, :].astype(F32) + nn(t, w_fin[...])).astype(BF16)

    vmem = pl.BlockSpec(memory_space=pltpu.VMEM)
    hbm = pl.BlockSpec(memory_space=pl.ANY)
    flops = 2 * tokens * chans * chans * (ROWS + 3 * ff_steps) + 4 * tokens * tokens * chans
    return pl.pallas_call(
        kernel,
        out_shape=jax.ShapeDtypeStruct(hidden.shape, BF16),
        in_specs=[vmem] * 4 + [hbm] * 7,
        out_specs=vmem,
        scratch_shapes=[
            pltpu.VMEM((2, 3, chans, chans), BF16),
            pltpu.VMEM((tokens, chans), BF16),
            pltpu.VMEM((tokens, chans), BF16),
            pltpu.VMEM((2, chans, tokens), BF16),
            pltpu.VMEM((tokens, chans), BF16),
            pltpu.VMEM((tokens, chans), F32),
            pltpu.VMEM((ROWS, chans), F32),
            pltpu.SemaphoreType.DMA((2, 3)),
        ],
        compiler_params=pltpu.CompilerParams(vmem_limit_bytes=50000000),
        cost_estimate=cost_of(flops, 50 * chans * chans),
        name='transformer',
    )(hidden, ctx_keys, ctx_vals, norms, proj_inout, qkv_t, self_out, cross_q_t, cross_out, ff_in, ff_out)


def solution(mesh):
    num_bands = mesh.shape['sp']

    def local_stage(latent, time_emb, context, res_conv, res_time, res_norm, attn_norm, proj_inout, self_qkv, self_out, cross_q, cross_kv, cross_out, ff_in, ff_out):
        images, band_rows, width, chans = latent.shape
        assert images == num_bands
        band = band_rows * width
        heads, head_dim = self_out.shape[:2]
        groups = res_norm.shape[3]
        text, text_dim = context.shape[1:]
        flat_kv = jnp.transpose(cross_kv, (0, 2, 3, 1)).reshape(2, chans, text_dim)
        first, norms, bias, ctx_keys, ctx_vals = res_block_in(
            latent.reshape(images, band, chans), in_hbm(time_emb), jnp.transpose(context, (1, 0, 2)).reshape(text * images, text_dim), res_conv, res_time,
            in_hbm(res_norm.reshape((-1,) + res_norm.shape[3:])), in_hbm(attn_norm), flat_kv, text, width)
        middle = transformer(
            first, ctx_keys, ctx_vals, norms, res_norm.shape[0] * res_norm.shape[1] * res_norm.shape[2], proj_inout,
            jnp.transpose(self_qkv, (0, 2, 3, 1)).reshape(3, chans, chans),
            self_out.reshape(chans, chans),
            jnp.transpose(cross_q, (1, 2, 0)).reshape(chans, chans),
            cross_out.reshape(chans, chans), ff_in, ff_out, groups, heads, text)
        out = res_block_out(middle, bias, res_conv, norms, width, groups, num_bands)
        return out.reshape(latent.shape)

    band_spec = P('dp', 'sp', None, None)
    shared = P()
    in_specs = (band_spec, P('dp', None), P('dp', None, None)) + (shared,) * 12
    return jax.shard_map(local_stage, mesh=mesh, in_specs=in_specs, out_specs=band_spec, check_vma=False)
```

```python
import functools

import jax
import jax.numpy as jnp
from jax import lax
from jax.experimental import pallas as pl
from jax.experimental.pallas import tpu as pltpu
from jax.sharding import PartitionSpec as P

BF16 = jnp.bfloat16
F32 = jnp.float32
MESH = pl.DeviceIdType.MESH
GN_EPS = 1e-6
LN_EPS = 1e-5
TM = 256
CK = 256
LANES = 128
ROWS = 8
STEP = 64
CROSS_PAIRS = 5
VMEM_IN, VMEM_MID, VMEM_OUT = 53_000_000, 48_000_000, 50_000_000


def loop(stop, **options):
    return pl.loop(0, stop, **options)


def keep_sum(vals):
    return jnp.sum(vals, axis=0, keepdims=True)


def one_hot(mask):
    return mask.astype(F32).astype(BF16)


def nn(lhs, rhs):
    return jnp.dot(lhs, rhs, preferred_element_type=F32)


def nt(lhs, rhs):
    return lax.dot_general(lhs, rhs, (((1,), (1,)), ((), ())), preferred_element_type=F32)


def split3(vals):
    high = vals.astype(BF16).astype(F32)
    rest = vals - high
    mid = rest.astype(BF16).astype(F32)
    return [high, mid, rest - mid]


def channel_sums(src, rows, chans):
    def step(idx, carry):
        tot, sqr = carry
        vals = src[pl.ds(pl.multiple_of(idx * STEP, STEP), STEP), :].astype(F32).reshape(ROWS, ROWS, chans)
        return tot + jnp.sum(vals, axis=0), sqr + jnp.sum(vals * vals, axis=0)

    zero = jnp.zeros((ROWS, chans), F32)
    return lax.fori_loop(0, rows // STEP, step, (zero, zero))


def layer_norm(tokens):
    centred = tokens - jnp.mean(tokens, axis=-1, keepdims=True)
    return (centred * lax.rsqrt(jnp.mean(centred * centred, axis=-1, keepdims=True) + LN_EPS)).astype(BF16)


def meet(peers, me):
    barrier = pltpu.get_barrier_semaphore()

    @pl.loop(1, peers)
    def _(step):
        pl.semaphore_signal(barrier, inc=1, device_id={'sp': lax.rem(me + step, peers)}, device_id_type=MESH)


def await_peers(peers):
    pl.semaphore_wait(pltpu.get_barrier_semaphore(), peers - 1)


def drain(ref, sem):
    pltpu.make_async_copy(ref, ref, sem).wait()


def remote(src, dst, send_sem, recv_sem, peer):
    return pltpu.make_async_remote_copy(src, dst, send_sem, recv_sem, device_id={'sp': peer}, device_id_type=MESH)


def chunk_cols(chunk):
    return pl.ds(pl.multiple_of(chunk * CK, CK), CK)


def tile_rows(tile, first=0):
    return pl.ds(pl.multiple_of(first + tile * TM, 32), TM)


def members(chans, groups):
    width = chans // groups
    chan = lax.broadcasted_iota(jnp.int32, (chans, LANES), 0)
    low = (lax.broadcasted_iota(jnp.int32, (chans, LANES), 1)) * width
    return one_hot((chan >= low) & (chan < low + width))


def group_sums(rows, member):
    count = rows.shape[0]
    high, mid, low = split3(rows)
    sums = nn(jnp.concatenate([high, mid, low], axis=0).astype(BF16), member)
    return sums[0:count] + sums[count:2 * count] + sums[2 * count:3 * count]


def group_affine(sums, gain, shift, member, count, coef, factor):
    mean = sums[0:1] / count
    rstd = lax.rsqrt(sums[1:2] / count - mean * mean + GN_EPS)
    back = jnp.concatenate(split3(mean) + split3(rstd) + [jnp.zeros((2, LANES), F32)], axis=0).astype(BF16)
    wide = nt(back, member)
    scale = keep_sum(wide[3:6]) * gain
    coef[0:1, :] = factor * scale
    coef[1:2, :] = factor * (shift - keep_sum(wide[:3]) * scale)


def row_sums(tot, sqr):
    return [keep_sum(tot), keep_sum(sqr)]


def eight_rows(rows):
    return jnp.concatenate(rows + [jnp.zeros((ROWS - len(rows), rows[0].shape[1]), F32)], axis=0)


class Pair:
    def __init__(self, peers, band, width):
        self.chips, self.band, self.width = peers // 2, band, width
        self.half, self.sub = self.chips // 2, 2 * band
        self.rows = self.half * self.sub
        self.me = lax.axis_index('sp')
        self.chip, self.core = lax.div(self.me, 2), lax.rem(self.me, 2)
        self.base, self.side, _ = self.seat(self.me)
        self.partner = self.device(self.base, 1 - self.side, self.core)
        self.owners = [self.device(self.base, slot, self.core) for slot in range(2)]

    def seat(self, device):
        chip, core = lax.div(device, 2), lax.rem(device, 2)
        side = lax.div(lax.rem(chip + self.chips - 2 * core, 4), 2)
        return lax.rem(chip - 2 * side + self.chips, self.chips), side, core

    def device(self, base, side, core):
        return 2 * lax.rem(base + 2 * side, self.chips) + core

    def first_chip(self, base, slot, side):
        return lax.rem(base + slot + 1 + (side + 1) * self.half, self.chips)

    def block_chip(self, slot, index, side=None):
        return lax.rem(self.first_chip(self.base, slot, self.side if side is None else side) + index, self.chips)

    def block_rows(self, index):
        return pl.ds(pl.multiple_of(self.width + index * self.sub, self.width), self.sub)

    def border(self, slot):
        return lax.rem(self.chips - self.block_chip(slot, 0), self.chips)

    def spot(self, slot, index):
        return self.width + index * self.sub + jnp.where(index >= self.border(slot), self.width, 0)

    def last_spot(self, slot):
        return self.width + self.rows + jnp.where(self.half >= self.border(slot), self.width, 0)

    def act_shape(self, chans):
        return (2, 3, self.rows + 3 * self.width, chans)

    def clear_border(self, act):
        for slot in range(2):
            @pl.when(self.half >= self.border(slot))
            def _():
                row = pl.ds(pl.multiple_of(self.width + self.border(slot) * self.sub, self.width), self.width)
                act[slot, :, row, :] = jnp.zeros((3, self.width, act.shape[3]), BF16)

    def build(self, src, act, coef, slot, first):
        def part(row, put, count):
            activate(src.at[slot], act.at[slot], coef.at[slot], pl.ds(first, CK), row, put, count, self.width)

        part(0, 0, self.width)
        part(self.width + self.rows, self.last_spot(slot), self.width)

        @loop(self.half)
        def _(index):
            part(self.width + index * self.sub, self.spot(slot, index), self.sub)

    def build_all(self, src, act, coef, slot):
        @loop(act.shape[3] // CK)
        def _(chunk):
            self.build(src, act, coef, slot, pl.multiple_of(chunk * CK, CK))

    def shifted(self, act, slot, tile, dy, dx, cols):
        blocks = TM // self.sub
        rows = [self.spot(slot, blocks * tile + index) + (dy - 1) * self.width for index in range(blocks)]
        return jnp.concatenate([act[slot, dx, pl.ds(pl.multiple_of(row, self.width), self.sub), cols] for row in rows], axis=0)

    def tiles(self, body, order=None):
        per = self.rows // TM

        @loop(2 * per if order is None else per)
        def _(step):
            body(lax.div(step, per) if order is None else order, lax.rem(step, per))

    def acc_rows(self, slot, tile):
        return pl.ds(pl.multiple_of(slot * self.rows + tile * TM, TM), TM)

    def swap_norm(self, mid, acc, bias, sums, member, norm_ref, row, count, coef, send_sem, recv_sem):
        copies, rows = [], []
        for slot in range(2):
            def step(idx, carry):
                first = pl.multiple_of(idx * STEP, STEP)
                rounded = (acc[pl.ds(first + slot * self.rows, STEP), :] + bias[slot:slot + 1, :]).astype(BF16)
                mid[slot, pl.ds(first + self.width, STEP), :] = rounded
                vals = rounded.astype(F32).reshape(ROWS, ROWS, acc.shape[1])
                return carry[0] + jnp.sum(vals, axis=0), carry[1] + jnp.sum(vals * vals, axis=0)

            zero = jnp.zeros((ROWS, acc.shape[1]), F32)
            rows += row_sums(*lax.fori_loop(0, self.rows // STEP, step, (zero, zero)))
            for here, there in ((self.width, self.width + self.rows), (self.rows, 0)):
                index = len(copies)
                copies.append(remote(mid.at[slot, pl.ds(here, self.width), :], mid.at[slot, pl.ds(there, self.width), :], send_sem.at[index], recv_sem.at[index], self.partner))
                copies[-1].start()
        sums[0] = group_sums(eight_rows(rows), member)
        copies.append(remote(sums.at[0], sums.at[1], send_sem.at[len(copies)], recv_sem.at[len(copies)], self.partner))
        copies[-1].start()
        wait_all(copies)
        total = sums[0] + sums[1]
        for slot in range(2):
            group_affine(total[2 * slot:2 * slot + 2], norm_ref[row:row + 1], norm_ref[row + 1:row + 2], member, count, coef.at[slot], 0.5)


def activate(src, act, coef, cols, row, put, count, width):
    half = src[pl.ds(pl.multiple_of(row, width), count), cols].astype(F32) * coef[0:1, cols] + coef[1:2, cols]
    vals = half + half * jnp.tanh(half)
    column = lax.rem(lax.broadcasted_iota(jnp.int32, vals.shape, 0), width)
    rows = pl.ds(pl.multiple_of(put, width), count)
    act[0, rows, cols] = jnp.where(column == 0, 0.0, pltpu.roll(vals, 1, 0)).astype(BF16)
    act[1, rows, cols] = vals.astype(BF16)
    act[2, rows, cols] = jnp.where(column == width - 1, 0.0, pltpu.roll(vals, count - 1, 0)).astype(BF16)


def taps():
    return [(dy, dx) for dy in range(3) for dx in range(3)]


def fetch_rows(kern, which, conv, chunk, wbuf, sem):
    slot = lax.rem(chunk, 2)
    return [pltpu.make_async_copy(kern.at[which, conv, dy, dx, chunk_cols(chunk), :], wbuf.at[slot, pl.ds(tap * CK, CK), :], sem.at[slot])
            for tap, (dy, dx) in enumerate(taps())]


def fetch_cols(kern, which, conv, chunk, wbuf, sem):
    slot = lax.rem(chunk, 2)
    return [pltpu.make_async_copy(kern.at[which, conv, dy, dx, :, chunk_cols(chunk)], wbuf.at[slot, tap], sem.at[slot])
            for tap, (dy, dx) in enumerate(taps())]


def start_all(copies):
    for copy in copies:
        copy.start()


def wait_all(copies):
    for copy in copies:
        copy.wait()


def chunk_product(pair, act, wbuf, chunk, slot, tile):
    cols = chunk_cols(chunk)
    return sum(nn(pair.shifted(act, slot, tile, dy, dx, cols), wbuf[lax.rem(chunk, 2), tap * CK:(tap + 1) * CK, :]) for tap, (dy, dx) in enumerate(taps()))


def column_product(pair, act, cbuf, chunk, slot, tile):
    return sum(nn(pair.shifted(act, slot, tile, dy, dx, slice(None)), cbuf[lax.rem(chunk, 2), tap]) for tap, (dy, dx) in enumerate(taps()))


def conv_columns(pair, kern, which, image, mid, act, cbuf, csem, coef, lead, emit):
    chunks = act.shape[3] // CK
    pair.build_all(mid, act, coef, lead)

    @loop(chunks)
    def _(chunk):
        @pl.when(chunk + 1 < chunks)
        def _():
            start_all(fetch_cols(kern, which, 1, chunk + 1, cbuf, csem))

        wait_all(fetch_cols(kern, which, 1, chunk, cbuf, csem))
        cols = chunk_cols(chunk)

        @loop(2)
        def _(turn):
            slot = lax.rem(lead + turn, 2)

            @pl.when((chunk == 0) & (turn == 1))
            def _():
                pair.build_all(mid, act, coef, slot)

            def body(slot, tile):
                rows = pl.ds(pl.multiple_of(pair.width + tile * TM, pair.width), TM)
                emit(slot, tile, rows, cols, (image[slot, rows, cols].astype(F32) + column_product(pair, act, cbuf, chunk, slot, tile)).astype(BF16))

            pair.tiles(body, slot)


def time_copy(res_time, which, wbuf, sem):
    return pltpu.make_async_copy(res_time.at[which], wbuf.at[1, pl.ds(0, res_time.shape[1]), :], sem)


def time_project(time_ref, wbuf, tproj):
    emb = time_ref[...].astype(F32)
    act = (emb / (1.0 + jnp.exp(-emb))).astype(BF16)
    tproj[...] = nn(act, wbuf[1, 0:act.shape[1], :])


def widen(param, chans):
    groups, width = param.shape
    group = lax.broadcasted_iota(jnp.int32, (groups, chans), 0) * width
    chan = lax.broadcasted_iota(jnp.int32, (groups, chans), 1)
    spread = one_hot((chan >= group) & (chan < group + width))
    wide = lax.dot_general(param, spread, (((0,), (0,)), ((), ())), preferred_element_type=F32)
    place = lax.broadcasted_iota(jnp.int32, (width, chans), 0)
    inside = lax.rem(lax.broadcasted_iota(jnp.int32, (width, chans), 1), width)
    return keep_sum(jnp.where(place == inside, wide, 0.0))


def res_block_in(latent, time_emb, context, res_conv, res_time, res_norm, attn_norm, cross_kv, text, width):
    which, other = 0, 1
    peers, band, chans = latent.shape
    groups = res_norm.shape[1]
    text_dim = context.shape[1]
    text_rows = -(-text // 16) * 16
    block_norms = res_norm.shape[0]
    tokens = peers * band
    chunks = chans // CK
    count = float(tokens * (chans // groups))
    ctx_half = text_dim // 2

    def kernel(lat, time_hbm, ctx_hbm, kern, wtime, norm_hbm, attn_hbm, ckv, out_ref, norm_ref, bias_ref, ctx_k, ctx_v,
               image, mid, act, wbuf, cbuf, acc, time_ref, tproj, rows, bias, mine, stats, sums, coef, norm_raw, attn_raw, ctx_mine, landed,
               wsem, csem, tsem, own_sem, small_sem, ctx_sem, send_sem, side_sem, recv_sem, stat_send, stat_recv, swap_send, swap_recv, give_send, give_recv):
        pair = Pair(peers, band, width)
        me = pair.me

        def own_rows(peer):
            return mid.at[lax.div(peer, pair.chips), pl.ds(pl.multiple_of(lax.rem(peer, pair.chips) * band, band), band), :]

        def load(peer):
            return pltpu.make_async_copy(lat.at[peer], own_rows(peer), own_sem)

        loop(peers)(lambda peer: load(peer).start())
        small = [pltpu.make_async_copy(src, dst, small_sem.at[index]) for index, (src, dst) in enumerate(((time_hbm, time_ref), (norm_hbm, norm_raw), (attn_hbm, attn_raw)))]
        start_all(small)
        weight = time_copy(wtime, which, wbuf, tsem)
        weight.start()
        start_all(fetch_rows(kern, which, 0, 0, wbuf, wsem))
        depth = act.shape[2]
        ctx_parts = [(part, piece, first, min(depth, text * peers - first)) for part in range(2) for piece, first in enumerate(range(0, text * peers, depth))]
        load_ctx = [pltpu.make_async_copy(ctx_hbm.at[pl.ds(first, size), pl.ds(part * ctx_half, ctx_half)], act.at[part, piece, pl.ds(0, size), pl.ds(0, ctx_half)], ctx_sem.at[0])
                    for part, piece, first, size in ctx_parts]
        start_all(load_ctx)
        load_kv = [pltpu.make_async_copy(ckv.at[index, :, pl.ds(part * CK, CK)], cbuf.at[index, part], ctx_sem.at[1]) for index in range(2) for part in range(text_dim // CK)]
        start_all(load_kv)
        meet(peers, me)
        member = members(chans, groups)
        await_peers(peers)

        def send(index):
            cols = chunk_cols(index)

            @loop(peers)
            def _(step):
                owner = lax.rem(me + step, peers)
                base, slot, core = pair.seat(owner)
                place = lax.rem(pair.chip - pair.first_chip(base, slot, 0) + pair.chips, pair.chips)
                side = lax.div(place, pair.half)
                place = place - side * pair.half
                near, far = pair.device(base, side, core), pair.device(base, 1 - side, core)
                src = lat.at[owner, :, cols]
                dst = image.at[slot, pl.ds(pl.multiple_of(width + place * pair.sub + pair.core * band, width), band), cols]

                @pl.when(near == me)
                def _():
                    pltpu.make_async_copy(src, dst, recv_sem.at[index]).start()

                @pl.when(near != me)
                def _():
                    remote(src, dst, send_sem, recv_sem.at[index], near).start()

                @pl.when((pair.core == 1) & (place == pair.half - 1))
                def _():
                    remote(lat.at[owner, pl.ds(band - width, width), cols], image.at[slot, pl.ds(0, width), cols], side_sem, recv_sem.at[index], far).start()

                @pl.when((pair.core == 0) & (place == 0))
                def _():
                    remote(lat.at[owner, pl.ds(0, width), cols], image.at[slot, pl.ds(width + pair.rows, width), cols], side_sem, recv_sem.at[index], far).start()

        send(0)
        loop(peers)(lambda peer: load(peer).wait())

        @loop(peers)
        def _(peer):
            vals = own_rows(peer)[...].astype(F32).reshape(band // ROWS, ROWS, chans)
            for part, total in enumerate((vals, vals * vals)):
                rows[pl.ds(part * peers + peer, 1), :] = keep_sum(jnp.sum(total, axis=0))

        found = group_sums(rows[...], member)
        for peer in range(peers):
            mine[peer, 0:1, :] = found[peer:peer + 1]
            mine[peer, 1:2, :] = found[peers + peer:peers + peer + 1]

        @pl.loop(1, peers)
        def _(step):
            peer = lax.rem(me + step, peers)
            base, _, core = pair.seat(peer)
            for slot in range(2):
                remote(mine.at[pair.device(base, slot, core)], stats.at[me, slot], stat_send, stat_recv, peer).start()

        pl.loop(1, chunks)(send)
        for slot in range(2):
            stats[me, slot] = mine[pair.owners[slot]]
        wait_all(small)
        for index in range(block_norms):
            norm_ref[index:index + 1, :] = widen(norm_raw[index], chans)
        for index in range(2):
            norm_ref[block_norms + index:block_norms + index + 1, :] = widen(attn_raw[index], chans)

        def time_rows(dst, copy):
            copy.wait()
            time_project(time_ref, wbuf, tproj)
            for slot in range(2):
                dst[slot:slot + 1, :] = tproj[pl.ds(pair.owners[slot], 1), :]

        time_rows(bias, weight)
        weight = time_copy(wtime, other, wbuf, tsem)
        weight.start()
        acc[...] = jnp.zeros_like(acc)
        wait_all(load_ctx)
        for part in range(2):
            total = 0.0
            for this, piece, first, size in ctx_parts:
                if this == part:
                    place = (text_rows, size)
                    wanted = lax.broadcasted_iota(jnp.int32, place, 0) * peers + (me - first)
                    pick = one_hot(lax.broadcasted_iota(jnp.int32, place, 1) == wanted)
                    total += nn(pick, act[part, piece, 0:size, 0:ctx_half])
            ctx_mine[:, part * ctx_half:(part + 1) * ctx_half] = total.astype(BF16)
        wait_all(load_kv)
        ctx_k[...] = sum(nt(ctx_mine[:, part * CK:(part + 1) * CK], cbuf[0, part]) for part in range(text_dim // CK)).astype(BF16)

        @loop(chans // CK)
        def _(block):
            part_rows = pl.ds(pl.multiple_of(block * CK, CK), CK)
            ctx_v[part_rows, :] = sum(nt(cbuf[1, part, part_rows, :], ctx_mine[:, part * CK:(part + 1) * CK]) for part in range(text_dim // CK)).astype(BF16)

        time_rows(bias_ref, weight)
        pair.clear_border(act)
        others = stats.at[pl.ds(0, peers - 1)]
        drain(others, stat_recv)
        drain(others, stat_send)
        row = 4 * which
        for slot in range(2):
            group_affine(jnp.sum(stats[:, slot], axis=0), norm_ref[row:row + 1], norm_ref[row + 1:row + 2], member, count, coef.at[slot], 0.5)

        @loop(chunks)
        def _(chunk):
            @pl.when(chunk + 1 < chunks)
            def _():
                start_all(fetch_rows(kern, which, 0, chunk + 1, wbuf, wsem))

            wait_all(fetch_rows(kern, which, 0, chunk, wbuf, wsem))
            drain(image.at[:, :, chunk_cols(chunk)], recv_sem.at[chunk])

            @loop(2)
            def _(slot):
                pair.build(image, act, coef, slot, pl.multiple_of(chunk * CK, CK))

            def body(slot, tile):
                acc[pair.acc_rows(slot, tile), :] += chunk_product(pair, act, wbuf, chunk, slot, tile)

            pair.tiles(body)

        start_all(fetch_cols(kern, which, 1, 0, cbuf, csem))
        pair.swap_norm(mid, acc, bias, sums, member, norm_ref, row + 2, count, coef, swap_send, swap_recv)
        give = 1 - pair.side

        blocks = TM // pair.sub

        def image_rows(slot, index, side=None):
            return pl.ds(pl.multiple_of(pair.block_chip(slot, index, side) * pair.sub, pair.sub), pair.sub)

        def emit(slot, tile, place, cols, vals):
            @pl.when(slot == give)
            def _():
                image[slot, place, cols] = vals

                @pl.when(tile == pair.rows // TM - 1)
                def _():
                    remote(image.at[slot, pl.ds(width, pair.rows), cols], landed.at[:, cols], give_send, give_recv, pair.partner).start()

            @pl.when(slot != give)
            def _():
                for index in range(blocks):
                    out_ref[image_rows(slot, blocks * tile + index), cols] = vals[index * pair.sub:(index + 1) * pair.sub]

        conv_columns(pair, kern, which, image, mid, act, cbuf, csem, coef, give, emit)
        for sem in (give_send, give_recv):
            drain(landed, sem)

        @loop(pair.half)
        def _(index):
            out_ref[image_rows(pair.side, index, give), :] = landed[pl.ds(pl.multiple_of(index * pair.sub, pair.sub), pair.sub), :]

        drain(lat.at[pl.ds(0, peers - 2)], send_sem)
        drain(lat.at[0:2], side_sem)

    vmem = pl.BlockSpec(memory_space=pltpu.VMEM)
    hbm = pl.BlockSpec(memory_space=pl.ANY)
    dma = pltpu.SemaphoreType.DMA
    rows = tokens // 2
    return pl.pallas_call(
        kernel,
        out_shape=[
            jax.ShapeDtypeStruct((tokens, chans), BF16),
            jax.ShapeDtypeStruct((block_norms + ROWS, chans), F32),
            jax.ShapeDtypeStruct((2, chans), F32),
            jax.ShapeDtypeStruct((text_rows, chans), BF16),
            jax.ShapeDtypeStruct((chans, text_rows), BF16),
        ],
        in_specs=[hbm] * ROWS,
        out_specs=[vmem] * 5,
        scratch_shapes=shared_scratch(rows, width, chans) + [
            pltpu.VMEM(time_emb.shape, BF16),
            pltpu.VMEM((peers, chans), F32),
            pltpu.VMEM((2 * peers, chans), F32),
            pltpu.VMEM((2, chans), F32),
            pltpu.VMEM((peers, 2, LANES), F32),
            pltpu.VMEM((peers, 2, 2, LANES), F32),
            pltpu.VMEM((2, ROWS, LANES), F32),
            pltpu.VMEM((2, ROWS, chans), F32),
            pltpu.VMEM(res_norm.shape, BF16),
            pltpu.VMEM(attn_norm.shape, BF16),
            pltpu.VMEM((text_rows, text_dim), BF16),
            pltpu.VMEM((rows, chans), BF16),
            dma((2,)), dma((2,)), dma, dma, dma((3,)), dma((2,)), dma, dma, dma((chunks,)), dma, dma, dma((5,)), dma((5,)), dma, dma,
        ],
        compiler_params=pltpu.CompilerParams(vmem_limit_bytes=VMEM_IN, collective_id=0, has_side_effects=True),
        cost_estimate=cost_of(36 * tokens * chans * chans, 36 * chans * chans),
        name='res_block_in',
    )(latent, time_emb, context, res_conv, res_time, res_norm, attn_norm, cross_kv)


def shared_scratch(rows, width, chans):
    beside = rows + 2 * width
    return [
        pltpu.VMEM((2, beside, chans), BF16),
        pltpu.VMEM((2, beside, chans), BF16),
        pltpu.VMEM((2, 3, beside + width, chans), BF16),
        pltpu.VMEM((2, len(taps()) * CK, chans), BF16),
        pltpu.VMEM((2, len(taps()), chans, CK), BF16),
        pltpu.VMEM((2 * rows, chans), F32),
    ]


def res_block_out(hidden, bias, res_conv, norms, width, groups, peers):
    which = 1
    tokens, chans = hidden.shape
    band = tokens // peers
    chunks = chans // CK
    count = float(tokens * (chans // groups))

    def kernel(hid, bias_ref, kern, norm_ref, out_ref, image, mid, act, wbuf, cbuf, acc, owned, sums, coef,
               wsem, csem, give_send, give_recv, tell_send, tell_recv, swap_send, swap_recv, send_sem, recv_sem):
        pair = Pair(peers, band, width)
        me, side = pair.me, pair.side
        start_all(fetch_rows(kern, which, 0, 0, wbuf, wsem))
        meet(peers, me)
        pair.clear_border(act)
        member = members(chans, groups)

        def pieces(holder):
            def image_rows(index, offset, size):
                return pl.ds(pl.multiple_of(lax.rem(pair.block_chip(side, index, holder) * pair.sub + offset, tokens), width), size)

            return [(image_rows(index, 0, pair.sub), pair.block_rows(index)) for index in range(pair.half)] + [
                (image_rows(0, tokens - width, width), pl.ds(0, width)), (image_rows(pair.half, 0, width), pl.ds(width + pair.rows, width))]

        beside = pl.ds(0, image.shape[1])

        @loop(chunks)
        def _(chunk):
            cols = chunk_cols(chunk)
            for src, dst in pieces(1 - side):
                cbuf[1, chunk, dst, :] = hid[src, cols]

        for src, dst in pieces(side):
            image[side, dst, :] = hid[src, :]
        await_peers(peers)

        @loop(chunks)
        def _(chunk):
            remote(cbuf.at[1, chunk, beside, :], image.at[side, :, chunk_cols(chunk)], give_send, give_recv.at[chunk], pair.partner).start()

        owned[side] = group_sums(eight_rows(row_sums(*channel_sums(hid, tokens, chans))), member)
        tell = remote(owned.at[side], owned.at[side], tell_send, tell_recv, pair.partner)
        tell.start()
        acc[...] = jnp.zeros_like(acc)
        tell.wait()
        row = 4 * which
        for slot in range(2):
            group_affine(owned[slot, 0:2], norm_ref[row:row + 1], norm_ref[row + 1:row + 2], member, count, coef.at[slot], 0.5)

        @loop(chunks)
        def _(chunk):
            @pl.when(chunk + 1 < chunks)
            def _():
                start_all(fetch_rows(kern, which, 0, chunk + 1, wbuf, wsem))

            wait_all(fetch_rows(kern, which, 0, chunk, wbuf, wsem))

            @loop(2)
            def _(turn):
                slot = lax.rem(side + turn, 2)

                @pl.when(turn == 1)
                def _():
                    drain(image.at[1 - side, :, chunk_cols(chunk)], give_recv.at[chunk])

                pair.build(image, act, coef, slot, pl.multiple_of(chunk * CK, CK))

                def body(slot, tile):
                    acc[pair.acc_rows(slot, tile), :] += chunk_product(pair, act, wbuf, chunk, slot, tile)

                pair.tiles(body, slot)

        start_all(fetch_cols(kern, which, 1, 0, cbuf, csem))
        drain(cbuf.at[1, 0:chunks, beside, :], give_send)
        pair.swap_norm(mid, acc, bias_ref, sums, member, norm_ref, row + 2, count, coef, swap_send, swap_recv)

        def emit(slot, tile, place, cols, vals):
            image[slot, place, cols] = vals
            slab = pair.device(pair.base, slot, pair.core)
            blocks = TM // pair.sub
            for index in range(blocks):
                block = blocks * tile + index
                for core in range(2):
                    peer = 2 * pair.block_chip(slot, block) + core
                    src = image.at[slot, pl.ds(pl.multiple_of(width + block * pair.sub + core * band, width), band), cols]

                    @pl.when(peer == me)
                    def _():
                        out_ref[slab, :, cols] = src[...]

                    @pl.when(peer != me)
                    def _():
                        remote(src, out_ref.at[slab, :, cols], send_sem, recv_sem, peer).start()

        conv_columns(pair, kern, which, image, mid, act, cbuf, csem, coef, side, emit)
        others = out_ref.at[pl.ds(0, peers - 2)]
        drain(others, send_sem)
        drain(others, recv_sem)

    vmem = pl.BlockSpec(memory_space=pltpu.VMEM)
    hbm = pl.BlockSpec(memory_space=pl.ANY)
    dma = pltpu.SemaphoreType.DMA
    return pl.pallas_call(
        kernel,
        out_shape=jax.ShapeDtypeStruct((peers, band, chans), BF16),
        in_specs=[vmem, vmem, hbm, vmem],
        out_specs=vmem,
        scratch_shapes=shared_scratch(tokens // 2, width, chans) + [
            pltpu.VMEM((2, ROWS, LANES), F32),
            pltpu.VMEM((2, ROWS, LANES), F32),
            pltpu.VMEM((2, ROWS, chans), F32),
            dma((2,)), dma((2,)), dma, dma((chunks,)), dma, dma, dma((5,)), dma((5,)), dma, dma,
        ],
        compiler_params=pltpu.CompilerParams(vmem_limit_bytes=VMEM_OUT, collective_id=1, has_side_effects=True),
        cost_estimate=cost_of(36 * tokens * chans * chans, 36 * chans * chans),
        name='res_block_out',
    )(hidden, bias, res_conv, norms)


def in_hbm(array):
    return pltpu.with_memory_space_constraint(array, pltpu.HBM)


def cost_of(flops, nbytes):
    return pl.CostEstimate(flops=flops, bytes_accessed=nbytes, transcendentals=0)


def transformer(hidden, ctx_keys, ctx_vals, norms, norm_row, proj_inout, qkv_t, self_out, cross_q_t, cross_out, ff_in, ff_out, groups, heads, text):
    tokens, chans = hidden.shape
    text_rows = ctx_keys.shape[0]
    head_dim = chans // heads
    pairs = heads // 2
    pair = 2 * head_dim
    count = float(tokens * (chans // groups))
    tiles = tokens // TM
    ff_steps = ff_out.shape[0] // chans
    qw = 512 if chans >= 1024 else CK
    kb = CK
    scale = head_dim ** -0.5
    half = chans // 2

    def kernel(h_ref, ctx_k, ctx_v, norm_ref, pio, wqkv, wo, cq, co, f1, f2, out_ref, ring, tok, aux, both, keys, acc, coef, rsem):
        units = {
            'in': (pio.at[0], 0, 0), 'q': (wqkv.at[0], 0, 1), 'k': (wqkv.at[1], 1, 0), 'v': (wqkv.at[2], 1, 1),
            'o': (wo, 1, 0), 'cq': (cq, 1, 1), 'co': (co, 1, 2), 'out': (pio.at[1], 0, 0),
        }

        def copy_of(name):
            src, group, place = units[name]
            return pltpu.make_async_copy(src, ring.at[group, place], rsem.at[group, place])

        def start(*names):
            for name in names:
                copy_of(name).start()

        def take(name):
            copy_of(name).wait()
            _, group, place = units[name]
            return ring.at[group, place]

        def ff_copies(step, group):
            cols = pl.multiple_of(step * chans, chans)
            return [
                pltpu.make_async_copy(f1.at[:, pl.ds(cols, chans)], ring.at[group, 0], rsem.at[group, 0]),
                pltpu.make_async_copy(f1.at[:, pl.ds(cols + ff_steps * chans, chans)], ring.at[group, 1], rsem.at[group, 1]),
                pltpu.make_async_copy(f2.at[pl.ds(cols, chans), :], ring.at[group, 2], rsem.at[group, 2]),
            ]

        start('in', 'q', 'k', 'v', 'co')

        tot, sqr = channel_sums(h_ref, tokens, chans)
        member = members(chans, groups)
        sums = group_sums(eight_rows(row_sums(tot, sqr)), member)
        group_affine(sums, norm_ref[norm_row:norm_row + 1], norm_ref[norm_row + 1:norm_row + 2], member, count, coef, 1.0)

        def project_rows(weight, src, base, normed_to):
            def norm_tile(tile):
                rows = tile_rows(tile)
                normed_to[rows, :] = layer_norm(tok[rows, :].astype(F32))

            @loop(tiles)
            def _(tile):
                norm_tile(jnp.maximum(tile - 1, 0))
                rows = tile_rows(tile)
                tok[rows, :] = (base(rows) + nn(src(rows), weight[...])).astype(BF16)

            norm_tile(tiles - 1)

        project_rows(take('in'), lambda rows: (h_ref[rows, :].astype(F32) * coef[0:1] + coef[1:2]).astype(BF16), lambda rows: 0.0, aux)

        q_t, v_t = both.at[0], both.at[1]

        def transposed(weight, src, dst, factor):
            @loop(2)
            def _(part):
                rows = pl.ds(pl.multiple_of(part * half, half), half)
                dst[rows, :] = (nt(weight[rows, :], src[...]).astype(BF16) * factor).astype(BF16)

        w_key = take('k')

        @loop(tokens // 512)
        def _(part):
            rows = pl.ds(pl.multiple_of(part * 512, 512), 512)
            keys[rows, :] = nt(aux[rows, :], w_key[...]).astype(BF16)
        start('o')

        @loop(2)
        def _(which):
            pltpu.make_async_copy(wqkv.at[2 * which], ring.at[which, 1], rsem.at[which, 1]).wait()
            transposed(ring.at[which, 1], aux, both.at[which], jnp.where(which == 0, scale, 1.0))
        start('cq')
        for copy in ff_copies(0, 0):
            copy.start()

        row_head = lax.broadcasted_iota(jnp.int32, (pair, 1), 0) < head_dim

        def query_of(hp, first, wide, head):
            both = q_t[pl.ds(pl.multiple_of(hp * pair, pair), pair), pl.ds(first, wide)]
            keep = row_head if head == 0 else jnp.logical_not(row_head)
            return jnp.where(keep, both, jnp.zeros_like(both))

        def pair_cols(hp):
            return pl.ds(pl.multiple_of(hp * pair, pair), pair)

        halves = tokens // qw
        blocks = pairs * halves
        scores = [acc.at[:, pl.ds(h * qw, qw)] for h in range(2)]
        probs = [out_ref.at[:, pl.ds(h * qw, qw)] for h in range(2)]
        parts = tokens // kb

        def place(block):
            hp = lax.div(block, halves)
            return hp, pl.multiple_of((block - hp * halves) * qw, qw)

        def fold(vals, func):
            return func(vals.reshape(-1, ROWS, vals.shape[-1]), axis=0)

        def score_part(block, query, head, part):
            hp, _ = place(block)
            vals = nn(keys[part * kb:(part + 1) * kb, pair_cols(hp)], query)
            scores[head][part * kb:(part + 1) * kb, :] = vals
            return fold(vals, jnp.max)

        def exp_part(head, part, top):
            vals = jnp.exp(scores[head][part * kb:(part + 1) * kb, :] - top)
            probs[head][part * kb:(part + 1) * kb, :] = vals.astype(BF16)
            return fold(vals, jnp.sum)

        def value_of(block, head, denom):
            hp, _ = place(block)
            vals = v_t[pl.ds(pl.multiple_of(hp * pair + head * head_dim, head_dim), head_dim), :]
            return nn(vals, probs[head][...]) * (1.0 / denom)

        def block_query(block, head):
            hp, first = place(block)
            return query_of(hp, first, qw, head)

        def softmax_stage(score_block, score_head, exp_head, top):
            tops, sums = [], []
            query = block_query(score_block, score_head)
            for part in range(parts):
                tops.append(score_part(score_block, query, score_head, part))
                sums.append(exp_part(exp_head, part, top))
            new_top = jnp.max(functools.reduce(jnp.maximum, tops), axis=0, keepdims=True)
            return new_top, keep_sum(functools.reduce(jnp.add, sums))

        def emit(block, low, high):
            hp, first = place(block)
            aux[pl.ds(first, qw), pair_cols(hp)] = jnp.concatenate([low, high], axis=0).T.astype(BF16)

        top_first = jnp.max(functools.reduce(jnp.maximum, [score_part(0, block_query(0, 0), 0, part) for part in range(parts)]), axis=0, keepdims=True)
        zero_row = jnp.ones((1, qw), F32)
        zero_out = jnp.zeros((head_dim, qw), F32)

        def attend_block(block, carry):
            top0, denom1, low = carry
            before = jnp.maximum(block - 1, 0)
            high = value_of(before, 1, denom1)
            emit(before, low, high)
            top1, denom0 = softmax_stage(block, 1, 0, top0)
            after = jnp.minimum(block + 1, blocks - 1)
            low = value_of(block, 0, denom0)
            top0, denom1 = softmax_stage(after, 0, 1, top1)
            return top0, denom1, low

        def attend_blocks(step, carry):
            for sub in range(4):
                carry = attend_block(step * 4 + sub, carry)
            return carry

        _, denom1, low = lax.fori_loop(0, blocks // 4, attend_blocks, (top_first, zero_row, zero_out))
        emit(blocks - 1, low, value_of(blocks - 1, 1, denom1))

        project_rows(take('o'), lambda rows: aux[rows, :], lambda rows: tok[rows, :].astype(F32), keys)
        transposed(take('cq'), keys, q_t, scale)

        text_valid = lax.broadcasted_iota(jnp.int32, (text_rows, 1), 0) < text

        wide_step = max(count for count in (CROSS_PAIRS, 2, 1) if pairs % count == 0)

        @loop(pairs // wide_step)
        def _(step):
            for sub in range(wide_step):
                hp = step * wide_step + sub
                outs = []
                for head in range(2):
                    vals = nn(ctx_k[:, pair_cols(hp)], query_of(hp, 0, tokens, head))
                    vals = jnp.where(text_valid, vals, -jnp.inf)
                    weights = jnp.exp(vals - jnp.max(vals, axis=0, keepdims=True))
                    denom = keep_sum(weights)
                    text_vals = ctx_v[pl.ds(pl.multiple_of(hp * pair + head * head_dim, head_dim), head_dim), :]
                    outs.append(nn(text_vals, weights.astype(BF16)) * (1.0 / denom))
                aux[:, pair_cols(hp)] = jnp.concatenate(outs, axis=0).T.astype(BF16)

        project_rows(take('co'), lambda rows: aux[rows, :], lambda rows: tok[rows, :].astype(F32), keys)
        for copy in ff_copies(1, 1):
            copy.start()
        acc[...] = jnp.zeros_like(acc)

        @loop(ff_steps)
        def _(step):
            group = lax.rem(step, 2)
            for copy in ff_copies(step, group):
                copy.wait()

            @loop(tiles, unroll=2)
            def _(tile):
                rows = tile_rows(tile)
                src = keys[rows, :]
                value = nn(src, ring[group, 0])
                gate = nn(src, ring[group, 1])
                gated = (value * (0.5 * gate * (1.0 + lax.erf(gate * (0.5 ** 0.5))))).astype(BF16)
                acc[rows, :] += nn(gated, ring[group, 2])

            @pl.when(step + 2 < ff_steps)
            def _():
                for copy in ff_copies(step + 2, group):
                    copy.start()

            @pl.when(step == ff_steps - 2)
            def _():
                start('out')

        w_fin = take('out')

        @loop(tiles)
        def _(tile):
            rows = tile_rows(tile)
            t = (tok[rows, :].astype(F32) + acc[rows, :]).astype(BF16)
            out_ref[rows, :] = (h_ref[rows, :].astype(F32) + nn(t, w_fin[...])).astype(BF16)

    vmem = pl.BlockSpec(memory_space=pltpu.VMEM)
    hbm = pl.BlockSpec(memory_space=pl.ANY)
    flops = 2 * tokens * chans * chans * (ROWS + 3 * ff_steps) + 4 * tokens * tokens * chans
    return pl.pallas_call(
        kernel,
        out_shape=jax.ShapeDtypeStruct(hidden.shape, BF16),
        in_specs=[vmem] * 4 + [hbm] * 7,
        out_specs=vmem,
        scratch_shapes=[
            pltpu.VMEM((2, 3, chans, chans), BF16),
            pltpu.VMEM((tokens, chans), BF16),
            pltpu.VMEM((tokens, chans), BF16),
            pltpu.VMEM((2, chans, tokens), BF16),
            pltpu.VMEM((tokens, chans), BF16),
            pltpu.VMEM((tokens, chans), F32),
            pltpu.VMEM((ROWS, chans), F32),
            pltpu.SemaphoreType.DMA((2, 3)),
        ],
        compiler_params=pltpu.CompilerParams(vmem_limit_bytes=VMEM_MID),
        cost_estimate=cost_of(flops, 50 * chans * chans),
        name='transformer',
    )(hidden, ctx_keys, ctx_vals, norms, proj_inout, qkv_t, self_out, cross_q_t, cross_out, ff_in, ff_out)


def solution(mesh):
    num_bands = mesh.shape['sp']

    def local_stage(latent, time_emb, context, res_conv, res_time, res_norm, attn_norm, proj_inout, self_qkv, self_out, cross_q, cross_kv, cross_out, ff_in, ff_out):
        images, band_rows, width, chans = latent.shape
        assert images == num_bands
        band = band_rows * width
        heads, head_dim = self_out.shape[:2]
        groups = res_norm.shape[3]
        text, text_dim = context.shape[1:]
        flat_kv = jnp.transpose(cross_kv, (0, 2, 3, 1)).reshape(2, chans, text_dim)
        first, norms, bias, ctx_keys, ctx_vals = res_block_in(
            latent.reshape(images, band, chans), in_hbm(time_emb), jnp.transpose(context, (1, 0, 2)).reshape(text * images, text_dim), res_conv, res_time,
            in_hbm(res_norm.reshape((-1,) + res_norm.shape[3:])), in_hbm(attn_norm), flat_kv, text, width)
        middle = transformer(
            first, ctx_keys, ctx_vals, norms, res_norm.shape[0] * res_norm.shape[1] * res_norm.shape[2], proj_inout,
            jnp.transpose(self_qkv, (0, 2, 3, 1)).reshape(3, chans, chans),
            self_out.reshape(chans, chans),
            jnp.transpose(cross_q, (1, 2, 0)).reshape(chans, chans),
            cross_out.reshape(chans, chans), ff_in, ff_out, groups, heads, text)
        out = res_block_out(middle, bias, res_conv, norms, width, groups, num_bands)
        return out.reshape(latent.shape)

    band_spec = P('dp', 'sp', None, None)
    shared = P()
    in_specs = (band_spec, P('dp', None), P('dp', None, None)) + (shared,) * 12
    return jax.shard_map(local_stage, mesh=mesh, in_specs=in_specs, out_specs=band_spec, check_vma=False)
```

```python
import functools

import jax
import jax.numpy as jnp
from jax import lax
from jax.experimental import pallas as pl
from jax.experimental.pallas import tpu as pltpu
from jax.sharding import PartitionSpec as P

BF16 = jnp.bfloat16
F32 = jnp.float32
MESH = pl.DeviceIdType.MESH
GN_EPS = 1e-6
LN_EPS = 1e-5
TM = 256
CK = 256
CROSS_PAIRS = 5
VMEM_IN, VMEM_MID, VMEM_OUT = 53_000_000, 48_000_000, 49_000_000


def loop(stop, **options):
    return pl.loop(0, stop, **options)


def one_hot(mask):
    return mask.astype(F32).astype(BF16)


def keep_sum(vals):
    return jnp.sum(vals, axis=0, keepdims=True)


def nn(lhs, rhs):
    return jnp.dot(lhs, rhs, preferred_element_type=F32)


def nt(lhs, rhs):
    return lax.dot_general(lhs, rhs, (((1,), (1,)), ((), ())), preferred_element_type=F32)


def split3(vals):
    high = vals.astype(BF16).astype(F32)
    rest = vals - high
    mid = rest.astype(BF16).astype(F32)
    return [high, mid, rest - mid]


def channel_sums(src, rows, chans):
    def step(idx, carry):
        tot, sqr = carry
        vals = src[pl.ds(pl.multiple_of(idx * 64, 64), 64), :].astype(F32).reshape(8, 8, chans)
        return tot + jnp.sum(vals, axis=0), sqr + jnp.sum(vals * vals, axis=0)

    zero = jnp.zeros((8, chans), F32)
    return lax.fori_loop(0, rows // 64, step, (zero, zero))


def layer_norm(tokens):
    centred = tokens - jnp.mean(tokens, axis=-1, keepdims=True)
    return (centred * lax.rsqrt(jnp.mean(centred * centred, axis=-1, keepdims=True) + LN_EPS)).astype(BF16)


def meet(peers, me):
    barrier = pltpu.get_barrier_semaphore()

    @pl.loop(1, peers)
    def _(step):
        pl.semaphore_signal(barrier, inc=1, device_id={'sp': lax.rem(me + step, peers)}, device_id_type=MESH)


def both_ways(step, peers):
    hop = lax.div(step + 1, 2)
    return jnp.where(lax.rem(step, 2) == 1, hop, peers - hop)


def await_peers(peers):
    pl.semaphore_wait(pltpu.get_barrier_semaphore(), peers - 1)


def drain(ref, sem):
    pltpu.make_async_copy(ref, ref, sem).wait()


def remote(src, dst, send_sem, recv_sem, peer):
    return pltpu.make_async_remote_copy(src, dst, send_sem, recv_sem, device_id={'sp': peer}, device_id_type=MESH)


def chunk_cols(chunk):
    return pl.ds(pl.multiple_of(chunk * CK, CK), CK)


def tile_rows(tile, first=0):
    return pl.ds(pl.multiple_of(first + tile * TM, 32), TM)


def members(chans, groups, offset=0):
    width = chans // groups
    chan = lax.broadcasted_iota(jnp.int32, (chans, 128), 0)
    low = (lax.broadcasted_iota(jnp.int32, (chans, 128), 1) - offset) * width
    return one_hot((chan >= low) & (chan < low + width))


def group_sums(rows, member):
    count = rows.shape[0]
    high, mid, low = split3(rows)
    sums = nn(jnp.concatenate([high, mid, low], axis=0).astype(BF16), member)
    return sums[0:count] + sums[count:2 * count] + sums[2 * count:3 * count]


def group_affine(sums, gain, shift, member, count, coef, factor):
    mean = sums[0:1] / count
    rstd = lax.rsqrt(sums[1:2] / count - mean * mean + GN_EPS)
    back = jnp.concatenate(split3(mean) + split3(rstd) + [jnp.zeros((2, 128), F32)], axis=0).astype(BF16)
    wide = nt(back, member)
    scale = keep_sum(wide[3:6]) * gain
    coef[0:1, :] = factor * scale
    coef[1:2, :] = factor * (shift - keep_sum(wide[:3]) * scale)


def two_rows(tot, sqr):
    rows = [keep_sum(tot), keep_sum(sqr)]
    return jnp.concatenate(rows + [jnp.zeros((6, tot.shape[1]), F32)], axis=0)


def activate(src, act, coef, first, wide, row, count, width):
    cols = pl.ds(first, wide)
    half = src[pl.ds(pl.multiple_of(row, width), count), cols].astype(F32) * coef[0:1, cols] + coef[1:2, cols]
    vals = half + half * jnp.tanh(half)
    column = lax.rem(lax.broadcasted_iota(jnp.int32, (count, wide), 0), width)
    put = pl.ds(pl.multiple_of(row + width, width), count)
    act[0, put, cols] = jnp.where(column == 0, 0.0, pltpu.roll(vals, 1, 0)).astype(BF16)
    act[1, put, cols] = vals.astype(BF16)
    act[2, put, cols] = jnp.where(column == width - 1, 0.0, pltpu.roll(vals, count - 1, 0)).astype(BF16)


def clear_edges(act, width):
    edge = jnp.zeros((width, act.shape[2]), BF16)
    for shift in range(3):
        act[shift, 0:width, :] = edge
        act[shift, act.shape[1] - width:act.shape[1], :] = edge


def shifted(act, shift, tile, row, width, cols):
    return act[shift, tile_rows(tile, row * width), cols]


def taps():
    return [(dy, dx) for dy in range(3) for dx in range(3)]


def fetch_rows(kern, which, conv, chunk, wbuf, sem):
    slot = lax.rem(chunk, 2)
    return [pltpu.make_async_copy(kern.at[which, conv, dy, dx, chunk_cols(chunk), :], wbuf.at[slot, pl.ds(tap * CK, CK), :], sem.at[slot])
            for tap, (dy, dx) in enumerate(taps())]


def fetch_halves(kern, which, conv, chunk, wbuf, sem):
    slot, half, count = lax.rem(chunk, 2), CK // 2, len(taps())
    return [pltpu.make_async_copy(kern.at[which, conv, dy, dx, pl.ds(chunk * CK + part * half, half), :], wbuf.at[slot, pl.ds((part * count + tap) * half, half), :], sem.at[slot])
            for part in range(2) for tap, (dy, dx) in enumerate(taps())]


def fetch_cols(kern, which, conv, chunk, wbuf, sem):
    slot = lax.rem(chunk, 2)
    return [pltpu.make_async_copy(kern.at[which, conv, dy, dx, :, chunk_cols(chunk)], wbuf.at[slot, tap], sem.at[slot])
            for tap, (dy, dx) in enumerate(taps())]


def start_all(copies):
    for copy in copies:
        copy.start()


def wait_all(copies):
    for copy in copies:
        copy.wait()


def chunk_product(act, wbuf, slot, chunk, tile, width):
    cols = chunk_cols(chunk)
    return sum(nn(shifted(act, dx, tile, dy, width, cols), wbuf[slot, tap * CK:(tap + 1) * CK, :]) for tap, (dy, dx) in enumerate(taps()))


def half_product(act, wbuf, slot, first, part, tile, width):
    depth = len(taps()) * (CK // 2)
    rows = jnp.concatenate([shifted(act, dx, tile, dy, width, pl.ds(first, CK // 2)) for dy, dx in taps()], axis=1)
    return nn(rows, wbuf[slot, pl.ds(pl.multiple_of(part * depth, depth), depth), :])


def conv_rows(fetch, src, act, wbuf, coef, acc, width):
    tokens, chans = acc.shape
    chunks = chans // CK
    acc[...] = jnp.zeros_like(acc)

    def build(chunk, tile):
        activate(src, act, coef, pl.multiple_of(chunk * CK, CK), CK, tile * TM, TM, width)

    @loop(tokens // TM)
    def _(tile):
        build(0, tile)

    @loop(chunks)
    def _(chunk):
        @pl.when(chunk + 1 < chunks)
        def _():
            start_all(fetch(chunk + 1))

        wait_all(fetch(chunk))

        @loop(tokens // TM)
        def _(tile):
            acc[tile_rows(tile), :] += chunk_product(act, wbuf, lax.rem(chunk, 2), chunk, tile, width)
            build(lax.rem(chunk + 1, chunks), tile)


def add_rows(dst, acc, other):
    @loop(acc.shape[0] // 64)
    def _(idx):
        rows = pl.ds(pl.multiple_of(idx * 64, 64), 64)
        dst[rows, :] = (other[rows, :].astype(F32) + acc[rows, :]).astype(BF16)


def time_copy(res_time, which, wbuf, sem):
    return pltpu.make_async_copy(res_time.at[which], wbuf.at[1, pl.ds(0, res_time.shape[1]), :], sem)


def time_row(time_ref, wbuf, tproj, image):
    emb = time_ref[...].astype(F32)
    act = (emb / (1.0 + jnp.exp(-emb))).astype(BF16)
    tproj[...] = nn(act, wbuf[1, 0:act.shape[1], :])
    return tproj[pl.ds(image, 1), :]


def widen(param, chans):
    groups, width = param.shape
    group = lax.broadcasted_iota(jnp.int32, (groups, chans), 0) * width
    chan = lax.broadcasted_iota(jnp.int32, (groups, chans), 1)
    spread = one_hot((chan >= group) & (chan < group + width))
    wide = lax.dot_general(param, spread, (((0,), (0,)), ((), ())), preferred_element_type=F32)
    place = lax.broadcasted_iota(jnp.int32, (width, chans), 0)
    inside = lax.rem(lax.broadcasted_iota(jnp.int32, (width, chans), 1), width)
    return keep_sum(jnp.where(place == inside, wide, 0.0))


def norm_from(src, member, norm_ref, row, count, coef):
    tot, sqr = channel_sums(src, src.shape[0], src.shape[1])
    group_affine(group_sums(two_rows(tot, sqr), member), norm_ref[row:row + 1], norm_ref[row + 1:row + 2], member, count, coef, 0.5)


def add_and_norm(mid, acc, bias, member, norm_ref, row, count, coef):
    def step(idx, carry):
        rows = pl.ds(pl.multiple_of(idx * 64, 64), 64)
        rounded = (acc[rows, :] + bias).astype(BF16)
        mid[rows, :] = rounded
        vals = rounded.astype(F32).reshape(8, 8, acc.shape[1])
        return carry[0] + jnp.sum(vals, axis=0), carry[1] + jnp.sum(vals * vals, axis=0)

    zero = jnp.zeros((8, acc.shape[1]), F32)
    tot, sqr = lax.fori_loop(0, acc.shape[0] // 64, step, (zero, zero))
    group_affine(group_sums(two_rows(tot, sqr), member), norm_ref[row:row + 1], norm_ref[row + 1:row + 2], member, count, coef, 0.5)


def res_block_in(latent, time_emb, context, res_conv, res_time, res_norm, attn_norm, cross_kv, text, width):
    which, other = 0, 1
    peers, band, chans = latent.shape
    groups = res_norm.shape[1]
    text_dim = context.shape[1]
    text_rows = -(-text // 16) * 16
    block_norms = res_norm.shape[0]
    tokens = peers * band
    last = chans // CK - 1
    half = CK // 2
    pieces = [(chunk * CK, CK) for chunk in range(last)] + [(last * CK, half), (last * CK + half, half)]
    count = float(tokens * (chans // groups))
    tiles = tokens // TM

    def kernel(lat, time_hbm, ctx_hbm, kern, wtime, norm_hbm, attn_hbm, ckv, out_ref, norm_ref, bias_ref, ctx_k, ctx_v,
               image, own, act, wbuf, acc, time_ref, tproj, rows, mine, stats, coef, norm_raw, attn_raw, ctx_raw, ctx_mine, ckv_buf,
               wsem, tsem, own_sem, small_sem, ctx_sem, send_sem, recv_sem, stat_send, stat_recv):
        me = lax.axis_index('sp')
        mid = own
        load = [pltpu.make_async_copy(lat.at[peer], own.at[pl.ds(peer * band, band), :], own_sem) for peer in range(peers)]
        start_all(load)
        small = [pltpu.make_async_copy(src, dst, small_sem.at[index]) for index, (src, dst) in enumerate(((time_hbm, time_ref), (norm_hbm, norm_raw), (attn_hbm, attn_raw)))]
        start_all(small)
        weight = time_copy(wtime, which, wbuf, tsem)
        weight.start()
        start_all(fetch_rows(kern, which, 0, 0, wbuf, wsem))
        ctx_copies = [pltpu.make_async_copy(ctx_hbm, ctx_raw, ctx_sem.at[0]), pltpu.make_async_copy(ckv, ckv_buf, ctx_sem.at[1])]
        start_all(ctx_copies)
        meet(peers, me)
        clear_edges(act, width)
        member = members(chans, groups)
        own_rows = pl.ds(pl.multiple_of(me * band, band), band)
        await_peers(peers)

        def send(index):
            first, wide = pieces[index]

            @pl.loop(1, peers)
            def _(step):
                peer = lax.rem(me + both_ways(step, peers), peers)
                remote(lat.at[peer, :, pl.ds(first, wide)], image.at[own_rows, pl.ds(first, wide)], send_sem.at[index], recv_sem.at[index], peer).start()

        send(0)
        wait_all(load)

        @loop(peers)
        def _(peer):
            vals = own[pl.ds(pl.multiple_of(peer * band, band), band), :].astype(F32).reshape(band // 8, 8, chans)
            rows[pl.ds(peer, 1), :] = keep_sum(jnp.sum(vals, axis=0))
            rows[pl.ds(peers + peer, 1), :] = keep_sum(jnp.sum(vals * vals, axis=0))

        sums = group_sums(rows[...], member)
        for peer in range(peers):
            mine[peer, 0:1, :] = sums[peer:peer + 1]
            mine[peer, 1:2, :] = sums[peers + peer:peers + peer + 1]

        @pl.loop(1, peers)
        def _(step):
            peer = lax.rem(me + step, peers)
            remote(mine.at[peer], stats.at[me], stat_send, stat_recv, peer).start()

        for index in range(1, len(pieces)):
            send(index)
        image[own_rows, :] = own[own_rows, :]
        stats[me] = mine[me]
        wait_all(small)
        for index in range(block_norms):
            norm_ref[index:index + 1, :] = widen(norm_raw[index], chans)
        for index in range(2):
            norm_ref[block_norms + index:block_norms + index + 1, :] = widen(attn_raw[index], chans)
        weight.wait()
        rows[0:1, :] = time_row(time_ref, wbuf, tproj, me)
        weight = time_copy(wtime, other, wbuf, tsem)
        weight.start()
        acc[...] = jnp.zeros_like(acc)
        ctx_copies[0].wait()
        place = (text_rows, text * peers)
        wanted = lax.broadcasted_iota(jnp.int32, place, 0) * peers + me
        pick = one_hot(lax.broadcasted_iota(jnp.int32, place, 1) == wanted)
        ctx_mine[...] = nn(pick, ctx_raw[...]).astype(BF16)
        ctx_copies[1].wait()
        ctx_k[...] = nt(ctx_mine[...], ckv_buf[0]).astype(BF16)

        @loop(chans // 256)
        def _(part):
            part_rows = pl.ds(pl.multiple_of(part * 256, 256), 256)
            ctx_v[part_rows, :] = nt(ckv_buf[1, part_rows, :], ctx_mine[...]).astype(BF16)

        weight.wait()
        bias_ref[...] = time_row(time_ref, wbuf, tproj, me)
        drain(stats.at[pl.ds(0, peers - 1)], stat_recv)
        drain(stats.at[pl.ds(0, peers - 1)], stat_send)
        row = 4 * which
        group_affine(jnp.sum(stats[...], axis=0), norm_ref[row:row + 1], norm_ref[row + 1:row + 2], member, count, coef, 0.5)

        def landed(index):
            first, wide = pieces[index]
            return image.at[pl.ds(0, tokens - band), pl.ds(first, wide)]

        @loop(last)
        def _(chunk):
            @pl.when(chunk + 1 < last)
            def _():
                start_all(fetch_rows(kern, which, 0, chunk + 1, wbuf, wsem))

            @pl.when(chunk + 1 == last)
            def _():
                start_all(fetch_halves(kern, which, 0, last, wbuf, wsem))

            wait_all(fetch_rows(kern, which, 0, chunk, wbuf, wsem))
            drain(image.at[pl.ds(0, tokens - band), chunk_cols(chunk)], recv_sem.at[chunk])

            @loop(tiles)
            def _(tile):
                activate(image, act, coef, pl.multiple_of(chunk * CK, CK), CK, tile * TM, TM, width)

            @loop(tiles)
            def _(tile):
                acc[tile_rows(tile), :] += chunk_product(act, wbuf, lax.rem(chunk, 2), chunk, tile, width)

        wait_all(fetch_halves(kern, which, 0, last, wbuf, wsem))

        @loop(2)
        def _(part):
            first = pl.multiple_of(last * CK + part * half, half)
            drain(image.at[pl.ds(0, tokens - band), pl.ds(first, half)], recv_sem.at[last + part])

            @loop(tiles)
            def _(tile):
                activate(image, act, coef, first, half, tile * TM, TM, width)

            @loop(tiles)
            def _(tile):
                acc[tile_rows(tile), :] += half_product(act, wbuf, last % 2, first, part, tile, width)

        start_all(fetch_rows(kern, which, 1, 0, wbuf, wsem))
        add_and_norm(mid, acc, rows[0:1, :], member, norm_ref, row + 2, count, coef)
        conv_rows(lambda chunk: fetch_rows(kern, which, 1, chunk, wbuf, wsem), mid, act, wbuf, coef, acc, width)
        add_rows(out_ref, acc, image)
        for index in range(len(pieces)):
            drain(landed(index), send_sem.at[index])

    vmem = pl.BlockSpec(memory_space=pltpu.VMEM)
    hbm = pl.BlockSpec(memory_space=pl.ANY)
    dma = pltpu.SemaphoreType.DMA
    return pl.pallas_call(
        kernel,
        out_shape=[
            jax.ShapeDtypeStruct((tokens, chans), BF16),
            jax.ShapeDtypeStruct((block_norms + 8, chans), F32),
            jax.ShapeDtypeStruct((1, chans), F32),
            jax.ShapeDtypeStruct((text_rows, chans), BF16),
            jax.ShapeDtypeStruct((chans, text_rows), BF16),
        ],
        in_specs=[hbm] * 8,
        out_specs=[vmem] * 5,
        scratch_shapes=[
            pltpu.VMEM((tokens, chans), BF16),
            pltpu.VMEM((tokens, chans), BF16),
            pltpu.VMEM((3, tokens + 2 * width, chans), BF16),
            pltpu.VMEM((2, len(taps()) * CK, chans), BF16),
            pltpu.VMEM((tokens, chans), F32),
            pltpu.VMEM(time_emb.shape, BF16),
            pltpu.VMEM((peers, chans), F32),
            pltpu.VMEM((2 * peers, chans), F32),
            pltpu.VMEM((peers, 8, 128), F32),
            pltpu.VMEM((peers, 8, 128), F32),
            pltpu.VMEM((8, chans), F32),
            pltpu.VMEM(res_norm.shape, BF16),
            pltpu.VMEM(attn_norm.shape, BF16),
            pltpu.VMEM(context.shape, BF16),
            pltpu.VMEM((text_rows, text_dim), BF16),
            pltpu.VMEM(cross_kv.shape, BF16),
            dma((2,)), dma, dma, dma((3,)), dma((2,)), dma((len(pieces),)), dma((len(pieces),)), dma, dma,
        ],
        compiler_params=pltpu.CompilerParams(vmem_limit_bytes=VMEM_IN, collective_id=0, has_side_effects=True),
        cost_estimate=cost_of(36 * tokens * chans * chans, 36 * chans * chans),
        name='res_block_in',
    )(latent, time_emb, context, res_conv, res_time, res_norm, attn_norm, cross_kv)


def res_block_out(hidden, bias, res_conv, norms, width, groups, peers):
    which = 1
    tokens, chans = hidden.shape
    band = tokens // peers
    chunks = chans // CK
    tiles = tokens // TM
    per_tile = TM // band
    count = float(tokens * (chans // groups))

    def kernel(x_ref, bias_ref, kern, norm_ref, out_ref, mid, result, act, wbuf, cbuf, acc, coef, wsem, csem, send_sem, recv_sem):
        me = lax.axis_index('sp')
        start_all(fetch_rows(kern, which, 0, 0, wbuf, wsem))
        meet(peers, me)
        clear_edges(act, width)
        member = members(chans, groups)
        row = 4 * which
        norm_from(x_ref, member, norm_ref, row, count, coef)
        conv_rows(lambda chunk: fetch_rows(kern, which, 0, chunk, wbuf, wsem), x_ref, act, wbuf, coef, acc, width)
        start_all(fetch_cols(kern, which, 1, 0, cbuf, csem))
        add_and_norm(mid, acc, bias_ref[...], member, norm_ref, row + 2, count, coef)

        def build(row, rows):
            @loop(chunks)
            def _(chunk):
                activate(mid, act, coef, pl.multiple_of(chunk * CK, CK), CK, row, rows, width)

        def build_tile(tile):
            build(tile * TM, TM)

            @pl.when(tile + 1 < tiles)
            def _():
                build((tile + 1) * TM, width)

        turn = lax.rem(lax.div(me, per_tile) + tiles // 2, tiles)
        build_tile(turn)

        @pl.when(turn > 0)
        def _():
            build(turn * TM - width, width)

        await_peers(peers)

        @loop(chunks)
        def _(chunk):
            slot = lax.rem(chunk, 2)
            cols = chunk_cols(chunk)

            @pl.when(chunk + 1 < chunks)
            def _():
                start_all(fetch_cols(kern, which, 1, chunk + 1, cbuf, csem))

            wait_all(fetch_cols(kern, which, 1, chunk, cbuf, csem))

            @loop(tiles)
            def _(step):
                tile = lax.rem(step + turn, tiles)
                part = sum(nn(shifted(act, dx, tile, dy, width, slice(None)), cbuf[slot, tap]) for tap, (dy, dx) in enumerate(taps()))
                rows = tile_rows(tile)
                result[rows, cols] = (x_ref[rows, cols].astype(F32) + part).astype(BF16)
                for idx in range(per_tile):
                    peer = tile * per_tile + idx
                    block = result.at[pl.ds(pl.multiple_of(peer * band, band), band), cols]

                    @pl.when(peer == me)
                    def _():
                        out_ref[me, :, cols] = block[...]

                    @pl.when(peer != me)
                    def _():
                        remote(block, out_ref.at[me, :, cols], send_sem, recv_sem, peer).start()

                @pl.when((chunk == 0) & (step + 1 < tiles))
                def _():
                    build_tile(lax.rem(step + 1 + turn, tiles))

        others = out_ref.at[pl.ds(0, peers - 1)]
        drain(others, send_sem)
        drain(others, recv_sem)

    vmem = pl.BlockSpec(memory_space=pltpu.VMEM)
    hbm = pl.BlockSpec(memory_space=pl.ANY)
    dma = pltpu.SemaphoreType.DMA
    return pl.pallas_call(
        kernel,
        out_shape=jax.ShapeDtypeStruct((peers, band, chans), BF16),
        in_specs=[vmem, vmem, hbm, vmem],
        out_specs=vmem,
        scratch_shapes=[
            pltpu.VMEM((tokens, chans), BF16),
            pltpu.VMEM((tokens, chans), BF16),
            pltpu.VMEM((3, tokens + 2 * width, chans), BF16),
            pltpu.VMEM((2, len(taps()) * CK, chans), BF16),
            pltpu.VMEM((2, len(taps()), chans, CK), BF16),
            pltpu.VMEM((tokens, chans), F32),
            pltpu.VMEM((8, chans), F32),
            dma((2,)), dma((2,)), dma, dma,
        ],
        compiler_params=pltpu.CompilerParams(vmem_limit_bytes=VMEM_OUT, collective_id=1, has_side_effects=True),
        cost_estimate=cost_of(36 * tokens * chans * chans, 36 * chans * chans),
        name='res_block_out',
    )(hidden, bias, res_conv, norms)


def cost_of(flops, nbytes):
    return pl.CostEstimate(flops=flops, bytes_accessed=nbytes, transcendentals=0)


def transformer(hidden, ctx_keys, ctx_vals, norms, norm_row, proj_inout, qkv_t, self_out, cross_q_t, cross_out, ff_in, ff_out, groups, heads, text):
    tokens, chans = hidden.shape
    text_rows = ctx_keys.shape[0]
    head_dim = chans // heads
    pairs = heads // 2
    pair = 2 * head_dim
    count = float(tokens * (chans // groups))
    tiles = tokens // TM
    ff_steps = ff_out.shape[0] // chans
    qw = 512 if chans >= 1024 else 256
    kb = 256
    scale = head_dim ** -0.5
    half = chans // 2

    def kernel(h_ref, ctx_k, ctx_v, norm_ref, pio, wqkv, wo, cq, co, f1, f2, out_ref, ring, tok, aux, both, keys, acc, coef, rsem):
        units = {
            'in': (pio.at[0], 0, 0), 'q': (wqkv.at[0], 0, 1), 'k': (wqkv.at[1], 1, 0), 'v': (wqkv.at[2], 1, 1),
            'o': (wo, 1, 0), 'cq': (cq, 1, 1), 'co': (co, 1, 2), 'out': (pio.at[1], 0, 0),
        }

        def copy_of(name):
            src, group, place = units[name]
            return pltpu.make_async_copy(src, ring.at[group, place], rsem.at[group, place])

        def start(*names):
            for name in names:
                copy_of(name).start()

        def take(name):
            copy_of(name).wait()
            _, group, place = units[name]
            return ring.at[group, place]

        def ff_copies(step, group):
            cols = pl.multiple_of(step * chans, chans)
            return [
                pltpu.make_async_copy(f1.at[:, pl.ds(cols, chans)], ring.at[group, 0], rsem.at[group, 0]),
                pltpu.make_async_copy(f1.at[:, pl.ds(cols + ff_steps * chans, chans)], ring.at[group, 1], rsem.at[group, 1]),
                pltpu.make_async_copy(f2.at[pl.ds(cols, chans), :], ring.at[group, 2], rsem.at[group, 2]),
            ]

        start('in', 'q', 'k', 'v', 'co')

        tot, sqr = channel_sums(h_ref, tokens, chans)
        member = members(chans, groups)
        sums = group_sums(two_rows(tot, sqr), member)
        group_affine(sums, norm_ref[norm_row:norm_row + 1], norm_ref[norm_row + 1:norm_row + 2], member, count, coef, 1.0)

        def project_rows(weight, src, base, normed_to):
            def norm_tile(tile):
                rows = tile_rows(tile)
                normed_to[rows, :] = layer_norm(tok[rows, :].astype(F32))

            @loop(tiles)
            def _(tile):
                norm_tile(jnp.maximum(tile - 1, 0))
                rows = tile_rows(tile)
                tok[rows, :] = (base(rows) + nn(src(rows), weight[...])).astype(BF16)

            norm_tile(tiles - 1)

        project_rows(take('in'), lambda rows: (h_ref[rows, :].astype(F32) * coef[0:1] + coef[1:2]).astype(BF16), lambda rows: 0.0, aux)

        q_t, v_t = both.at[0], both.at[1]

        def transposed(weight, src, dst, factor):
            @loop(2)
            def _(part):
                rows = pl.ds(pl.multiple_of(part * half, half), half)
                dst[rows, :] = (nt(weight[rows, :], src[...]).astype(BF16) * factor).astype(BF16)

        w_key = take('k')

        @loop(tokens // 512)
        def _(part):
            rows = pl.ds(pl.multiple_of(part * 512, 512), 512)
            keys[rows, :] = nt(aux[rows, :], w_key[...]).astype(BF16)
        start('o')

        @loop(2)
        def _(which):
            pltpu.make_async_copy(wqkv.at[2 * which], ring.at[which, 1], rsem.at[which, 1]).wait()
            transposed(ring.at[which, 1], aux, both.at[which], jnp.where(which == 0, scale, 1.0))
        start('cq')
        for copy in ff_copies(0, 0):
            copy.start()

        row_head = lax.broadcasted_iota(jnp.int32, (pair, 1), 0) < head_dim

        def query_of(hp, first, wide, head):
            both = q_t[pl.ds(pl.multiple_of(hp * pair, pair), pair), pl.ds(first, wide)]
            keep = row_head if head == 0 else jnp.logical_not(row_head)
            return jnp.where(keep, both, jnp.zeros_like(both))

        def pair_cols(hp):
            return pl.ds(pl.multiple_of(hp * pair, pair), pair)

        halves = tokens // qw
        blocks = pairs * halves
        scores = [acc.at[:, pl.ds(h * qw, qw)] for h in range(2)]
        probs = [out_ref.at[:, pl.ds(h * qw, qw)] for h in range(2)]
        parts = tokens // kb

        def place(block):
            hp = lax.div(block, halves)
            return hp, pl.multiple_of((block - hp * halves) * qw, qw)

        def fold(vals, func):
            return func(vals.reshape(-1, 8, vals.shape[-1]), axis=0)

        def score_part(block, query, head, part):
            hp, _ = place(block)
            vals = nn(keys[part * kb:(part + 1) * kb, pair_cols(hp)], query)
            scores[head][part * kb:(part + 1) * kb, :] = vals
            return fold(vals, jnp.max)

        def exp_part(head, part, top):
            vals = jnp.exp(scores[head][part * kb:(part + 1) * kb, :] - top)
            probs[head][part * kb:(part + 1) * kb, :] = vals.astype(BF16)
            return fold(vals, jnp.sum)

        def value_of(block, head, denom):
            hp, _ = place(block)
            vals = v_t[pl.ds(pl.multiple_of(hp * pair + head * head_dim, head_dim), head_dim), :]
            return nn(vals, probs[head][...]) * (1.0 / denom)

        def block_query(block, head):
            hp, first = place(block)
            return query_of(hp, first, qw, head)

        def softmax_stage(score_block, score_head, exp_head, top):
            tops, sums = [], []
            query = block_query(score_block, score_head)
            for part in range(parts):
                tops.append(score_part(score_block, query, score_head, part))
                sums.append(exp_part(exp_head, part, top))
            new_top = jnp.max(functools.reduce(jnp.maximum, tops), axis=0, keepdims=True)
            return new_top, keep_sum(functools.reduce(jnp.add, sums))

        def emit(block, low, high):
            hp, first = place(block)
            aux[pl.ds(first, qw), pair_cols(hp)] = jnp.concatenate([low, high], axis=0).T.astype(BF16)

        top_first = jnp.max(functools.reduce(jnp.maximum, [score_part(0, block_query(0, 0), 0, part) for part in range(parts)]), axis=0, keepdims=True)
        zero_row = jnp.ones((1, qw), F32)
        zero_out = jnp.zeros((head_dim, qw), F32)

        def attend_block(block, carry):
            top0, denom1, low = carry
            before = jnp.maximum(block - 1, 0)
            high = value_of(before, 1, denom1)
            emit(before, low, high)
            top1, denom0 = softmax_stage(block, 1, 0, top0)
            after = jnp.minimum(block + 1, blocks - 1)
            low = value_of(block, 0, denom0)
            top0, denom1 = softmax_stage(after, 0, 1, top1)
            return top0, denom1, low

        def attend_blocks(step, carry):
            for sub in range(4):
                carry = attend_block(step * 4 + sub, carry)
            return carry

        _, denom1, low = lax.fori_loop(0, blocks // 4, attend_blocks, (top_first, zero_row, zero_out))
        emit(blocks - 1, low, value_of(blocks - 1, 1, denom1))

        project_rows(take('o'), lambda rows: aux[rows, :], lambda rows: tok[rows, :].astype(F32), keys)
        transposed(take('cq'), keys, q_t, scale)

        text_valid = lax.broadcasted_iota(jnp.int32, (text_rows, 1), 0) < text

        wide_step = max(count for count in (CROSS_PAIRS, 2, 1) if pairs % count == 0)

        @loop(pairs // wide_step)
        def _(step):
            for sub in range(wide_step):
                hp = step * wide_step + sub
                outs = []
                for head in range(2):
                    vals = nn(ctx_k[:, pair_cols(hp)], query_of(hp, 0, tokens, head))
                    vals = jnp.where(text_valid, vals, -jnp.inf)
                    weights = jnp.exp(vals - jnp.max(vals, axis=0, keepdims=True))
                    denom = keep_sum(weights)
                    text_vals = ctx_v[pl.ds(pl.multiple_of(hp * pair + head * head_dim, head_dim), head_dim), :]
                    outs.append(nn(text_vals, weights.astype(BF16)) * (1.0 / denom))
                aux[:, pair_cols(hp)] = jnp.concatenate(outs, axis=0).T.astype(BF16)

        project_rows(take('co'), lambda rows: aux[rows, :], lambda rows: tok[rows, :].astype(F32), keys)
        for copy in ff_copies(1, 1):
            copy.start()
        acc[...] = jnp.zeros_like(acc)

        @loop(ff_steps)
        def _(step):
            group = lax.rem(step, 2)
            for copy in ff_copies(step, group):
                copy.wait()

            @loop(tiles, unroll=2)
            def _(tile):
                rows = tile_rows(tile)
                src = keys[rows, :]
                value = nn(src, ring[group, 0])
                gate = nn(src, ring[group, 1])
                gated = (value * (0.5 * gate * (1.0 + lax.erf(gate * (0.5 ** 0.5))))).astype(BF16)
                acc[rows, :] += nn(gated, ring[group, 2])

            @pl.when(step + 2 < ff_steps)
            def _():
                for copy in ff_copies(step + 2, group):
                    copy.start()

            @pl.when(step == ff_steps - 2)
            def _():
                start('out')

        w_fin = take('out')

        @loop(tiles)
        def _(tile):
            rows = tile_rows(tile)
            t = (tok[rows, :].astype(F32) + acc[rows, :]).astype(BF16)
            out_ref[rows, :] = (h_ref[rows, :].astype(F32) + nn(t, w_fin[...])).astype(BF16)

    vmem = pl.BlockSpec(memory_space=pltpu.VMEM)
    hbm = pl.BlockSpec(memory_space=pl.ANY)
    flops = 2 * tokens * chans * chans * (8 + 3 * ff_steps) + 4 * tokens * tokens * chans
    return pl.pallas_call(
        kernel,
        out_shape=jax.ShapeDtypeStruct(hidden.shape, BF16),
        in_specs=[vmem] * 4 + [hbm] * 7,
        out_specs=vmem,
        scratch_shapes=[
            pltpu.VMEM((2, 3, chans, chans), BF16),
            pltpu.VMEM((tokens, chans), BF16),
            pltpu.VMEM((tokens, chans), BF16),
            pltpu.VMEM((2, chans, tokens), BF16),
            pltpu.VMEM((tokens, chans), BF16),
            pltpu.VMEM((tokens, chans), F32),
            pltpu.VMEM((8, chans), F32),
            pltpu.SemaphoreType.DMA((2, 3)),
        ],
        compiler_params=pltpu.CompilerParams(vmem_limit_bytes=VMEM_MID),
        cost_estimate=cost_of(flops, 50 * chans * chans),
        name='transformer',
    )(hidden, ctx_keys, ctx_vals, norms, proj_inout, qkv_t, self_out, cross_q_t, cross_out, ff_in, ff_out)


def solution(mesh):
    num_bands = mesh.shape['sp']

    def local_stage(latent, time_emb, context, res_conv, res_time, res_norm, attn_norm, proj_inout, self_qkv, self_out, cross_q, cross_kv, cross_out, ff_in, ff_out):
        images, band_rows, width, chans = latent.shape
        assert images == num_bands
        band = band_rows * width
        heads, head_dim = self_out.shape[:2]
        groups = res_norm.shape[3]
        text, text_dim = context.shape[1:]
        flat_kv = jnp.transpose(cross_kv, (0, 2, 3, 1)).reshape(2, chans, text_dim)
        first, norms, bias, ctx_keys, ctx_vals = res_block_in(
            latent.reshape(images, band, chans), pltpu.with_memory_space_constraint(time_emb, pltpu.HBM), jnp.transpose(context, (1, 0, 2)).reshape(text * images, text_dim), res_conv, res_time,
            pltpu.with_memory_space_constraint(res_norm.reshape((-1,) + res_norm.shape[3:]), pltpu.HBM), pltpu.with_memory_space_constraint(attn_norm, pltpu.HBM), flat_kv, text, width)
        middle = transformer(
            first, ctx_keys, ctx_vals, norms, res_norm.shape[0] * res_norm.shape[1] * res_norm.shape[2], proj_inout,
            jnp.transpose(self_qkv, (0, 2, 3, 1)).reshape(3, chans, chans),
            self_out.reshape(chans, chans),
            jnp.transpose(cross_q, (1, 2, 0)).reshape(chans, chans),
            cross_out.reshape(chans, chans), ff_in, ff_out, groups, heads, text)
        out = res_block_out(middle, bias, res_conv, norms, width, groups, num_bands)
        return out.reshape(latent.shape)

    band_spec = P('dp', 'sp', None, None)
    shared = P()
    in_specs = (band_spec, P('dp', None), P('dp', None, None)) + (shared,) * 12
    return jax.shard_map(local_stage, mesh=mesh, in_specs=in_specs, out_specs=band_spec, check_vma=False)
```

```python
import functools

import jax
import jax.numpy as jnp
from jax import lax
from jax.experimental import pallas as pl
from jax.experimental.pallas import tpu as pltpu
from jax.sharding import PartitionSpec as P

BF16 = jnp.bfloat16
F32 = jnp.float32
MESH = pl.DeviceIdType.MESH
GN_EPS = 1e-6
LN_EPS = 1e-5
TM = 256
CK = 256
STEP = 64
CROSS_PAIRS = 5
VMEM_IN, VMEM_MID, VMEM_OUT = 53_000_000, 48_000_000, 49_000_000


def loop(stop, **options):
    return pl.loop(0, stop, **options)


def one_hot(mask):
    return mask.astype(F32).astype(BF16)


def keep_sum(vals):
    return jnp.sum(vals, axis=0, keepdims=True)


def nn(lhs, rhs):
    return jnp.dot(lhs, rhs, preferred_element_type=F32)


def nt(lhs, rhs):
    return lax.dot_general(lhs, rhs, (((1,), (1,)), ((), ())), preferred_element_type=F32)


def split3(vals):
    high = vals.astype(BF16).astype(F32)
    rest = vals - high
    mid = rest.astype(BF16).astype(F32)
    return [high, mid, rest - mid]


def channel_sums(src, rows, chans):
    def step(idx, carry):
        tot, sqr = carry
        vals = src[pl.ds(pl.multiple_of(idx * 64, 64), 64), :].astype(F32).reshape(8, 8, chans)
        return tot + jnp.sum(vals, axis=0), sqr + jnp.sum(vals * vals, axis=0)

    zero = jnp.zeros((8, chans), F32)
    return lax.fori_loop(0, rows // 64, step, (zero, zero))


def layer_norm(tokens):
    centred = tokens - jnp.mean(tokens, axis=-1, keepdims=True)
    return (centred * lax.rsqrt(jnp.mean(centred * centred, axis=-1, keepdims=True) + LN_EPS)).astype(BF16)


def meet(peers, me):
    barrier = pltpu.get_barrier_semaphore()

    @pl.loop(1, peers)
    def _(step):
        pl.semaphore_signal(barrier, inc=1, device_id={'sp': lax.rem(me + step, peers)}, device_id_type=MESH)


def await_peers(peers):
    pl.semaphore_wait(pltpu.get_barrier_semaphore(), peers - 1)


def drain(ref, sem):
    pltpu.make_async_copy(ref, ref, sem).wait()


def remote(src, dst, send_sem, recv_sem, peer):
    return pltpu.make_async_remote_copy(src, dst, send_sem, recv_sem, device_id={'sp': peer}, device_id_type=MESH)


def chunk_cols(chunk):
    return pl.ds(pl.multiple_of(chunk * CK, CK), CK)


def tile_rows(tile, first=0):
    return pl.ds(pl.multiple_of(first + tile * TM, 32), TM)


def members(chans, groups, offset=0):
    width = chans // groups
    chan = lax.broadcasted_iota(jnp.int32, (chans, 128), 0)
    low = (lax.broadcasted_iota(jnp.int32, (chans, 128), 1) - offset) * width
    return one_hot((chan >= low) & (chan < low + width))


def group_sums(rows, member):
    count = rows.shape[0]
    high, mid, low = split3(rows)
    sums = nn(jnp.concatenate([high, mid, low], axis=0).astype(BF16), member)
    return sums[0:count] + sums[count:2 * count] + sums[2 * count:3 * count]


def group_affine(sums, gain, shift, member, count, coef, factor):
    mean = sums[0:1] / count
    rstd = lax.rsqrt(sums[1:2] / count - mean * mean + GN_EPS)
    back = jnp.concatenate(split3(mean) + split3(rstd) + [jnp.zeros((2, 128), F32)], axis=0).astype(BF16)
    wide = nt(back, member)
    scale = keep_sum(wide[3:6]) * gain
    coef[0:1, :] = factor * scale
    coef[1:2, :] = factor * (shift - keep_sum(wide[:3]) * scale)


def two_rows(tot, sqr):
    rows = [keep_sum(tot), keep_sum(sqr)]
    return jnp.concatenate(rows + [jnp.zeros((6, tot.shape[1]), F32)], axis=0)


def activate(src, act, coef, first, wide, row, count, width):
    cols = pl.ds(first, wide)
    half = src[pl.ds(pl.multiple_of(row, width), count), cols].astype(F32) * coef[0:1, cols] + coef[1:2, cols]
    vals = half + half * jnp.tanh(half)
    column = lax.rem(lax.broadcasted_iota(jnp.int32, (count, wide), 0), width)
    put = pl.ds(pl.multiple_of(row + width, width), count)
    act[0, put, cols] = jnp.where(column == 0, 0.0, pltpu.roll(vals, 1, 0)).astype(BF16)
    act[1, put, cols] = vals.astype(BF16)
    act[2, put, cols] = jnp.where(column == width - 1, 0.0, pltpu.roll(vals, count - 1, 0)).astype(BF16)


def clear_edges(act, width):
    edge = jnp.zeros((width, act.shape[2]), BF16)
    for shift in range(3):
        act[shift, 0:width, :] = edge
        act[shift, act.shape[1] - width:act.shape[1], :] = edge


def shifted(act, shift, tile, row, width, cols):
    return act[shift, tile_rows(tile, row * width), cols]


def taps():
    return [(dy, dx) for dy in range(3) for dx in range(3)]


def fetch_rows(kern, which, conv, chunk, wbuf, sem):
    slot = lax.rem(chunk, 2)
    return [pltpu.make_async_copy(kern.at[which, conv, dy, dx, chunk_cols(chunk), :], wbuf.at[slot, pl.ds(tap * CK, CK), :], sem.at[slot])
            for tap, (dy, dx) in enumerate(taps())]


def fetch_halves(kern, which, conv, chunk, wbuf, sem):
    slot, half, count = lax.rem(chunk, 2), CK // 2, len(taps())
    return [pltpu.make_async_copy(kern.at[which, conv, dy, dx, pl.ds(chunk * CK + part * half, half), :], wbuf.at[slot, pl.ds((part * count + tap) * half, half), :], sem.at[slot])
            for part in range(2) for tap, (dy, dx) in enumerate(taps())]


def fetch_cols(kern, which, conv, chunk, wbuf, sem):
    slot = lax.rem(chunk, 2)
    return [pltpu.make_async_copy(kern.at[which, conv, dy, dx, :, chunk_cols(chunk)], wbuf.at[slot, tap], sem.at[slot])
            for tap, (dy, dx) in enumerate(taps())]


def start_all(copies):
    for copy in copies:
        copy.start()


def wait_all(copies):
    for copy in copies:
        copy.wait()


def chunk_product(act, wbuf, slot, chunk, tile, width):
    cols = chunk_cols(chunk)
    return sum(nn(shifted(act, dx, tile, dy, width, cols), wbuf[slot, tap * CK:(tap + 1) * CK, :]) for tap, (dy, dx) in enumerate(taps()))


def half_product(act, wbuf, slot, first, part, tile, width):
    depth = len(taps()) * (CK // 2)
    rows = jnp.concatenate([shifted(act, dx, tile, dy, width, pl.ds(first, CK // 2)) for dy, dx in taps()], axis=1)
    return nn(rows, wbuf[slot, pl.ds(pl.multiple_of(part * depth, depth), depth), :])


def conv_rows(fetch, src, act, wbuf, coef, acc, width):
    tokens, chans = acc.shape
    chunks = chans // CK

    def build(chunk, tile):
        activate(src, act, coef, pl.multiple_of(chunk * CK, CK), CK, tile * TM, TM, width)

    @loop(tokens // TM)
    def _(tile):
        build(0, tile)

    @loop(chunks)
    def _(chunk):
        @pl.when(chunk + 1 < chunks)
        def _():
            start_all(fetch(chunk + 1))

        wait_all(fetch(chunk))

        @loop(tokens // TM)
        def _(tile):
            acc[tile_rows(tile), :] += chunk_product(act, wbuf, lax.rem(chunk, 2), chunk, tile, width)
            build(lax.rem(chunk + 1, chunks), tile)


def add_rows(dst, acc, other):
    @loop(acc.shape[0] // 64)
    def _(idx):
        rows = pl.ds(pl.multiple_of(idx * 64, 64), 64)
        dst[rows, :] = (other[rows, :].astype(F32) + acc[rows, :]).astype(BF16)


def time_copy(res_time, which, wbuf, sem):
    return pltpu.make_async_copy(res_time.at[which], wbuf.at[1, pl.ds(0, res_time.shape[1]), :], sem)


def time_row(time_ref, wbuf, tproj, image):
    emb = time_ref[...].astype(F32)
    act = (emb / (1.0 + jnp.exp(-emb))).astype(BF16)
    tproj[...] = nn(act, wbuf[1, 0:act.shape[1], :])
    return tproj[pl.ds(image, 1), :]


def widen(param, chans):
    groups, width = param.shape
    group = lax.broadcasted_iota(jnp.int32, (groups, chans), 0) * width
    chan = lax.broadcasted_iota(jnp.int32, (groups, chans), 1)
    spread = one_hot((chan >= group) & (chan < group + width))
    wide = lax.dot_general(param, spread, (((0,), (0,)), ((), ())), preferred_element_type=F32)
    place = lax.broadcasted_iota(jnp.int32, (width, chans), 0)
    inside = lax.rem(lax.broadcasted_iota(jnp.int32, (width, chans), 1), width)
    return keep_sum(jnp.where(place == inside, wide, 0.0))


def norm_from(src, member, norm_ref, row, count, coef):
    tot, sqr = channel_sums(src, src.shape[0], src.shape[1])
    group_affine(group_sums(two_rows(tot, sqr), member), norm_ref[row:row + 1], norm_ref[row + 1:row + 2], member, count, coef, 0.5)


def add_and_norm(mid, acc, bias, member, norm_ref, row, count, coef):
    def step(idx, carry):
        rows = pl.ds(pl.multiple_of(idx * 64, 64), 64)
        rounded = (acc[rows, :] + bias).astype(BF16)
        mid[rows, :] = rounded
        acc[rows, :] = jnp.zeros((STEP, acc.shape[1]), F32)
        vals = rounded.astype(F32).reshape(8, 8, acc.shape[1])
        return carry[0] + jnp.sum(vals, axis=0), carry[1] + jnp.sum(vals * vals, axis=0)

    zero = jnp.zeros((8, acc.shape[1]), F32)
    tot, sqr = lax.fori_loop(0, acc.shape[0] // 64, step, (zero, zero))
    group_affine(group_sums(two_rows(tot, sqr), member), norm_ref[row:row + 1], norm_ref[row + 1:row + 2], member, count, coef, 0.5)


def res_block_in(latent, time_emb, context, res_conv, res_time, res_norm, attn_norm, cross_kv, text, width):
    which, other = 0, 1
    peers, band, chans = latent.shape
    groups = res_norm.shape[1]
    text_dim = context.shape[1]
    text_rows = -(-text // 16) * 16
    block_norms = res_norm.shape[0]
    tokens = peers * band
    last = chans // CK - 1
    half = CK // 2
    pieces = [(chunk * CK, CK) for chunk in range(last)] + [(last * CK, half), (last * CK + half, half)]
    count = float(tokens * (chans // groups))
    tiles = tokens // TM

    def kernel(lat, time_hbm, ctx_hbm, kern, wtime, norm_hbm, attn_hbm, ckv, out_ref, norm_ref, bias_ref, ctx_k, ctx_v,
               image, own, act, wbuf, acc, time_ref, tproj, rows, mine, stats, coef, norm_raw, attn_raw, ctx_raw, ctx_mine, ckv_buf,
               wsem, tsem, own_sem, small_sem, ctx_sem, send_sem, recv_sem, stat_send, stat_recv):
        me = lax.axis_index('sp')
        mid = own
        load = [pltpu.make_async_copy(lat.at[peer], own.at[pl.ds(peer * band, band), :], own_sem) for peer in range(peers)]
        start_all(load)
        small = [pltpu.make_async_copy(src, dst, small_sem.at[index]) for index, (src, dst) in enumerate(((time_hbm, time_ref), (norm_hbm, norm_raw), (attn_hbm, attn_raw)))]
        start_all(small)
        weight = time_copy(wtime, which, wbuf, tsem)
        weight.start()
        start_all(fetch_rows(kern, which, 0, 0, wbuf, wsem))
        ctx_copies = [pltpu.make_async_copy(ctx_hbm, ctx_raw, ctx_sem.at[0]), pltpu.make_async_copy(ckv, ckv_buf, ctx_sem.at[1])]
        start_all(ctx_copies)
        meet(peers, me)
        clear_edges(act, width)
        member = members(chans, groups)
        own_rows = pl.ds(pl.multiple_of(me * band, band), band)
        await_peers(peers)

        def send(index):
            first, wide = pieces[index]

            @pl.loop(1, peers)
            def _(step):
                peer = lax.rem(me + step, peers)
                remote(lat.at[peer, :, pl.ds(first, wide)], image.at[own_rows, pl.ds(first, wide)], send_sem.at[index], recv_sem.at[index], peer).start()

        send(0)
        wait_all(load)

        @loop(peers)
        def _(peer):
            vals = own[pl.ds(pl.multiple_of(peer * band, band), band), :].astype(F32).reshape(band // 8, 8, chans)
            rows[pl.ds(peer, 1), :] = keep_sum(jnp.sum(vals, axis=0))
            rows[pl.ds(peers + peer, 1), :] = keep_sum(jnp.sum(vals * vals, axis=0))

        sums = group_sums(rows[...], member)
        for peer in range(peers):
            mine[peer, 0:1, :] = sums[peer:peer + 1]
            mine[peer, 1:2, :] = sums[peers + peer:peers + peer + 1]

        @pl.loop(1, peers)
        def _(step):
            peer = lax.rem(me + step, peers)
            remote(mine.at[peer], stats.at[me], stat_send, stat_recv, peer).start()

        for index in range(1, len(pieces)):
            send(index)
        image[own_rows, :] = own[own_rows, :]
        stats[me] = mine[me]
        wait_all(small)
        for index in range(block_norms):
            norm_ref[index:index + 1, :] = widen(norm_raw[index], chans)
        for index in range(2):
            norm_ref[block_norms + index:block_norms + index + 1, :] = widen(attn_raw[index], chans)
        weight.wait()
        rows[0:1, :] = time_row(time_ref, wbuf, tproj, me)
        weight = time_copy(wtime, other, wbuf, tsem)
        weight.start()
        acc[...] = jnp.zeros_like(acc)
        ctx_copies[0].wait()
        place = (text_rows, text * peers)
        wanted = lax.broadcasted_iota(jnp.int32, place, 0) * peers + me
        pick = one_hot(lax.broadcasted_iota(jnp.int32, place, 1) == wanted)
        ctx_mine[...] = nn(pick, ctx_raw[...]).astype(BF16)
        ctx_copies[1].wait()
        ctx_k[...] = nt(ctx_mine[...], ckv_buf[0]).astype(BF16)

        @loop(chans // 256)
        def _(part):
            part_rows = pl.ds(pl.multiple_of(part * 256, 256), 256)
            ctx_v[part_rows, :] = nt(ckv_buf[1, part_rows, :], ctx_mine[...]).astype(BF16)

        weight.wait()
        bias_ref[...] = time_row(time_ref, wbuf, tproj, me)
        drain(stats.at[pl.ds(0, peers - 1)], stat_recv)
        drain(stats.at[pl.ds(0, peers - 1)], stat_send)
        row = 4 * which
        group_affine(jnp.sum(stats[...], axis=0), norm_ref[row:row + 1], norm_ref[row + 1:row + 2], member, count, coef, 0.5)

        def landed(index):
            first, wide = pieces[index]
            return image.at[pl.ds(0, tokens - band), pl.ds(first, wide)]

        @loop(last)
        def _(chunk):
            @pl.when(chunk + 1 < last)
            def _():
                start_all(fetch_rows(kern, which, 0, chunk + 1, wbuf, wsem))

            @pl.when(chunk + 1 == last)
            def _():
                start_all(fetch_halves(kern, which, 0, last, wbuf, wsem))

            wait_all(fetch_rows(kern, which, 0, chunk, wbuf, wsem))
            drain(image.at[pl.ds(0, tokens - band), chunk_cols(chunk)], recv_sem.at[chunk])

            @loop(tiles)
            def _(tile):
                activate(image, act, coef, pl.multiple_of(chunk * CK, CK), CK, tile * TM, TM, width)

            @loop(tiles)
            def _(tile):
                acc[tile_rows(tile), :] += chunk_product(act, wbuf, lax.rem(chunk, 2), chunk, tile, width)

        wait_all(fetch_halves(kern, which, 0, last, wbuf, wsem))

        @loop(2)
        def _(part):
            first = pl.multiple_of(last * CK + part * half, half)
            drain(image.at[pl.ds(0, tokens - band), pl.ds(first, half)], recv_sem.at[last + part])

            @loop(tiles)
            def _(tile):
                activate(image, act, coef, first, half, tile * TM, TM, width)

            @loop(tiles)
            def _(tile):
                acc[tile_rows(tile), :] += half_product(act, wbuf, last % 2, first, part, tile, width)

        start_all(fetch_rows(kern, which, 1, 0, wbuf, wsem))
        add_and_norm(mid, acc, rows[0:1, :], member, norm_ref, row + 2, count, coef)
        conv_rows(lambda chunk: fetch_rows(kern, which, 1, chunk, wbuf, wsem), mid, act, wbuf, coef, acc, width)
        add_rows(out_ref, acc, image)
        for index in range(len(pieces)):
            drain(landed(index), send_sem.at[index])

    vmem = pl.BlockSpec(memory_space=pltpu.VMEM)
    hbm = pl.BlockSpec(memory_space=pl.ANY)
    dma = pltpu.SemaphoreType.DMA
    return pl.pallas_call(
        kernel,
        out_shape=[
            jax.ShapeDtypeStruct((tokens, chans), BF16),
            jax.ShapeDtypeStruct((block_norms + 8, chans), F32),
            jax.ShapeDtypeStruct((1, chans), F32),
            jax.ShapeDtypeStruct((text_rows, chans), BF16),
            jax.ShapeDtypeStruct((chans, text_rows), BF16),
        ],
        in_specs=[hbm] * 8,
        out_specs=[vmem] * 5,
        scratch_shapes=[
            pltpu.VMEM((tokens, chans), BF16),
            pltpu.VMEM((tokens, chans), BF16),
            pltpu.VMEM((3, tokens + 2 * width, chans), BF16),
            pltpu.VMEM((2, len(taps()) * CK, chans), BF16),
            pltpu.VMEM((tokens, chans), F32),
            pltpu.VMEM(time_emb.shape, BF16),
            pltpu.VMEM((peers, chans), F32),
            pltpu.VMEM((2 * peers, chans), F32),
            pltpu.VMEM((peers, 8, 128), F32),
            pltpu.VMEM((peers, 8, 128), F32),
            pltpu.VMEM((8, chans), F32),
            pltpu.VMEM(res_norm.shape, BF16),
            pltpu.VMEM(attn_norm.shape, BF16),
            pltpu.VMEM(context.shape, BF16),
            pltpu.VMEM((text_rows, text_dim), BF16),
            pltpu.VMEM(cross_kv.shape, BF16),
            dma((2,)), dma, dma, dma((3,)), dma((2,)), dma((len(pieces),)), dma((len(pieces),)), dma, dma,
        ],
        compiler_params=pltpu.CompilerParams(vmem_limit_bytes=VMEM_IN, collective_id=0, has_side_effects=True),
        cost_estimate=cost_of(36 * tokens * chans * chans, 36 * chans * chans),
        name='res_block_in',
    )(latent, time_emb, context, res_conv, res_time, res_norm, attn_norm, cross_kv)


def res_block_out(hidden, bias, res_conv, norms, width, groups, peers):
    which = 1
    tokens, chans = hidden.shape
    band = tokens // peers
    chunks = chans // CK
    tiles = tokens // TM
    per_tile = TM // band
    count = float(tokens * (chans // groups))

    def kernel(x_ref, bias_ref, kern, norm_ref, out_ref, mid, result, act, wbuf, cbuf, acc, coef, wsem, csem, send_sem, recv_sem):
        me = lax.axis_index('sp')
        start_all(fetch_rows(kern, which, 0, 0, wbuf, wsem))
        meet(peers, me)
        clear_edges(act, width)
        member = members(chans, groups)
        row = 4 * which
        acc[...] = jnp.zeros_like(acc)
        norm_from(x_ref, member, norm_ref, row, count, coef)
        conv_rows(lambda chunk: fetch_rows(kern, which, 0, chunk, wbuf, wsem), x_ref, act, wbuf, coef, acc, width)
        start_all(fetch_cols(kern, which, 1, 0, cbuf, csem))
        add_and_norm(mid, acc, bias_ref[...], member, norm_ref, row + 2, count, coef)

        def build(row, rows):
            @loop(chunks)
            def _(chunk):
                activate(mid, act, coef, pl.multiple_of(chunk * CK, CK), CK, row, rows, width)

        def build_tile(tile):
            build(tile * TM, TM)

            @pl.when(tile + 1 < tiles)
            def _():
                build((tile + 1) * TM, width)

        turn = lax.rem(lax.div(me, per_tile) + tiles // 2, tiles)
        build_tile(turn)

        @pl.when(turn > 0)
        def _():
            build(turn * TM - width, width)

        await_peers(peers)

        @loop(chunks)
        def _(chunk):
            slot = lax.rem(chunk, 2)
            cols = chunk_cols(chunk)

            @pl.when(chunk + 1 < chunks)
            def _():
                start_all(fetch_cols(kern, which, 1, chunk + 1, cbuf, csem))

            wait_all(fetch_cols(kern, which, 1, chunk, cbuf, csem))

            @loop(tiles)
            def _(step):
                tile = lax.rem(step + turn, tiles)
                part = sum(nn(shifted(act, dx, tile, dy, width, slice(None)), cbuf[slot, tap]) for tap, (dy, dx) in enumerate(taps()))
                rows = tile_rows(tile)
                result[rows, cols] = (x_ref[rows, cols].astype(F32) + part).astype(BF16)
                for idx in range(per_tile):
                    peer = tile * per_tile + idx
                    block = result.at[pl.ds(pl.multiple_of(peer * band, band), band), cols]

                    @pl.when(peer == me)
                    def _():
                        out_ref[me, :, cols] = block[...]

                    @pl.when(peer != me)
                    def _():
                        remote(block, out_ref.at[me, :, cols], send_sem, recv_sem, peer).start()

                @pl.when((chunk == 0) & (step + 1 < tiles))
                def _():
                    build_tile(lax.rem(step + 1 + turn, tiles))

        others = out_ref.at[pl.ds(0, peers - 1)]
        drain(others, send_sem)
        drain(others, recv_sem)

    vmem = pl.BlockSpec(memory_space=pltpu.VMEM)
    hbm = pl.BlockSpec(memory_space=pl.ANY)
    dma = pltpu.SemaphoreType.DMA
    return pl.pallas_call(
        kernel,
        out_shape=jax.ShapeDtypeStruct((peers, band, chans), BF16),
        in_specs=[vmem, vmem, hbm, vmem],
        out_specs=vmem,
        scratch_shapes=[
            pltpu.VMEM((tokens, chans), BF16),
            pltpu.VMEM((tokens, chans), BF16),
            pltpu.VMEM((3, tokens + 2 * width, chans), BF16),
            pltpu.VMEM((2, len(taps()) * CK, chans), BF16),
            pltpu.VMEM((2, len(taps()), chans, CK), BF16),
            pltpu.VMEM((tokens, chans), F32),
            pltpu.VMEM((8, chans), F32),
            dma((2,)), dma((2,)), dma, dma,
        ],
        compiler_params=pltpu.CompilerParams(vmem_limit_bytes=VMEM_OUT, collective_id=1, has_side_effects=True),
        cost_estimate=cost_of(36 * tokens * chans * chans, 36 * chans * chans),
        name='res_block_out',
    )(hidden, bias, res_conv, norms)


def cost_of(flops, nbytes):
    return pl.CostEstimate(flops=flops, bytes_accessed=nbytes, transcendentals=0)


def transformer(hidden, ctx_keys, ctx_vals, norms, norm_row, proj_inout, qkv_t, self_out, cross_q_t, cross_out, ff_in, ff_out, groups, heads, text):
    tokens, chans = hidden.shape
    text_rows = ctx_keys.shape[0]
    head_dim = chans // heads
    pairs = heads // 2
    pair = 2 * head_dim
    count = float(tokens * (chans // groups))
    tiles = tokens // TM
    ff_steps = ff_out.shape[0] // chans
    qw = 512 if chans >= 1024 else 256
    kb = 256
    scale = head_dim ** -0.5
    half = chans // 2

    def kernel(h_ref, ctx_k, ctx_v, norm_ref, pio, wqkv, wo, cq, co, f1, f2, out_ref, ring, tok, aux, both, keys, acc, coef, rsem):
        units = {
            'in': (pio.at[0], 0, 0), 'q': (wqkv.at[0], 0, 1), 'k': (wqkv.at[1], 1, 0), 'v': (wqkv.at[2], 1, 1),
            'o': (wo, 1, 0), 'cq': (cq, 1, 1), 'co': (co, 1, 2), 'out': (pio.at[1], 0, 0),
        }

        def copy_of(name):
            src, group, place = units[name]
            return pltpu.make_async_copy(src, ring.at[group, place], rsem.at[group, place])

        def start(*names):
            for name in names:
                copy_of(name).start()

        def take(name):
            copy_of(name).wait()
            _, group, place = units[name]
            return ring.at[group, place]

        def ff_copies(step, group):
            cols = pl.multiple_of(step * chans, chans)
            return [
                pltpu.make_async_copy(f1.at[:, pl.ds(cols, chans)], ring.at[group, 0], rsem.at[group, 0]),
                pltpu.make_async_copy(f1.at[:, pl.ds(cols + ff_steps * chans, chans)], ring.at[group, 1], rsem.at[group, 1]),
                pltpu.make_async_copy(f2.at[pl.ds(cols, chans), :], ring.at[group, 2], rsem.at[group, 2]),
            ]

        start('in', 'q', 'k', 'v', 'co')

        tot, sqr = channel_sums(h_ref, tokens, chans)
        member = members(chans, groups)
        sums = group_sums(two_rows(tot, sqr), member)
        group_affine(sums, norm_ref[norm_row:norm_row + 1], norm_ref[norm_row + 1:norm_row + 2], member, count, coef, 1.0)

        def project_rows(weight, src, base, normed_to, clear=None):
            def norm_tile(tile):
                rows = tile_rows(tile)
                normed_to[rows, :] = layer_norm(tok[rows, :].astype(F32))

            @loop(tiles)
            def _(tile):
                norm_tile(jnp.maximum(tile - 1, 0))
                rows = tile_rows(tile)
                tok[rows, :] = (base(rows) + nn(src(rows), weight[...])).astype(BF16)
                if clear is not None:
                    clear[rows, :] = jnp.zeros((TM, chans), F32)

            norm_tile(tiles - 1)

        project_rows(take('in'), lambda rows: (h_ref[rows, :].astype(F32) * coef[0:1] + coef[1:2]).astype(BF16), lambda rows: 0.0, aux)

        q_t, v_t = both.at[0], both.at[1]

        def transposed(weight, src, dst, factor):
            @loop(2)
            def _(part):
                rows = pl.ds(pl.multiple_of(part * half, half), half)
                dst[rows, :] = (nt(weight[rows, :], src[...]).astype(BF16) * factor).astype(BF16)

        w_key = take('k')

        @loop(tokens // 512)
        def _(part):
            rows = pl.ds(pl.multiple_of(part * 512, 512), 512)
            keys[rows, :] = nt(aux[rows, :], w_key[...]).astype(BF16)
        start('o')

        @loop(2)
        def _(which):
            pltpu.make_async_copy(wqkv.at[2 * which], ring.at[which, 1], rsem.at[which, 1]).wait()
            transposed(ring.at[which, 1], aux, both.at[which], jnp.where(which == 0, scale, 1.0))
        start('cq')
        for copy in ff_copies(0, 0):
            copy.start()

        row_head = lax.broadcasted_iota(jnp.int32, (pair, 1), 0) < head_dim

        def query_of(hp, first, wide, head):
            both = q_t[pl.ds(pl.multiple_of(hp * pair, pair), pair), pl.ds(first, wide)]
            keep = row_head if head == 0 else jnp.logical_not(row_head)
            return jnp.where(keep, both, jnp.zeros_like(both))

        def pair_cols(hp):
            return pl.ds(pl.multiple_of(hp * pair, pair), pair)

        halves = tokens // qw
        blocks = pairs * halves
        unroll = next(count for count in (5, 4, 2, 1) if blocks % count == 0)
        scores = [acc.at[:, pl.ds(h * qw, qw)] for h in range(2)]
        probs = [out_ref.at[:, pl.ds(h * qw, qw)] for h in range(2)]
        parts = tokens // kb

        def place(block):
            hp = lax.div(block, halves)
            return hp, pl.multiple_of((block - hp * halves) * qw, qw)

        def fold(vals, func):
            return func(vals.reshape(-1, 8, vals.shape[-1]), axis=0)

        def score_part(block, query, head, part):
            hp, _ = place(block)
            vals = nn(keys[part * kb:(part + 1) * kb, pair_cols(hp)], query)
            scores[head][part * kb:(part + 1) * kb, :] = vals
            return fold(vals, jnp.max)

        def exp_part(head, part, top):
            vals = jnp.exp(scores[head][part * kb:(part + 1) * kb, :] - top)
            probs[head][part * kb:(part + 1) * kb, :] = vals.astype(BF16)
            return fold(vals, jnp.sum)

        def value_of(block, head, denom):
            hp, _ = place(block)
            vals = v_t[pl.ds(pl.multiple_of(hp * pair + head * head_dim, head_dim), head_dim), :]
            return nn(vals, probs[head][...]) * (1.0 / denom)

        def block_query(block, head):
            hp, first = place(block)
            return query_of(hp, first, qw, head)

        def softmax_stage(score_block, score_head, exp_head, top):
            tops, sums = [], []
            query = block_query(score_block, score_head)
            for part in range(parts):
                tops.append(score_part(score_block, query, score_head, part))
                sums.append(exp_part(exp_head, part, top))
            new_top = jnp.max(functools.reduce(jnp.maximum, tops), axis=0, keepdims=True)
            return new_top, keep_sum(functools.reduce(jnp.add, sums))

        def emit(block, low, high):
            hp, first = place(block)
            aux[pl.ds(first, qw), pair_cols(hp)] = jnp.concatenate([low, high], axis=0).T.astype(BF16)

        top_first = jnp.max(functools.reduce(jnp.maximum, [score_part(0, block_query(0, 0), 0, part) for part in range(parts)]), axis=0, keepdims=True)
        zero_row = jnp.ones((1, qw), F32)
        zero_out = jnp.zeros((head_dim, qw), F32)

        def attend_block(block, carry):
            top0, denom1, low = carry
            before = jnp.maximum(block - 1, 0)
            high = value_of(before, 1, denom1)
            emit(before, low, high)
            top1, denom0 = softmax_stage(block, 1, 0, top0)
            after = jnp.minimum(block + 1, blocks - 1)
            low = value_of(block, 0, denom0)
            top0, denom1 = softmax_stage(after, 0, 1, top1)
            return top0, denom1, low

        def attend_blocks(step, carry):
            for sub in range(unroll):
                carry = attend_block(step * unroll + sub, carry)
            return carry

        _, denom1, low = lax.fori_loop(0, blocks // unroll, attend_blocks, (top_first, zero_row, zero_out))
        emit(blocks - 1, low, value_of(blocks - 1, 1, denom1))

        project_rows(take('o'), lambda rows: aux[rows, :], lambda rows: tok[rows, :].astype(F32), keys)
        transposed(take('cq'), keys, q_t, scale)

        text_valid = lax.broadcasted_iota(jnp.int32, (text_rows, 1), 0) < text

        wide_step = max(count for count in (CROSS_PAIRS, 2, 1) if pairs % count == 0)

        @loop(pairs // wide_step)
        def _(step):
            for sub in range(wide_step):
                hp = step * wide_step + sub
                outs = []
                for head in range(2):
                    vals = nn(ctx_k[:, pair_cols(hp)], query_of(hp, 0, tokens, head))
                    vals = jnp.where(text_valid, vals, -jnp.inf)
                    weights = jnp.exp(vals - jnp.max(vals, axis=0, keepdims=True))
                    denom = keep_sum(weights)
                    text_vals = ctx_v[pl.ds(pl.multiple_of(hp * pair + head * head_dim, head_dim), head_dim), :]
                    outs.append(nn(text_vals, weights.astype(BF16)) * (1.0 / denom))
                aux[:, pair_cols(hp)] = jnp.concatenate(outs, axis=0).T.astype(BF16)

        project_rows(take('co'), lambda rows: aux[rows, :], lambda rows: tok[rows, :].astype(F32), keys, acc)
        for copy in ff_copies(1, 1):
            copy.start()

        @loop(ff_steps)
        def _(step):
            group = lax.rem(step, 2)
            for copy in ff_copies(step, group):
                copy.wait()

            @loop(tiles, unroll=2)
            def _(tile):
                rows = tile_rows(tile)
                src = keys[rows, :]
                value = nn(src, ring[group, 0])
                gate = nn(src, ring[group, 1])
                gated = (value * (0.5 * gate * (1.0 + lax.erf(gate * (0.5 ** 0.5))))).astype(BF16)
                acc[rows, :] += nn(gated, ring[group, 2])

            @pl.when(step + 2 < ff_steps)
            def _():
                for copy in ff_copies(step + 2, group):
                    copy.start()

            @pl.when(step == ff_steps - 2)
            def _():
                start('out')

        w_fin = take('out')

        @loop(tiles)
        def _(tile):
            rows = tile_rows(tile)
            t = (tok[rows, :].astype(F32) + acc[rows, :]).astype(BF16)
            out_ref[rows, :] = (h_ref[rows, :].astype(F32) + nn(t, w_fin[...])).astype(BF16)

    vmem = pl.BlockSpec(memory_space=pltpu.VMEM)
    hbm = pl.BlockSpec(memory_space=pl.ANY)
    flops = 2 * tokens * chans * chans * (8 + 3 * ff_steps) + 4 * tokens * tokens * chans
    return pl.pallas_call(
        kernel,
        out_shape=jax.ShapeDtypeStruct(hidden.shape, BF16),
        in_specs=[vmem] * 4 + [hbm] * 7,
        out_specs=vmem,
        scratch_shapes=[
            pltpu.VMEM((2, 3, chans, chans), BF16),
            pltpu.VMEM((tokens, chans), BF16),
            pltpu.VMEM((tokens, chans), BF16),
            pltpu.VMEM((2, chans, tokens), BF16),
            pltpu.VMEM((tokens, chans), BF16),
            pltpu.VMEM((tokens, chans), F32),
            pltpu.VMEM((8, chans), F32),
            pltpu.SemaphoreType.DMA((2, 3)),
        ],
        compiler_params=pltpu.CompilerParams(vmem_limit_bytes=VMEM_MID),
        cost_estimate=cost_of(flops, 50 * chans * chans),
        name='transformer',
    )(hidden, ctx_keys, ctx_vals, norms, proj_inout, qkv_t, self_out, cross_q_t, cross_out, ff_in, ff_out)


def solution(mesh):
    num_bands = mesh.shape['sp']

    def local_stage(latent, time_emb, context, res_conv, res_time, res_norm, attn_norm, proj_inout, self_qkv, self_out, cross_q, cross_kv, cross_out, ff_in, ff_out):
        images, band_rows, width, chans = latent.shape
        assert images == num_bands
        band = band_rows * width
        heads, head_dim = self_out.shape[:2]
        groups = res_norm.shape[3]
        text, text_dim = context.shape[1:]
        flat_kv = jnp.transpose(cross_kv, (0, 2, 3, 1)).reshape(2, chans, text_dim)
        first, norms, bias, ctx_keys, ctx_vals = res_block_in(
            latent.reshape(images, band, chans), pltpu.with_memory_space_constraint(time_emb, pltpu.HBM), jnp.transpose(context, (1, 0, 2)).reshape(text * images, text_dim), res_conv, res_time,
            pltpu.with_memory_space_constraint(res_norm.reshape((-1,) + res_norm.shape[3:]), pltpu.HBM), pltpu.with_memory_space_constraint(attn_norm, pltpu.HBM), flat_kv, text, width)
        middle = transformer(
            first, ctx_keys, ctx_vals, norms, res_norm.shape[0] * res_norm.shape[1] * res_norm.shape[2], proj_inout,
            jnp.transpose(self_qkv, (0, 2, 3, 1)).reshape(3, chans, chans),
            self_out.reshape(chans, chans),
            jnp.transpose(cross_q, (1, 2, 0)).reshape(chans, chans),
            cross_out.reshape(chans, chans), ff_in, ff_out, groups, heads, text)
        out = res_block_out(middle, bias, res_conv, norms, width, groups, num_bands)
        return out.reshape(latent.shape)

    band_spec = P('dp', 'sp', None, None)
    shared = P()
    in_specs = (band_spec, P('dp', None), P('dp', None, None)) + (shared,) * 12
    return jax.shard_map(local_stage, mesh=mesh, in_specs=in_specs, out_specs=band_spec, check_vma=False)
```

```python
import functools

import jax
import jax.numpy as jnp
from jax import lax
from jax.experimental import pallas as pl
from jax.experimental.pallas import tpu as pltpu
from jax.sharding import PartitionSpec as P

BF16 = jnp.bfloat16
F32 = jnp.float32
MESH = pl.DeviceIdType.MESH
GN_EPS = 1e-6
LN_EPS = 1e-5
TM = 256
CK = 256
STEP = 64
CROSS_PAIRS = 5
VMEM_IN, VMEM_MID, VMEM_OUT = 53_000_000, 48_000_000, 49_000_000


def loop(stop, **options):
    return pl.loop(0, stop, **options)


def one_hot(mask):
    return mask.astype(F32).astype(BF16)


def keep_sum(vals):
    return jnp.sum(vals, axis=0, keepdims=True)


def nn(lhs, rhs):
    return jnp.dot(lhs, rhs, preferred_element_type=F32)


def nt(lhs, rhs):
    return lax.dot_general(lhs, rhs, (((1,), (1,)), ((), ())), preferred_element_type=F32)


def split3(vals):
    high = vals.astype(BF16).astype(F32)
    rest = vals - high
    mid = rest.astype(BF16).astype(F32)
    return [high, mid, rest - mid]


def channel_sums(src, rows, chans):
    def step(idx, carry):
        tot, sqr = carry
        vals = src[pl.ds(pl.multiple_of(idx * 64, 64), 64), :].astype(F32).reshape(8, 8, chans)
        return tot + jnp.sum(vals, axis=0), sqr + jnp.sum(vals * vals, axis=0)

    zero = jnp.zeros((8, chans), F32)
    return lax.fori_loop(0, rows // 64, step, (zero, zero))


def layer_norm(tokens):
    centred = tokens - jnp.mean(tokens, axis=-1, keepdims=True)
    return (centred * lax.rsqrt(jnp.mean(centred * centred, axis=-1, keepdims=True) + LN_EPS)).astype(BF16)


def meet(peers, me):
    barrier = pltpu.get_barrier_semaphore()

    @pl.loop(1, peers)
    def _(step):
        pl.semaphore_signal(barrier, inc=1, device_id={'sp': lax.rem(me + step, peers)}, device_id_type=MESH)


def far_first(step, peers):
    hop = lax.div(step, 2)
    return peers // 2 + jnp.where(lax.rem(step, 2) == 1, hop, -hop)


def await_peers(peers):
    pl.semaphore_wait(pltpu.get_barrier_semaphore(), peers - 1)


def drain(ref, sem):
    pltpu.make_async_copy(ref, ref, sem).wait()


def remote(src, dst, send_sem, recv_sem, peer):
    return pltpu.make_async_remote_copy(src, dst, send_sem, recv_sem, device_id={'sp': peer}, device_id_type=MESH)


def chunk_cols(chunk):
    return pl.ds(pl.multiple_of(chunk * CK, CK), CK)


def tile_rows(tile, first=0):
    return pl.ds(pl.multiple_of(first + tile * TM, 32), TM)


def members(chans, groups, offset=0):
    width = chans // groups
    chan = lax.broadcasted_iota(jnp.int32, (chans, 128), 0)
    low = (lax.broadcasted_iota(jnp.int32, (chans, 128), 1) - offset) * width
    return one_hot((chan >= low) & (chan < low + width))


def group_sums(rows, member):
    count = rows.shape[0]
    high, mid, low = split3(rows)
    sums = nn(jnp.concatenate([high, mid, low], axis=0).astype(BF16), member)
    return sums[0:count] + sums[count:2 * count] + sums[2 * count:3 * count]


def group_affine(sums, gain, shift, member, count, coef, factor):
    mean = sums[0:1] / count
    rstd = lax.rsqrt(sums[1:2] / count - mean * mean + GN_EPS)
    back = jnp.concatenate(split3(mean) + split3(rstd) + [jnp.zeros((2, 128), F32)], axis=0).astype(BF16)
    wide = nt(back, member)
    scale = keep_sum(wide[3:6]) * gain
    coef[0:1, :] = factor * scale
    coef[1:2, :] = factor * (shift - keep_sum(wide[:3]) * scale)


def two_rows(tot, sqr):
    rows = [keep_sum(tot), keep_sum(sqr)]
    return jnp.concatenate(rows + [jnp.zeros((6, tot.shape[1]), F32)], axis=0)


def activate(src, act, coef, first, wide, row, count, width):
    cols = pl.ds(first, wide)
    half = src[pl.ds(pl.multiple_of(row, width), count), cols].astype(F32) * coef[0:1, cols] + coef[1:2, cols]
    vals = half + half * jnp.tanh(half)
    column = lax.rem(lax.broadcasted_iota(jnp.int32, (count, wide), 0), width)
    put = pl.ds(pl.multiple_of(row + width, width), count)
    act[0, put, cols] = jnp.where(column == 0, 0.0, pltpu.roll(vals, 1, 0)).astype(BF16)
    act[1, put, cols] = vals.astype(BF16)
    act[2, put, cols] = jnp.where(column == width - 1, 0.0, pltpu.roll(vals, count - 1, 0)).astype(BF16)


def clear_edges(act, width):
    edge = jnp.zeros((width, act.shape[2]), BF16)
    for shift in range(3):
        act[shift, 0:width, :] = edge
        act[shift, act.shape[1] - width:act.shape[1], :] = edge


def shifted(act, shift, tile, row, width, cols):
    return act[shift, tile_rows(tile, row * width), cols]


def taps():
    return [(dy, dx) for dy in range(3) for dx in range(3)]


def fetch_rows(kern, which, conv, chunk, wbuf, sem):
    slot = lax.rem(chunk, 2)
    return [pltpu.make_async_copy(kern.at[which, conv, dy, dx, chunk_cols(chunk), :], wbuf.at[slot, pl.ds(tap * CK, CK), :], sem.at[slot])
            for tap, (dy, dx) in enumerate(taps())]


def fetch_halves(kern, which, conv, chunk, wbuf, sem):
    slot, half, count = lax.rem(chunk, 2), CK // 2, len(taps())
    return [pltpu.make_async_copy(kern.at[which, conv, dy, dx, pl.ds(chunk * CK + part * half, half), :], wbuf.at[slot, pl.ds((part * count + tap) * half, half), :], sem.at[slot])
            for part in range(2) for tap, (dy, dx) in enumerate(taps())]


def fetch_cols(kern, which, conv, chunk, wbuf, sem):
    slot = lax.rem(chunk, 2)
    return [pltpu.make_async_copy(kern.at[which, conv, dy, dx, :, chunk_cols(chunk)], wbuf.at[slot, tap], sem.at[slot])
            for tap, (dy, dx) in enumerate(taps())]


def start_all(copies):
    for copy in copies:
        copy.start()


def wait_all(copies):
    for copy in copies:
        copy.wait()


def chunk_product(act, wbuf, slot, chunk, tile, width):
    cols = chunk_cols(chunk)
    return sum(nn(shifted(act, dx, tile, dy, width, cols), wbuf[slot, tap * CK:(tap + 1) * CK, :]) for tap, (dy, dx) in enumerate(taps()))


def half_product(act, wbuf, slot, first, part, tile, width):
    depth = len(taps()) * (CK // 2)
    rows = jnp.concatenate([shifted(act, dx, tile, dy, width, pl.ds(first, CK // 2)) for dy, dx in taps()], axis=1)
    return nn(rows, wbuf[slot, pl.ds(pl.multiple_of(part * depth, depth), depth), :])


def conv_rows(fetch, src, act, wbuf, coef, acc, width):
    tokens, chans = acc.shape
    chunks = chans // CK

    def build(chunk, tile):
        activate(src, act, coef, pl.multiple_of(chunk * CK, CK), CK, tile * TM, TM, width)

    @loop(tokens // TM)
    def _(tile):
        build(0, tile)

    @loop(chunks)
    def _(chunk):
        @pl.when(chunk + 1 < chunks)
        def _():
            start_all(fetch(chunk + 1))

        wait_all(fetch(chunk))

        @loop(tokens // TM)
        def _(tile):
            acc[tile_rows(tile), :] += chunk_product(act, wbuf, lax.rem(chunk, 2), chunk, tile, width)
            build(lax.rem(chunk + 1, chunks), tile)


def add_rows(dst, acc, other):
    @loop(acc.shape[0] // 64)
    def _(idx):
        rows = pl.ds(pl.multiple_of(idx * 64, 64), 64)
        dst[rows, :] = (other[rows, :].astype(F32) + acc[rows, :]).astype(BF16)


def time_copy(res_time, which, wbuf, sem):
    return pltpu.make_async_copy(res_time.at[which], wbuf.at[1, pl.ds(0, res_time.shape[1]), :], sem)


def time_row(time_ref, wbuf, tproj, image):
    emb = time_ref[...].astype(F32)
    act = (emb / (1.0 + jnp.exp(-emb))).astype(BF16)
    tproj[...] = nn(act, wbuf[1, 0:act.shape[1], :])
    return tproj[pl.ds(image, 1), :]


def widen(param, chans):
    groups, width = param.shape
    group = lax.broadcasted_iota(jnp.int32, (groups, chans), 0) * width
    chan = lax.broadcasted_iota(jnp.int32, (groups, chans), 1)
    spread = one_hot((chan >= group) & (chan < group + width))
    wide = lax.dot_general(param, spread, (((0,), (0,)), ((), ())), preferred_element_type=F32)
    place = lax.broadcasted_iota(jnp.int32, (width, chans), 0)
    inside = lax.rem(lax.broadcasted_iota(jnp.int32, (width, chans), 1), width)
    return keep_sum(jnp.where(place == inside, wide, 0.0))


def norm_from(src, member, norm_ref, row, count, coef):
    tot, sqr = channel_sums(src, src.shape[0], src.shape[1])
    group_affine(group_sums(two_rows(tot, sqr), member), norm_ref[row:row + 1], norm_ref[row + 1:row + 2], member, count, coef, 0.5)


def add_and_norm(mid, acc, bias, member, norm_ref, row, count, coef):
    def step(idx, carry):
        rows = pl.ds(pl.multiple_of(idx * 64, 64), 64)
        rounded = (acc[rows, :] + bias).astype(BF16)
        mid[rows, :] = rounded
        acc[rows, :] = jnp.zeros((STEP, acc.shape[1]), F32)
        vals = rounded.astype(F32).reshape(8, 8, acc.shape[1])
        return carry[0] + jnp.sum(vals, axis=0), carry[1] + jnp.sum(vals * vals, axis=0)

    zero = jnp.zeros((8, acc.shape[1]), F32)
    tot, sqr = lax.fori_loop(0, acc.shape[0] // 64, step, (zero, zero))
    group_affine(group_sums(two_rows(tot, sqr), member), norm_ref[row:row + 1], norm_ref[row + 1:row + 2], member, count, coef, 0.5)


def res_block_in(latent, time_emb, context, res_conv, res_time, res_norm, attn_norm, cross_kv, text, width):
    which, other = 0, 1
    peers, band, chans = latent.shape
    groups = res_norm.shape[1]
    text_dim = context.shape[1]
    text_rows = -(-text // 16) * 16
    block_norms = res_norm.shape[0]
    tokens = peers * band
    last = chans // CK - 1
    half = CK // 2
    pieces = [(chunk * CK, CK) for chunk in range(last)] + [(last * CK, half), (last * CK + half, half)]
    count = float(tokens * (chans // groups))
    tiles = tokens // TM

    def kernel(lat, time_hbm, ctx_hbm, kern, wtime, norm_hbm, attn_hbm, ckv, out_ref, norm_ref, bias_ref, ctx_k, ctx_v,
               image, own, act, wbuf, acc, time_ref, tproj, rows, mine, stats, coef, norm_raw, attn_raw, ctx_raw, ctx_mine, ckv_buf,
               wsem, tsem, own_sem, small_sem, ctx_sem, send_sem, recv_sem, stat_send, stat_recv):
        me = lax.axis_index('sp')
        mid = own
        load = [pltpu.make_async_copy(lat.at[peer], own.at[pl.ds(peer * band, band), :], own_sem) for peer in range(peers)]
        start_all(load)
        small = [pltpu.make_async_copy(src, dst, small_sem.at[index]) for index, (src, dst) in enumerate(((time_hbm, time_ref), (norm_hbm, norm_raw), (attn_hbm, attn_raw)))]
        start_all(small)
        weight = time_copy(wtime, which, wbuf, tsem)
        weight.start()
        start_all(fetch_rows(kern, which, 0, 0, wbuf, wsem))
        ctx_copies = [pltpu.make_async_copy(ctx_hbm, ctx_raw, ctx_sem.at[0]), pltpu.make_async_copy(ckv, ckv_buf, ctx_sem.at[1])]
        start_all(ctx_copies)
        meet(peers, me)
        clear_edges(act, width)
        member = members(chans, groups)
        own_rows = pl.ds(pl.multiple_of(me * band, band), band)
        await_peers(peers)

        def send(index):
            first, wide = pieces[index]

            @pl.loop(1, peers)
            def _(step):
                peer = lax.rem(me + far_first(step, peers), peers)
                remote(lat.at[peer, :, pl.ds(first, wide)], image.at[own_rows, pl.ds(first, wide)], send_sem.at[index], recv_sem.at[index], peer).start()

        send(0)
        wait_all(load)

        @loop(peers)
        def _(peer):
            vals = own[pl.ds(pl.multiple_of(peer * band, band), band), :].astype(F32).reshape(band // 8, 8, chans)
            rows[pl.ds(peer, 1), :] = keep_sum(jnp.sum(vals, axis=0))
            rows[pl.ds(peers + peer, 1), :] = keep_sum(jnp.sum(vals * vals, axis=0))

        sums = group_sums(rows[...], member)
        for peer in range(peers):
            mine[peer, 0:1, :] = sums[peer:peer + 1]
            mine[peer, 1:2, :] = sums[peers + peer:peers + peer + 1]

        @pl.loop(1, peers)
        def _(step):
            peer = lax.rem(me + step, peers)
            remote(mine.at[peer], stats.at[me], stat_send, stat_recv, peer).start()

        for index in range(1, len(pieces)):
            send(index)
        image[own_rows, :] = own[own_rows, :]
        stats[me] = mine[me]
        wait_all(small)
        for index in range(block_norms):
            norm_ref[index:index + 1, :] = widen(norm_raw[index], chans)
        for index in range(2):
            norm_ref[block_norms + index:block_norms + index + 1, :] = widen(attn_raw[index], chans)
        weight.wait()
        rows[0:1, :] = time_row(time_ref, wbuf, tproj, me)
        weight = time_copy(wtime, other, wbuf, tsem)
        weight.start()
        acc[...] = jnp.zeros_like(acc)
        ctx_copies[0].wait()
        place = (text_rows, text * peers)
        wanted = lax.broadcasted_iota(jnp.int32, place, 0) * peers + me
        pick = one_hot(lax.broadcasted_iota(jnp.int32, place, 1) == wanted)
        ctx_mine[...] = nn(pick, ctx_raw[...]).astype(BF16)
        ctx_copies[1].wait()
        ctx_k[...] = nt(ctx_mine[...], ckv_buf[0]).astype(BF16)

        @loop(chans // 256)
        def _(part):
            part_rows = pl.ds(pl.multiple_of(part * 256, 256), 256)
            ctx_v[part_rows, :] = nt(ckv_buf[1, part_rows, :], ctx_mine[...]).astype(BF16)

        weight.wait()
        bias_ref[...] = time_row(time_ref, wbuf, tproj, me)
        drain(stats.at[pl.ds(0, peers - 1)], stat_recv)
        drain(stats.at[pl.ds(0, peers - 1)], stat_send)
        row = 4 * which
        group_affine(jnp.sum(stats[...], axis=0), norm_ref[row:row + 1], norm_ref[row + 1:row + 2], member, count, coef, 0.5)

        def landed(index):
            first, wide = pieces[index]
            return image.at[pl.ds(0, tokens - band), pl.ds(first, wide)]

        @loop(last)
        def _(chunk):
            @pl.when(chunk + 1 < last)
            def _():
                start_all(fetch_rows(kern, which, 0, chunk + 1, wbuf, wsem))

            @pl.when(chunk + 1 == last)
            def _():
                start_all(fetch_halves(kern, which, 0, last, wbuf, wsem))

            wait_all(fetch_rows(kern, which, 0, chunk, wbuf, wsem))
            drain(image.at[pl.ds(0, tokens - band), chunk_cols(chunk)], recv_sem.at[chunk])

            @loop(tiles)
            def _(tile):
                activate(image, act, coef, pl.multiple_of(chunk * CK, CK), CK, tile * TM, TM, width)

            @loop(tiles)
            def _(tile):
                acc[tile_rows(tile), :] += chunk_product(act, wbuf, lax.rem(chunk, 2), chunk, tile, width)

        wait_all(fetch_halves(kern, which, 0, last, wbuf, wsem))

        @loop(2)
        def _(part):
            first = pl.multiple_of(last * CK + part * half, half)
            drain(image.at[pl.ds(0, tokens - band), pl.ds(first, half)], recv_sem.at[last + part])

            @loop(tiles)
            def _(tile):
                activate(image, act, coef, first, half, tile * TM, TM, width)

            @loop(tiles)
            def _(tile):
                acc[tile_rows(tile), :] += half_product(act, wbuf, last % 2, first, part, tile, width)

        start_all(fetch_rows(kern, which, 1, 0, wbuf, wsem))
        add_and_norm(mid, acc, rows[0:1, :], member, norm_ref, row + 2, count, coef)
        conv_rows(lambda chunk: fetch_rows(kern, which, 1, chunk, wbuf, wsem), mid, act, wbuf, coef, acc, width)
        add_rows(out_ref, acc, image)
        for index in range(len(pieces)):
            drain(landed(index), send_sem.at[index])

    vmem = pl.BlockSpec(memory_space=pltpu.VMEM)
    hbm = pl.BlockSpec(memory_space=pl.ANY)
    dma = pltpu.SemaphoreType.DMA
    return pl.pallas_call(
        kernel,
        out_shape=[
            jax.ShapeDtypeStruct((tokens, chans), BF16),
            jax.ShapeDtypeStruct((block_norms + 8, chans), F32),
            jax.ShapeDtypeStruct((1, chans), F32),
            jax.ShapeDtypeStruct((text_rows, chans), BF16),
            jax.ShapeDtypeStruct((chans, text_rows), BF16),
        ],
        in_specs=[hbm] * 8,
        out_specs=[vmem] * 5,
        scratch_shapes=[
            pltpu.VMEM((tokens, chans), BF16),
            pltpu.VMEM((tokens, chans), BF16),
            pltpu.VMEM((3, tokens + 2 * width, chans), BF16),
            pltpu.VMEM((2, len(taps()) * CK, chans), BF16),
            pltpu.VMEM((tokens, chans), F32),
            pltpu.VMEM(time_emb.shape, BF16),
            pltpu.VMEM((peers, chans), F32),
            pltpu.VMEM((2 * peers, chans), F32),
            pltpu.VMEM((peers, 8, 128), F32),
            pltpu.VMEM((peers, 8, 128), F32),
            pltpu.VMEM((8, chans), F32),
            pltpu.VMEM(res_norm.shape, BF16),
            pltpu.VMEM(attn_norm.shape, BF16),
            pltpu.VMEM(context.shape, BF16),
            pltpu.VMEM((text_rows, text_dim), BF16),
            pltpu.VMEM(cross_kv.shape, BF16),
            dma((2,)), dma, dma, dma((3,)), dma((2,)), dma((len(pieces),)), dma((len(pieces),)), dma, dma,
        ],
        compiler_params=pltpu.CompilerParams(vmem_limit_bytes=VMEM_IN, collective_id=0, has_side_effects=True),
        cost_estimate=cost_of(36 * tokens * chans * chans, 36 * chans * chans),
        name='res_block_in',
    )(latent, time_emb, context, res_conv, res_time, res_norm, attn_norm, cross_kv)


def res_block_out(hidden, bias, res_conv, norms, width, groups, peers):
    which = 1
    tokens, chans = hidden.shape
    band = tokens // peers
    chunks = chans // CK
    tiles = tokens // TM
    per_tile = TM // band
    count = float(tokens * (chans // groups))

    def kernel(x_ref, bias_ref, kern, norm_ref, out_ref, mid, result, act, wbuf, cbuf, acc, coef, wsem, csem, send_sem, recv_sem):
        me = lax.axis_index('sp')
        start_all(fetch_rows(kern, which, 0, 0, wbuf, wsem))
        meet(peers, me)
        clear_edges(act, width)
        member = members(chans, groups)
        row = 4 * which
        acc[...] = jnp.zeros_like(acc)
        norm_from(x_ref, member, norm_ref, row, count, coef)
        conv_rows(lambda chunk: fetch_rows(kern, which, 0, chunk, wbuf, wsem), x_ref, act, wbuf, coef, acc, width)
        start_all(fetch_cols(kern, which, 1, 0, cbuf, csem))
        add_and_norm(mid, acc, bias_ref[...], member, norm_ref, row + 2, count, coef)

        def build(row, rows):
            @loop(chunks)
            def _(chunk):
                activate(mid, act, coef, pl.multiple_of(chunk * CK, CK), CK, row, rows, width)

        def build_tile(tile):
            build(tile * TM, TM)

            @pl.when(tile + 1 < tiles)
            def _():
                build((tile + 1) * TM, width)

        turn = lax.rem(lax.div(me, per_tile) + tiles // 2, tiles)
        build_tile(turn)

        @pl.when(turn > 0)
        def _():
            build(turn * TM - width, width)

        await_peers(peers)

        @loop(chunks)
        def _(chunk):
            slot = lax.rem(chunk, 2)
            cols = chunk_cols(chunk)

            @pl.when(chunk + 1 < chunks)
            def _():
                start_all(fetch_cols(kern, which, 1, chunk + 1, cbuf, csem))

            wait_all(fetch_cols(kern, which, 1, chunk, cbuf, csem))

            @loop(tiles)
            def _(step):
                tile = lax.rem(step + turn, tiles)
                part = sum(nn(shifted(act, dx, tile, dy, width, slice(None)), cbuf[slot, tap]) for tap, (dy, dx) in enumerate(taps()))
                rows = tile_rows(tile)
                result[rows, cols] = (x_ref[rows, cols].astype(F32) + part).astype(BF16)
                for idx in range(per_tile):
                    peer = tile * per_tile + idx
                    block = result.at[pl.ds(pl.multiple_of(peer * band, band), band), cols]

                    @pl.when(peer == me)
                    def _():
                        out_ref[me, :, cols] = block[...]

                    @pl.when(peer != me)
                    def _():
                        remote(block, out_ref.at[me, :, cols], send_sem, recv_sem, peer).start()

                @pl.when((chunk == 0) & (step + 1 < tiles))
                def _():
                    build_tile(lax.rem(step + 1 + turn, tiles))

        others = out_ref.at[pl.ds(0, peers - 1)]
        drain(others, send_sem)
        drain(others, recv_sem)

    vmem = pl.BlockSpec(memory_space=pltpu.VMEM)
    hbm = pl.BlockSpec(memory_space=pl.ANY)
    dma = pltpu.SemaphoreType.DMA
    return pl.pallas_call(
        kernel,
        out_shape=jax.ShapeDtypeStruct((peers, band, chans), BF16),
        in_specs=[vmem, vmem, hbm, vmem],
        out_specs=vmem,
        scratch_shapes=[
            pltpu.VMEM((tokens, chans), BF16),
            pltpu.VMEM((tokens, chans), BF16),
            pltpu.VMEM((3, tokens + 2 * width, chans), BF16),
            pltpu.VMEM((2, len(taps()) * CK, chans), BF16),
            pltpu.VMEM((2, len(taps()), chans, CK), BF16),
            pltpu.VMEM((tokens, chans), F32),
            pltpu.VMEM((8, chans), F32),
            dma((2,)), dma((2,)), dma, dma,
        ],
        compiler_params=pltpu.CompilerParams(vmem_limit_bytes=VMEM_OUT, collective_id=1, has_side_effects=True),
        cost_estimate=cost_of(36 * tokens * chans * chans, 36 * chans * chans),
        name='res_block_out',
    )(hidden, bias, res_conv, norms)


def cost_of(flops, nbytes):
    return pl.CostEstimate(flops=flops, bytes_accessed=nbytes, transcendentals=0)


def transformer(hidden, ctx_keys, ctx_vals, norms, norm_row, proj_inout, qkv_t, self_out, cross_q_t, cross_out, ff_in, ff_out, groups, heads, text):
    tokens, chans = hidden.shape
    text_rows = ctx_keys.shape[0]
    head_dim = chans // heads
    pairs = heads // 2
    pair = 2 * head_dim
    count = float(tokens * (chans // groups))
    tiles = tokens // TM
    ff_steps = ff_out.shape[0] // chans
    qw = 512 if chans >= 1024 else 256
    kb = 256
    scale = head_dim ** -0.5
    half = chans // 2

    def kernel(h_ref, ctx_k, ctx_v, norm_ref, pio, wqkv, wo, cq, co, f1, f2, out_ref, ring, tok, aux, both, keys, acc, coef, rsem):
        units = {
            'in': (pio.at[0], 0, 0), 'q': (wqkv.at[0], 0, 1), 'k': (wqkv.at[1], 1, 0), 'v': (wqkv.at[2], 1, 1),
            'o': (wo, 1, 0), 'cq': (cq, 1, 1), 'co': (co, 1, 2), 'out': (pio.at[1], 0, 0),
        }

        def copy_of(name):
            src, group, place = units[name]
            return pltpu.make_async_copy(src, ring.at[group, place], rsem.at[group, place])

        def start(*names):
            for name in names:
                copy_of(name).start()

        def take(name):
            copy_of(name).wait()
            _, group, place = units[name]
            return ring.at[group, place]

        def ff_copies(step, group):
            cols = pl.multiple_of(step * chans, chans)
            return [
                pltpu.make_async_copy(f1.at[:, pl.ds(cols, chans)], ring.at[group, 0], rsem.at[group, 0]),
                pltpu.make_async_copy(f1.at[:, pl.ds(cols + ff_steps * chans, chans)], ring.at[group, 1], rsem.at[group, 1]),
                pltpu.make_async_copy(f2.at[pl.ds(cols, chans), :], ring.at[group, 2], rsem.at[group, 2]),
            ]

        start('in', 'q', 'k', 'v', 'co')

        tot, sqr = channel_sums(h_ref, tokens, chans)
        member = members(chans, groups)
        sums = group_sums(two_rows(tot, sqr), member)
        group_affine(sums, norm_ref[norm_row:norm_row + 1], norm_ref[norm_row + 1:norm_row + 2], member, count, coef, 1.0)

        def project_rows(weight, src, base, normed_to, clear=None):
            def norm_tile(tile):
                rows = tile_rows(tile)
                normed_to[rows, :] = layer_norm(tok[rows, :].astype(F32))

            @loop(tiles)
            def _(tile):
                norm_tile(jnp.maximum(tile - 1, 0))
                rows = tile_rows(tile)
                tok[rows, :] = (base(rows) + nn(src(rows), weight[...])).astype(BF16)
                if clear is not None:
                    clear[rows, :] = jnp.zeros((TM, chans), F32)

            norm_tile(tiles - 1)

        project_rows(take('in'), lambda rows: (h_ref[rows, :].astype(F32) * coef[0:1] + coef[1:2]).astype(BF16), lambda rows: 0.0, aux)

        q_t, v_t = both.at[0], both.at[1]

        def transposed(weight, src, dst, factor):
            @loop(2)
            def _(part):
                rows = pl.ds(pl.multiple_of(part * half, half), half)
                dst[rows, :] = (nt(weight[rows, :], src[...]).astype(BF16) * factor).astype(BF16)

        w_key = take('k')

        @loop(tokens // 512)
        def _(part):
            rows = pl.ds(pl.multiple_of(part * 512, 512), 512)
            keys[rows, :] = nt(aux[rows, :], w_key[...]).astype(BF16)
        start('o')

        @loop(2)
        def _(which):
            pltpu.make_async_copy(wqkv.at[2 * which], ring.at[which, 1], rsem.at[which, 1]).wait()
            transposed(ring.at[which, 1], aux, both.at[which], jnp.where(which == 0, scale, 1.0))
        start('cq')
        for copy in ff_copies(0, 0):
            copy.start()

        row_head = lax.broadcasted_iota(jnp.int32, (pair, 1), 0) < head_dim

        def query_of(hp, first, wide, head):
            both = q_t[pl.ds(pl.multiple_of(hp * pair, pair), pair), pl.ds(first, wide)]
            keep = row_head if head == 0 else jnp.logical_not(row_head)
            return jnp.where(keep, both, jnp.zeros_like(both))

        def pair_cols(hp):
            return pl.ds(pl.multiple_of(hp * pair, pair), pair)

        halves = tokens // qw
        blocks = pairs * halves
        unroll = next(count for count in (5, 4, 2, 1) if blocks % count == 0)
        scores = [acc.at[:, pl.ds(h * qw, qw)] for h in range(2)]
        probs = [out_ref.at[:, pl.ds(h * qw, qw)] for h in range(2)]
        parts = tokens // kb

        def place(block):
            hp = lax.div(block, halves)
            return hp, pl.multiple_of((block - hp * halves) * qw, qw)

        def fold(vals, func):
            return func(vals.reshape(-1, 8, vals.shape[-1]), axis=0)

        def score_part(block, query, head, part):
            hp, _ = place(block)
            vals = nn(keys[part * kb:(part + 1) * kb, pair_cols(hp)], query)
            scores[head][part * kb:(part + 1) * kb, :] = vals
            return fold(vals, jnp.max)

        def exp_part(head, part, top):
            vals = jnp.exp(scores[head][part * kb:(part + 1) * kb, :] - top)
            probs[head][part * kb:(part + 1) * kb, :] = vals.astype(BF16)
            return fold(vals, jnp.sum)

        def value_of(block, head, denom):
            hp, _ = place(block)
            vals = v_t[pl.ds(pl.multiple_of(hp * pair + head * head_dim, head_dim), head_dim), :]
            return nn(vals, probs[head][...]) * (1.0 / denom)

        def block_query(block, head):
            hp, first = place(block)
            return query_of(hp, first, qw, head)

        def softmax_stage(score_block, score_head, exp_head, top):
            tops, sums = [], []
            query = block_query(score_block, score_head)
            for part in range(parts):
                tops.append(score_part(score_block, query, score_head, part))
                sums.append(exp_part(exp_head, part, top))
            new_top = jnp.max(functools.reduce(jnp.maximum, tops), axis=0, keepdims=True)
            return new_top, keep_sum(functools.reduce(jnp.add, sums))

        def emit(block, low, high):
            hp, first = place(block)
            aux[pl.ds(first, qw), pair_cols(hp)] = jnp.concatenate([low, high], axis=0).T.astype(BF16)

        top_first = jnp.max(functools.reduce(jnp.maximum, [score_part(0, block_query(0, 0), 0, part) for part in range(parts)]), axis=0, keepdims=True)
        zero_row = jnp.ones((1, qw), F32)
        zero_out = jnp.zeros((head_dim, qw), F32)

        def attend_block(block, carry):
            top0, denom1, low = carry
            before = jnp.maximum(block - 1, 0)
            high = value_of(before, 1, denom1)
            emit(before, low, high)
            top1, denom0 = softmax_stage(block, 1, 0, top0)
            after = jnp.minimum(block + 1, blocks - 1)
            low = value_of(block, 0, denom0)
            top0, denom1 = softmax_stage(after, 0, 1, top1)
            return top0, denom1, low

        def attend_blocks(step, carry):
            for sub in range(unroll):
                carry = attend_block(step * unroll + sub, carry)
            return carry

        _, denom1, low = lax.fori_loop(0, blocks // unroll, attend_blocks, (top_first, zero_row, zero_out))
        emit(blocks - 1, low, value_of(blocks - 1, 1, denom1))

        project_rows(take('o'), lambda rows: aux[rows, :], lambda rows: tok[rows, :].astype(F32), keys)
        transposed(take('cq'), keys, q_t, scale)

        text_valid = lax.broadcasted_iota(jnp.int32, (text_rows, 1), 0) < text

        wide_step = max(count for count in (CROSS_PAIRS, 2, 1) if pairs % count == 0)

        @loop(pairs // wide_step)
        def _(step):
            for sub in range(wide_step):
                hp = step * wide_step + sub
                outs = []
                for head in range(2):
                    vals = nn(ctx_k[:, pair_cols(hp)], query_of(hp, 0, tokens, head))
                    vals = jnp.where(text_valid, vals, -jnp.inf)
                    weights = jnp.exp(vals - jnp.max(vals, axis=0, keepdims=True))
                    denom = keep_sum(weights)
                    text_vals = ctx_v[pl.ds(pl.multiple_of(hp * pair + head * head_dim, head_dim), head_dim), :]
                    outs.append(nn(text_vals, weights.astype(BF16)) * (1.0 / denom))
                aux[:, pair_cols(hp)] = jnp.concatenate(outs, axis=0).T.astype(BF16)

        project_rows(take('co'), lambda rows: aux[rows, :], lambda rows: tok[rows, :].astype(F32), keys, acc)
        for copy in ff_copies(1, 1):
            copy.start()

        @loop(ff_steps)
        def _(step):
            group = lax.rem(step, 2)
            for copy in ff_copies(step, group):
                copy.wait()

            @loop(tiles, unroll=2)
            def _(tile):
                rows = tile_rows(tile)
                src = keys[rows, :]
                value = nn(src, ring[group, 0])
                gate = nn(src, ring[group, 1])
                gated = (value * (0.5 * gate * (1.0 + lax.erf(gate * (0.5 ** 0.5))))).astype(BF16)
                acc[rows, :] += nn(gated, ring[group, 2])

            @pl.when(step + 2 < ff_steps)
            def _():
                for copy in ff_copies(step + 2, group):
                    copy.start()

            @pl.when(step == ff_steps - 2)
            def _():
                start('out')

        w_fin = take('out')

        @loop(tiles)
        def _(tile):
            rows = tile_rows(tile)
            t = (tok[rows, :].astype(F32) + acc[rows, :]).astype(BF16)
            out_ref[rows, :] = (h_ref[rows, :].astype(F32) + nn(t, w_fin[...])).astype(BF16)

    vmem = pl.BlockSpec(memory_space=pltpu.VMEM)
    hbm = pl.BlockSpec(memory_space=pl.ANY)
    flops = 2 * tokens * chans * chans * (8 + 3 * ff_steps) + 4 * tokens * tokens * chans
    return pl.pallas_call(
        kernel,
        out_shape=jax.ShapeDtypeStruct(hidden.shape, BF16),
        in_specs=[vmem] * 4 + [hbm] * 7,
        out_specs=vmem,
        scratch_shapes=[
            pltpu.VMEM((2, 3, chans, chans), BF16),
            pltpu.VMEM((tokens, chans), BF16),
            pltpu.VMEM((tokens, chans), BF16),
            pltpu.VMEM((2, chans, tokens), BF16),
            pltpu.VMEM((tokens, chans), BF16),
            pltpu.VMEM((tokens, chans), F32),
            pltpu.VMEM((8, chans), F32),
            pltpu.SemaphoreType.DMA((2, 3)),
        ],
        compiler_params=pltpu.CompilerParams(vmem_limit_bytes=VMEM_MID),
        cost_estimate=cost_of(flops, 50 * chans * chans),
        name='transformer',
    )(hidden, ctx_keys, ctx_vals, norms, proj_inout, qkv_t, self_out, cross_q_t, cross_out, ff_in, ff_out)


def solution(mesh):
    num_bands = mesh.shape['sp']

    def local_stage(latent, time_emb, context, res_conv, res_time, res_norm, attn_norm, proj_inout, self_qkv, self_out, cross_q, cross_kv, cross_out, ff_in, ff_out):
        images, band_rows, width, chans = latent.shape
        assert images == num_bands
        band = band_rows * width
        heads, head_dim = self_out.shape[:2]
        groups = res_norm.shape[3]
        text, text_dim = context.shape[1:]
        flat_kv = jnp.transpose(cross_kv, (0, 2, 3, 1)).reshape(2, chans, text_dim)
        first, norms, bias, ctx_keys, ctx_vals = res_block_in(
            latent.reshape(images, band, chans), pltpu.with_memory_space_constraint(time_emb, pltpu.HBM), jnp.transpose(context, (1, 0, 2)).reshape(text * images, text_dim), res_conv, res_time,
            pltpu.with_memory_space_constraint(res_norm.reshape((-1,) + res_norm.shape[3:]), pltpu.HBM), pltpu.with_memory_space_constraint(attn_norm, pltpu.HBM), flat_kv, text, width)
        middle = transformer(
            first, ctx_keys, ctx_vals, norms, res_norm.shape[0] * res_norm.shape[1] * res_norm.shape[2], proj_inout,
            jnp.transpose(self_qkv, (0, 2, 3, 1)).reshape(3, chans, chans),
            self_out.reshape(chans, chans),
            jnp.transpose(cross_q, (1, 2, 0)).reshape(chans, chans),
            cross_out.reshape(chans, chans), ff_in, ff_out, groups, heads, text)
        out = res_block_out(middle, bias, res_conv, norms, width, groups, num_bands)
        return out.reshape(latent.shape)

    band_spec = P('dp', 'sp', None, None)
    shared = P()
    in_specs = (band_spec, P('dp', None), P('dp', None, None)) + (shared,) * 12
    return jax.shard_map(local_stage, mesh=mesh, in_specs=in_specs, out_specs=band_spec, check_vma=False)
```
